32 devices in a mesh: dp: 8 (over y, x, core), seq: 4 (over z).
Axes of the slice: x: 2, y: 2, z: 4, core: 2. Of those that a mesh axis runs over, the one named last changes fastest.
Arguments:
- inputs: bfloat16 [24, 1024, 768], P('dp', 'seq'), may hold values from -6 to 6
- segments: int32 [24, 1024], P('dp'), may hold values from 0 to 3, never falling along the last dimension, each value on 1 to 512 neighbouring positions
- cotangent: bfloat16 [24, 1024, 768], P('dp', 'seq'), may hold values from -6 to 6
- weights: float32 [768, 9216], P(None, 'dp'), may hold values from -0.18042196 to 0.18042196
- first_moment: float32 [768, 9216], P(None, 'dp'), may hold values from -112 to 112
- second_moment: float32 [768, 9216], P(None, 'dp'), may hold values from 12.288 to 98.304
- bases: float32 [4, 768, 768], replicated, may hold values from -0.08660254 to 0.8866025
- right_bases: float32 [9216, 3072], P('dp'), may hold values from -0.08660254 to 0.8866025, as said below
- small: float32 [9216], replicated, may hold values from -2 to 2
- small_first: float32 [9216], replicated, may hold values from -112 to 112
- small_second: float32 [9216], replicated, may hold values from 12.288 to 98.304
Outputs:
- output: bfloat16 [24, 1024, 768], P('dp', 'seq')
- input_grad: bfloat16 [24, 1024, 768], P('dp', 'seq')
- weight_grad: float32 [768, 9216], P(None, 'dp')
- first_new: float32 [768, 9216], P(None, 'dp')
- second_new: float32 [768, 9216], P(None, 'dp')
- weights_new: float32 [768, 9216], P(None, 'dp')
- weights_low: bfloat16 [768, 9216], P(None, 'dp')
- small_grad: float32 [9216], replicated
- small_first_new: float32 [9216], replicated
- small_second_new: float32 [9216], replicated
- small_new: float32 [9216], replicated
The draws below stay inside these ranges and needn't reach their ends.
Inputs may be any that keep to these rules, and one draw needn't show every extreme that they name: `segments`: along each row the ids never fall; every id covers 1 to 512 positions and one covers exactly 512. `right_bases`: entries of a row past the number of columns of that row's block are zero.
All inputs are finite; a program needn't handle non-finite values.
Results may differ from the reference program's by a relative error of at most 0.012.
Values may be sent and summed in bfloat16 or wider, within the bound.
A program may use at most 256 MiB of HBM per device.

```python
import math
import jax
import jax.numpy as jnp
import numpy as np
from jax import lax

D = 768
HEADS = 12
HD = 64
FF = 3072
LEN = 1024
NSEG = 4
STEP = 10
SEQS = 3
SEQUENCES = 24
WCOLS = 9216
RPAD = 3072
SMALLN = 9216
N_DP = 8


def column_kinds():
    share = WCOLS // N_DP
    rows = jnp.arange(WCOLS)
    shard = rows // share
    within = rows % share
    width_qkv = 3 * D // N_DP
    width_out = D // N_DP
    width_ff = FF // N_DP
    begin = jnp.where(within < width_qkv, 0, jnp.where(within < width_qkv + width_out, width_qkv, jnp.where(within < width_qkv + width_out + width_ff, width_qkv + width_out, width_qkv + width_out + width_ff)))
    width = jnp.where(within < width_qkv, width_qkv, jnp.where(within < width_qkv + width_out, width_out, width_ff))
    is_down = within >= width_qkv + width_out + width_ff
    local = shard * width + within - begin
    extent = width * N_DP
    return (local, extent, is_down)


def draw_weights(key, part):
    raw = jnp.clip(jax.random.normal(key, (D, WCOLS), jnp.float32), -5.0, 5.0)
    local, extent, is_down = column_kinds()
    factor = jnp.where(is_down, FF ** (-0.5), D ** (-0.5))
    return (raw * factor[None, :]).astype(jnp.float32)


def draw_bases(key, part):
    raw = jnp.clip(jax.random.normal(key, (4, D, D), jnp.float32), -4.0, 4.0)
    ident = jnp.eye(D, dtype=jnp.float32)[None]
    return (0.8 * ident + 0.6 * D ** (-0.5) * raw).astype(jnp.float32)


def draw_right_bases(key, part):
    raw = jnp.clip(jax.random.normal(key, (WCOLS, RPAD), jnp.float32), -4.0, 4.0)
    local, extent, is_down = column_kinds()
    cols = jnp.arange(RPAD)
    ident = (cols[None, :] == local[:, None]).astype(jnp.float32)
    factor = 0.6 / jnp.sqrt(extent.astype(jnp.float32))
    values = 0.8 * ident + factor[:, None] * raw
    return jnp.where(cols[None, :] < extent[:, None], values, 0.0).astype(jnp.float32)


def draw_small(key, part):
    gain_key, shift_key = jax.random.split(key)
    gains = jax.random.uniform(gain_key, (2 * D,), jnp.float32, 0.6, 1.4)
    shifts = jnp.clip(0.5 * jax.random.normal(shift_key, (6 * D + FF,), jnp.float32), -2.0, 2.0)
    return jnp.concatenate([gains, shifts]).astype(jnp.float32)


def levels(rng, shape, cuts, least, largest):
    factor_of = 1.0
    for position, shards_of in cuts:
        heights = jax.random.uniform(jax.random.fold_in(jax.random.fold_in(rng, 6), position), (shards_of,), jnp.float32, least / len(cuts), largest / len(cuts))
        factor_of = factor_of * jnp.repeat(jnp.exp(heights), shape[position] // shards_of).reshape((-1,) + (1,) * (len(shape) - 1 - position))
    return factor_of


def split_up(count, total, bound, lean):
    weights = [(1 << 20) // math.isqrt(rank ** lean) + 1 for rank in range(2, count + 1)]
    surplus, counts = total - bound - (count - 1), [1] * (count - 1)
    while surplus > 0:
        free = [i for i in range(count - 1) if counts[i] < bound]
        mass, budget = sum([weights[i] for i in free]), surplus
        for i in free:
            extra = min(bound - counts[i], max(1, budget * weights[i] // mass), surplus)
            counts[i] = counts[i] + extra
            surplus = surplus - extra
    return np.array([bound] + counts)


def ragged_sizes(own_key, amount, total, bound, slope):
    if amount == 2:
        one = jax.random.randint(own_key, (), max(1, total - bound), min(bound, total - 1) + 1)
        return jnp.stack([one, total - one])
    lengths = jnp.asarray(split_up(amount, total, bound, slope), jnp.int32)
    couples = (amount - 1) // 2
    giver, taker = lengths[1:1 + 2 * couples:2], lengths[2:2 + 2 * couples:2]
    room = jnp.minimum(giver - 1, bound - taker)
    moved = jax.random.randint(jax.random.fold_in(own_key, 1), (couples,), 0, 1 << 20) % (room + 1)
    lengths = lengths.at[1:1 + 2 * couples:2].set(giver - moved).at[2:2 + 2 * couples:2].set(taker + moved)
    return lengths[jax.random.permutation(jax.random.fold_in(own_key, 2), amount)]


def normal_values(own_key, shape, scale, reach, cuts=(), kind=jnp.bfloat16):
    loudness = levels(own_key, shape, cuts, -0.22, 0.18) if cuts else 1.0
    values = jax.random.normal(own_key, shape, jnp.float32) * scale * loudness
    return jnp.minimum(jnp.maximum(values, -reach), reach).astype(kind)


def setup_inputs(seed: int = 0) -> dict:
    seeds = jax.random.split(jax.random.key(seed), 12)
    inputs = normal_values(seeds[0], (SEQUENCES, LEN, D), 1.0, 6.0, ((0, 8), (1, 4)))
    segments = jax.vmap(lambda own: jnp.searchsorted(jnp.cumsum(ragged_sizes(own, NSEG, LEN, LEN // 2, 0)), jnp.arange(LEN), side="right"))(jax.random.split(seeds[1], SEQUENCES)).reshape((SEQUENCES, LEN)).astype(jnp.int32)
    cotangent = normal_values(seeds[2], (SEQUENCES, LEN, D), 1.0, 6.0, ((0, 8), (1, 4)))
    weights = draw_weights(jax.random.fold_in(seeds[11], 71), 0)
    first_moment = normal_values(seeds[4], (D, WCOLS), (0.11 * (N_DP * SEQS * LEN) ** 0.5), 112.0, ((1, 8),), jnp.float32)
    second_moment = jnp.clip(jnp.exp(math.log(98.304) - 2.0794415 * jax.random.uniform(seeds[5], (D, WCOLS), jnp.float32) ** levels(seeds[5], (D, WCOLS), ((1, 8),), -0.2, 0.2)), 12.288, 98.304)
    bases = draw_bases(jax.random.fold_in(seeds[11], 71), 0)
    right_bases = draw_right_bases(jax.random.fold_in(seeds[11], 71), 0)
    small = draw_small(jax.random.fold_in(seeds[11], 71), 0)
    small_first = normal_values(seeds[9], (SMALLN,), (0.11 * (N_DP * SEQS * LEN) ** 0.5), 112.0, (), jnp.float32)
    small_second = jnp.clip(jnp.exp(jax.random.uniform(seeds[10], (SMALLN,), jnp.float32, math.log(12.288), math.log(98.304))), 12.288, 98.304)
    return dict(inputs=inputs, segments=segments, cotangent=cotangent, weights=weights, first_moment=first_moment, second_moment=second_moment, bases=bases, right_bases=right_bases, small=small, small_first=small_first, small_second=small_second)


@jax.custom_vjp
def low(v):
    return lax.optimization_barrier(v.astype(jnp.bfloat16)).astype(jnp.float32)

@jax.custom_vjp
def low_back(v):
    return v

def low_keep(v):
    return (low(v), None)

def low_pass(kept, grad):
    return (grad,)

def back_keep(v):
    return (v, None)

def back_low(kept, grad):
    return (low(grad),)
low.defvjp(low_keep, low_pass)
low_back.defvjp(back_keep, back_low)
highest = lax.Precision.HIGHEST
norm_eps = 1e-12
beta_first = 0.9
beta_second = 0.999
adam_eps = 1e-08
learn_rate = 0.03
small_rate = 0.3
per_block = 4

def block_layout():
    widths = [3 * D // N_DP, D // N_DP, FF // N_DP, FF // N_DP]
    offsets = [0, widths[0], widths[0] + widths[1], widths[0] + widths[1] + widths[2]]
    return (widths, offsets)

def split_cols(matrix):
    widths, offsets = block_layout()
    share = WCOLS // N_DP
    shaped = matrix.reshape(matrix.shape[0], N_DP, share)
    return [shaped[:, :, offsets[which]:offsets[which] + widths[which]].reshape(matrix.shape[0], N_DP * widths[which]) for which in range(4)]

def join_cols(parts):
    widths, offsets = block_layout()
    rows = parts[0].shape[0]
    return jnp.concatenate([parts[which].reshape(rows, N_DP, widths[which]) for which in range(4)], axis=2).reshape(rows, WCOLS)

def right_blocks(right_bases):
    widths, offsets = block_layout()
    share = WCOLS // N_DP
    shaped = right_bases.reshape(N_DP, share, RPAD)
    result = []
    for which in range(4):
        extent = N_DP * widths[which]
        result.append(shaped[:, offsets[which]:offsets[which] + widths[which], :extent].reshape(extent, extent))
    return result

def unpack(small):
    return [small[index * D:(index + 1) * D] for index in range(8)] + [small[8 * D:]]

def normalize(resid, gain, shift):
    centre = resid - lax.optimization_barrier(jnp.mean(resid, axis=-1, keepdims=True))
    spread = lax.optimization_barrier(jnp.mean(centre * centre, axis=-1, keepdims=True))
    return centre * lax.rsqrt(spread + norm_eps) * gain + shift

def forward(acts, marks, weights, small):
    gain_one, gain_two, shift_one, shift_two, bias_query, bias_value, bias_out, bias_down, bias_up = unpack(small)
    weights_low = low(weights)
    w_qkv, w_out, w_up, w_down = split_cols(weights_low)
    token_rows = low(acts)
    project = jnp.einsum('gtd,de->gte', token_rows, w_qkv, precision=highest)
    queries = low_back(low(project[..., :D] + bias_query))
    keys_all = low_back(low(project[..., D:2 * D]))
    values = low_back(low(project[..., 2 * D:] + bias_value))
    blocks = acts.shape[0]
    queries = queries.reshape(blocks, LEN, HEADS, HD)
    keys_all = keys_all.reshape(blocks, LEN, HEADS, HD)
    values = values.reshape(blocks, LEN, HEADS, HD)
    scores = low_back(jnp.einsum('gqhd,gkhd->ghqk', queries, keys_all, precision=highest) * HD ** (-0.5))
    same_doc = (marks[:, :, None] == marks[:, None, :])[:, None]
    masked = jnp.where(same_doc, scores, -1e+30)
    probs = jax.nn.softmax(masked, axis=-1)
    mixed = jnp.einsum('ghqk,gkhd->gqhd', low(probs), values, precision=highest)
    context = low_back(low(mixed.reshape(blocks, LEN, D)))
    attended = low_back(jnp.einsum('gtc,cd->gtd', context, w_out, precision=highest) + bias_out)
    first = normalize(acts + attended, gain_one, shift_one)
    upward = low_back(jnp.einsum('gtd,df->gtf', low(first), w_up, precision=highest) + bias_up)
    active = low(jax.nn.gelu(upward, approximate=False))
    downward = low_back(jnp.einsum('gtf,df->gtd', active, w_down, precision=highest) + bias_down)
    return normalize(first + downward, gain_two, shift_two)

def moments(grad, first, second):
    first_out = beta_first * first + (1.0 - beta_first) * grad
    second_out = beta_second * second + (1.0 - beta_second) * grad * grad
    heading = first_out / (1.0 - beta_first ** STEP) / (jnp.sqrt(second_out / (1.0 - beta_second ** STEP)) + adam_eps)
    return (first_out, second_out, heading)

def reference(inputs, segments, cotangent, weights, first_moment, second_moment, bases, right_bases, small, small_first, small_second):
    blocks = SEQUENCES // per_block
    acts = inputs.astype(jnp.float32).reshape(blocks, per_block, LEN, D)
    marks = segments.reshape(blocks, per_block, LEN)
    pulls = cotangent.astype(jnp.float32).reshape(blocks, per_block, LEN, D)

    def visit(carry, item):
        grad_w, grad_s = carry
        block_in, block_seg, block_cot = item

        def apply(act, wts, sml):
            return forward(act, block_seg, wts, sml)
        result, puller = jax.vjp(apply, block_in, weights, small)
        d_in, d_w, d_s = puller(block_cot)
        return ((grad_w + d_w, grad_s + d_s), (result.astype(jnp.bfloat16), d_in.astype(jnp.bfloat16)))
    start = (jnp.zeros_like(weights), jnp.zeros_like(small))
    (weight_grad, small_grad), (outs, grads_in) = lax.scan(visit, start, (acts, marks, pulls))
    rights = right_blocks(right_bases)
    grad_parts = split_cols(weight_grad)
    rotated = join_cols([jnp.dot(jnp.dot(bases[which].T, grad_parts[which], precision=highest), rights[which], precision=highest) for which in range(4)])
    first_new, second_new, heading = moments(rotated, first_moment, second_moment)
    head_parts = split_cols(heading)
    update = join_cols([jnp.dot(jnp.dot(bases[which], head_parts[which], precision=highest), rights[which].T, precision=highest) for which in range(4)])
    weights_new = weights - learn_rate * update
    small_first_new, small_second_new, small_heading = moments(small_grad, small_first, small_second)
    small_new = small - small_rate * small_heading
    return (outs.reshape(SEQUENCES, LEN, D), grads_in.reshape(SEQUENCES, LEN, D), weight_grad, first_new, second_new, weights_new, weights_new.astype(jnp.bfloat16), small_grad, small_first_new, small_second_new, small_new)
```

```python
import functools
import math

import jax
import jax.numpy as jnp
from jax import lax
from jax.experimental import pallas as pl
from jax.experimental.pallas import tpu as pltpu
from jax.sharding import PartitionSpec as P

D = 768
HEADS = 12
HD = 64
FF = 3072
STEP = 10


norm_eps = 1e-12
beta_first = 0.9
beta_second = 0.999
adam_eps = 1e-08
learn_rate = 0.03
small_rate = 0.3

TILE = 256
LANES = 128
WINDOWS = (256, 512, 640, 768, 1024)
NEG = -1e30
VMEM_LIMIT = 60 * 1024 * 1024


def dot_dims(left, right, left_dim, right_dim):
    return lax.dot_general(
        left, right, (((left_dim,), (right_dim,)), ((), ())), preferred_element_type=jnp.float32
    )


def normalize(resid, gain, shift):
    centre = resid - jnp.mean(resid, axis=-1, keepdims=True)
    spread = jnp.mean(centre * centre, axis=-1, keepdims=True)
    inv_std = lax.rsqrt(spread + norm_eps)
    scaled = centre * inv_std
    return (scaled * gain + shift, scaled, inv_std)


def norm_back(grad, scaled, inv_std, gain):
    lifted = grad * gain
    return inv_std * (
        lifted
        - jnp.mean(lifted, axis=-1, keepdims=True)
        - scaled * jnp.mean(lifted * scaled, axis=-1, keepdims=True)
    )


def moments(grad, first, second):
    first_out = beta_first * first + (1.0 - beta_first) * grad
    second_out = beta_second * second + (1.0 - beta_second) * grad * grad
    heading = (
        first_out
        / (1.0 - beta_first**STEP)
        / (jnp.sqrt(second_out / (1.0 - beta_second**STEP)) + adam_eps)
    )
    return (first_out, second_out, heading)


def windows_of(length):
    return tuple(size for size in WINDOWS if size < length) + (length,)


def key_windows(marks):
    rows, length = marks.shape
    tile = min(TILE, length)
    sizes = windows_of(length)
    heads = marks[:, ::tile]
    tails = marks[:, tile - 1 :: tile]
    low = jnp.sum((marks[:, None, :] < heads[:, :, None]).astype(jnp.int32), axis=-1)
    high = jnp.sum((marks[:, None, :] <= tails[:, :, None]).astype(jnp.int32), axis=-1)
    begin = low // LANES * LANES
    need = high - begin
    which = jnp.zeros_like(need)
    for size in sizes[:-1]:
        which = which + (need > size).astype(jnp.int32)
    width = jnp.asarray(sizes, jnp.int32)[which]
    begin = jnp.minimum(begin, length - width)
    return jnp.stack([begin, which], axis=-1).reshape(rows, -1)


def head_lanes(half, shape):
    lane = lax.broadcasted_iota(jnp.int32, shape, 1)
    return (lane >= half * HD) & (lane < (half + 1) * HD)


def attend_kernel(sizes, tile, table, q_ref, k_ref, v_ref, col_ref, row_ref, ctx_ref, log_ref, vt_ref):
    length = k_ref.shape[0]
    row = pl.program_id(0)
    vt_ref[...] = v_ref[...].astype(jnp.float32).T.astype(jnp.bfloat16)

    @pl.loop(0, length // tile)
    def _(step):
        begin = pl.multiple_of(table[row, 2 * step], LANES)
        which = table[row, 2 * step + 1]
        rows = pl.ds(pl.multiple_of(step * tile, tile), tile)
        for number, size in enumerate(sizes):

            @pl.when(which == number)
            def _(size=size):
                keys = k_ref[pl.ds(begin, size), :]
                marks = col_ref[pl.ds(begin, size), :]
                same = jnp.concatenate([marks] * (tile // LANES), axis=1) == row_ref[0, :, rows]
                here = q_ref[rows, :]
                done = []
                for half in range(2):
                    mine = jnp.where(head_lanes(half, here.shape), here * HD ** (-0.5), 0.0).astype(
                        jnp.bfloat16
                    )
                    raw = jnp.where(same, dot_dims(keys, mine, 1, 1), NEG)
                    peak = jnp.max(raw, axis=0, keepdims=True)
                    expo = jnp.exp(raw - peak)
                    total = jnp.sum(expo, axis=0, keepdims=True)
                    mixed = jnp.dot(
                        vt_ref[half * HD : (half + 1) * HD, pl.ds(begin, size)],
                        expo.astype(jnp.bfloat16),
                        preferred_element_type=jnp.float32,
                    )
                    done.append(mixed * (1.0 / total))
                    log_ref[0, half : half + 1, rows] = peak + jnp.log(total)
                ctx_ref[rows, :] = jnp.concatenate(done, axis=0).T.astype(jnp.bfloat16)


def attend(table, project, marks_col, marks_row, rows, length):
    pairs = HEADS * HD // LANES
    tile = min(TILE, length)
    sizes = windows_of(length)
    columns = lambda part: pl.BlockSpec((length, LANES), lambda i, j, t: (i, part * pairs + j))
    flops = 4 * rows * HEADS * length * length * HD
    return pl.pallas_call(
        functools.partial(attend_kernel, sizes, tile),
        out_shape=(
            jax.ShapeDtypeStruct((rows * length, D), jnp.bfloat16),
            jax.ShapeDtypeStruct((rows * pairs, 2, length), jnp.float32),
        ),
        grid_spec=pltpu.PrefetchScalarGridSpec(
            num_scalar_prefetch=1,
            grid=(rows, pairs),
            in_specs=[
                columns(0),
                columns(1),
                columns(2),
                pl.BlockSpec((length, LANES), lambda i, j, t: (i, 0)),
                pl.BlockSpec((1, 1, length), lambda i, j, t: (i, 0, 0)),
            ],
            out_specs=[
                pl.BlockSpec((length, LANES), lambda i, j, t: (i, j)),
                pl.BlockSpec((1, 2, length), lambda i, j, t: (i * pairs + j, 0, 0)),
            ],
            scratch_shapes=[pltpu.VMEM((LANES, length), jnp.bfloat16)],
        ),
        compiler_params=pltpu.CompilerParams(vmem_limit_bytes=VMEM_LIMIT),
        cost_estimate=pl.CostEstimate(
            flops=flops, bytes_accessed=8 * rows * length * D, transcendentals=rows * HEADS * length * length
        ),
        name="attend",
    )(table, project, project, project, marks_col, marks_row)


def attend_back_kernel(
    sizes, tile, table, q_ref, k_ref, v_ref, g_ref, col_ref, row_ref, log_ref, out_ref, kt_ref, dk_ref, dv_ref
):
    length = k_ref.shape[0]
    row = pl.program_id(0)
    kt_ref[...] = k_ref[...].astype(jnp.float32).T.astype(jnp.bfloat16)
    dk_ref[...] = jnp.zeros_like(dk_ref)
    dv_ref[...] = jnp.zeros_like(dv_ref)
    scale = HD ** (-0.5)

    @pl.loop(0, length // tile)
    def _(step):
        begin = pl.multiple_of(table[row, 2 * step], LANES)
        which = table[row, 2 * step + 1]
        rows = pl.ds(pl.multiple_of(step * tile, tile), tile)
        for number, size in enumerate(sizes):

            @pl.when(which == number)
            def _(size=size):
                window = pl.ds(begin, size)
                keys = k_ref[window, :]
                vals = v_ref[window, :]
                marks = col_ref[window, :]
                same = jnp.concatenate([marks] * (tile // LANES), axis=1) == row_ref[0, :, rows]
                here = q_ref[rows, :]
                grad = g_ref[rows, :]
                done = []
                for half in range(2):
                    lanes = head_lanes(half, here.shape)
                    mine = jnp.where(lanes, here * scale, 0.0).astype(jnp.bfloat16)
                    own = jnp.where(lanes, grad, 0.0).astype(jnp.bfloat16)
                    raw = jnp.where(same, dot_dims(keys, mine, 1, 1), NEG)
                    probs = jnp.exp(raw - log_ref[0, half : half + 1, rows])
                    d_probs = dot_dims(vals, own, 1, 1)
                    dv_ref[window, :] += jnp.dot(
                        probs.astype(jnp.bfloat16), own, preferred_element_type=jnp.float32
                    )
                    product = probs * d_probs
                    inner = jnp.sum(product, axis=0, keepdims=True)
                    d_scores = (product - probs * inner).astype(jnp.bfloat16)
                    dk_ref[window, :] += jnp.dot(d_scores, mine, preferred_element_type=jnp.float32)
                    done.append(
                        jnp.dot(
                            kt_ref[half * HD : (half + 1) * HD, window],
                            d_scores,
                            preferred_element_type=jnp.float32,
                        )
                    )
                out_ref[0, rows, :] = (jnp.concatenate(done, axis=0) * scale).T.astype(jnp.bfloat16)

    out_ref[1, :, :] = dk_ref[...].astype(jnp.bfloat16)
    out_ref[2, :, :] = dv_ref[...].astype(jnp.bfloat16)


def attend_back(table, project, grad, marks_col, marks_row, log_sum, rows, length):
    pairs = HEADS * HD // LANES
    tile = min(TILE, length)
    sizes = windows_of(length)
    columns = lambda part: pl.BlockSpec((length, LANES), lambda i, j, t: (i, part * pairs + j))
    flops = 10 * rows * HEADS * length * length * HD
    return pl.pallas_call(
        functools.partial(attend_back_kernel, sizes, tile),
        out_shape=jax.ShapeDtypeStruct((3, rows * length, D), jnp.bfloat16),
        grid_spec=pltpu.PrefetchScalarGridSpec(
            num_scalar_prefetch=1,
            grid=(rows, pairs),
            in_specs=[
                columns(0),
                columns(1),
                columns(2),
                columns(0),
                pl.BlockSpec((length, LANES), lambda i, j, t: (i, 0)),
                pl.BlockSpec((1, 1, length), lambda i, j, t: (i, 0, 0)),
                pl.BlockSpec((1, 2, length), lambda i, j, t: (i * pairs + j, 0, 0)),
            ],
            out_specs=pl.BlockSpec((3, length, LANES), lambda i, j, t: (0, i, j)),
            scratch_shapes=[
                pltpu.VMEM((LANES, length), jnp.bfloat16),
                pltpu.VMEM((length, LANES), jnp.float32),
                pltpu.VMEM((length, LANES), jnp.float32),
            ],
        ),
        compiler_params=pltpu.CompilerParams(vmem_limit_bytes=VMEM_LIMIT),
        cost_estimate=pl.CostEstimate(
            flops=flops, bytes_accessed=14 * rows * length * D, transcendentals=rows * HEADS * length * length
        ),
        name="attend_back",
    )(table, project, project, project, grad, marks_col, marks_row, log_sum)


def on_device(
    inputs,
    segments,
    cotangent,
    weights,
    first_moment,
    second_moment,
    bases,
    right_bases,
    small,
    small_first,
    small_second,
):
    number, quarter, width = inputs.shape
    length = segments.shape[1]
    groups = lax.axis_size("seq")
    owners = lax.axis_size("dp")
    place = lax.axis_index("seq")
    rows = -(-number // groups)
    padded = rows * groups
    tokens = rows * length
    block_widths = [3 * D // owners, D // owners, FF // owners, FF // owners]
    block_starts = [sum(block_widths[:which]) for which in range(4)]

    def blocks_of(matrix):
        return [
            matrix[block_starts[which] : block_starts[which] + block_widths[which]]
            for which in range(4)
        ]

    def to_rows(array):
        array = jnp.pad(array, ((0, padded - number), (0, 0), (0, 0)))
        moved = lax.all_to_all(array, "seq", split_axis=0, concat_axis=1, tiled=True)
        return moved.reshape(tokens, width)

    def to_quarters(array):
        array = array.reshape(rows, length, width)
        moved = lax.all_to_all(array, "seq", split_axis=1, concat_axis=0, tiled=True)
        return moved[:number]

    x = to_rows(inputs)
    pull = to_rows(cotangent)
    low = weights.astype(jnp.bfloat16).T
    w_qkv, w_out, w_up, w_down = [
        lax.all_gather(block, "dp", axis=0, tiled=True) for block in blocks_of(low)
    ]
    pieces = [small[index * D : (index + 1) * D] for index in range(8)] + [small[8 * D :]]
    (
        gain_one,
        gain_two,
        shift_one,
        shift_two,
        bias_query,
        bias_value,
        bias_out,
        bias_down,
        bias_up,
    ) = pieces

    filler = jnp.broadcast_to(
        (jnp.arange(length, dtype=jnp.int32) // TILE)[None], (padded - number, length)
    )
    marks = lax.dynamic_slice_in_dim(
        jnp.concatenate([segments, filler], axis=0), place * rows, rows, axis=0
    )
    table = key_windows(marks)
    marks_col = jnp.broadcast_to(marks.reshape(tokens, 1), (tokens, LANES))
    marks_row = marks.reshape(rows, 1, length)

    acts = x.astype(jnp.float32)
    bias_qkv = jnp.concatenate([bias_query, jnp.zeros_like(bias_query), bias_value])
    project = (dot_dims(x, w_qkv, 1, 1) + bias_qkv).astype(jnp.bfloat16)
    context, log_sum = attend(table, project, marks_col, marks_row, rows, length)
    attended = dot_dims(context, w_out, 1, 1) + bias_out
    first, scaled_one, inv_one = normalize(acts + attended, gain_one, shift_one)
    first_low = first.astype(jnp.bfloat16)
    upward = dot_dims(first_low, w_up, 1, 1) + bias_up
    active_full, gelu_pull = jax.vjp(lambda value: jax.nn.gelu(value, approximate=False), upward)
    active = active_full.astype(jnp.bfloat16)
    downward = dot_dims(active, w_down, 1, 0) + bias_down
    output, scaled_two, inv_two = normalize(first + downward, gain_two, shift_two)
    grad_out = pull.astype(jnp.float32)
    d_two = norm_back(grad_out, scaled_two, inv_two, gain_two)
    grad_gain_two = jnp.sum(grad_out * scaled_two, axis=0)
    grad_shift_two = jnp.sum(grad_out, axis=0)
    d_down = d_two.astype(jnp.bfloat16)
    grad_bias_down = jnp.sum(d_down.astype(jnp.float32), axis=0)
    grad_down = dot_dims(active, d_down, 0, 0).astype(jnp.bfloat16)
    d_active = dot_dims(d_down, w_down, 1, 1)
    (d_up_full,) = gelu_pull(d_active)
    d_up = d_up_full.astype(jnp.bfloat16)
    grad_bias_up = jnp.sum(d_up.astype(jnp.float32), axis=0)
    grad_up = dot_dims(d_up, first_low, 0, 0).astype(jnp.bfloat16)
    d_first = d_two + dot_dims(d_up, w_up, 1, 0)
    d_one = norm_back(d_first, scaled_one, inv_one, gain_one)
    grad_gain_one = jnp.sum(d_first * scaled_one, axis=0)
    grad_shift_one = jnp.sum(d_first, axis=0)
    d_att = d_one.astype(jnp.bfloat16)
    grad_bias_out = jnp.sum(d_att.astype(jnp.float32), axis=0)
    grad_outw = dot_dims(d_att, context, 0, 0).astype(jnp.bfloat16)
    d_context = dot_dims(d_att, w_out, 1, 0).astype(jnp.bfloat16)
    d_qkv = attend_back(table, project, d_context, marks_col, marks_row, log_sum, rows, length)
    grad_bias_query = jnp.sum(d_qkv[0].astype(jnp.float32), axis=0)
    grad_bias_value = jnp.sum(d_qkv[2].astype(jnp.float32), axis=0)
    grad_qkv = jnp.concatenate([dot_dims(d_qkv[part], x, 0, 0) for part in range(3)], axis=0).astype(
        jnp.bfloat16
    )
    input_grad = d_one
    for part in range(3):
        input_grad = input_grad + dot_dims(d_qkv[part], w_qkv[part * D : (part + 1) * D], 1, 0)
    input_grad = to_quarters(input_grad.astype(jnp.bfloat16))
    output = to_quarters(output.astype(jnp.bfloat16))

    small_local = jnp.concatenate(
        [
            grad_gain_one,
            grad_gain_two,
            grad_shift_one,
            grad_shift_two,
            grad_bias_query,
            grad_bias_value,
            grad_bias_out,
            grad_bias_down,
            grad_bias_up,
        ]
    )
    small_grad = lax.psum(small_local, ("dp", "seq"))

    grads = [grad_qkv, grad_outw, grad_up, grad_down]
    mine = jnp.concatenate(
        [lax.psum_scatter(grad, "dp", scatter_dimension=0, tiled=True) for grad in grads], axis=0
    )
    mine = lax.psum(mine, "seq")
    reduced = mine.T.astype(jnp.float32)
    bases_low = bases.astype(jnp.bfloat16)
    rights = [
        right_bases[
            block_starts[which] : block_starts[which] + block_widths[which],
            : owners * block_widths[which],
        ].astype(jnp.bfloat16)
        for which in range(4)
    ]
    rotated = []
    for which, block in enumerate(blocks_of(mine)):
        turned = dot_dims(block, bases_low[which], 1, 0).astype(jnp.bfloat16)
        term = dot_dims(rights[which], turned, 0, 0).astype(jnp.bfloat16)
        rotated.append(lax.psum_scatter(term, "dp", scatter_dimension=0, tiled=True))
    rotated = jnp.concatenate(rotated, axis=0).T.astype(jnp.float32)
    first_new, second_new, heading = moments(rotated, first_moment, second_moment)
    heading = heading.astype(jnp.bfloat16)
    update = []
    for which in range(4):
        block = heading[:, block_starts[which] : block_starts[which] + block_widths[which]]
        step = dot_dims(block, bases_low[which], 0, 1).astype(jnp.bfloat16)
        every = lax.all_gather(step, "dp", axis=0, tiled=True)
        update.append(dot_dims(every, rights[which], 0, 1))
    weights_new = weights - learn_rate * jnp.concatenate(update, axis=1)
    small_first_new, small_second_new, small_heading = moments(
        small_grad, small_first, small_second
    )
    small_new = small - small_rate * small_heading
    return (
        output,
        input_grad,
        reduced,
        first_new,
        second_new,
        weights_new,
        weights_new.astype(jnp.bfloat16),
        small_grad,
        small_first_new,
        small_second_new,
        small_new,
    )


def solution(mesh):
    return jax.shard_map(
        on_device,
        mesh=mesh,
        in_specs=(
            P("dp", "seq", None),
            P("dp", None),
            P("dp", "seq", None),
            P(None, "dp"),
            P(None, "dp"),
            P(None, "dp"),
            P(),
            P("dp", None),
            P(),
            P(),
            P(),
        ),
        out_specs=(
            P("dp", "seq", None),
            P("dp", "seq", None),
            P(None, "dp"),
            P(None, "dp"),
            P(None, "dp"),
            P(None, "dp"),
            P(None, "dp"),
            P(),
            P(),
            P(),
            P(),
        ),
        check_vma=False,
    )
```

```python
import functools
import math

import jax
import jax.numpy as jnp
from jax import lax
from jax.experimental import pallas as pl
from jax.experimental.pallas import tpu as pltpu
from jax.sharding import PartitionSpec as P

D = 768
HEADS = 12
HD = 64
FF = 3072
STEP = 10


norm_eps = 1e-12
beta_first = 0.9
beta_second = 0.999
adam_eps = 1e-08
learn_rate = 0.03
small_rate = 0.3

TILE = 256
LANES = 128
WINDOWS = (256, 512, 640, 768, 1024)
NEG = -1e30
VMEM_LIMIT = 60 * 1024 * 1024


def dot_dims(left, right, left_dim, right_dim):
    return lax.dot_general(
        left, right, (((left_dim,), (right_dim,)), ((), ())), preferred_element_type=jnp.float32
    )


def normalize(resid, gain, shift):
    centre = resid - jnp.mean(resid, axis=-1, keepdims=True)
    spread = jnp.mean(centre * centre, axis=-1, keepdims=True)
    inv_std = lax.rsqrt(spread + norm_eps)
    scaled = centre * inv_std
    return (scaled * gain + shift, scaled, inv_std)


def norm_back(grad, scaled, inv_std, gain):
    lifted = grad * gain
    return inv_std * (
        lifted
        - jnp.mean(lifted, axis=-1, keepdims=True)
        - scaled * jnp.mean(lifted * scaled, axis=-1, keepdims=True)
    )


def moments(grad, first, second):
    first_out = beta_first * first + (1.0 - beta_first) * grad
    second_out = beta_second * second + (1.0 - beta_second) * grad * grad
    heading = (
        first_out
        / (1.0 - beta_first**STEP)
        / (jnp.sqrt(second_out / (1.0 - beta_second**STEP)) + adam_eps)
    )
    return (first_out, second_out, heading)


def windows_of(length):
    return tuple(size for size in WINDOWS if size < length) + (length,)


def key_windows(marks):
    rows, length = marks.shape
    tile = min(TILE, length)
    sizes = windows_of(length)
    heads = marks[:, ::tile]
    tails = marks[:, tile - 1 :: tile]
    low = jnp.sum((marks[:, None, :] < heads[:, :, None]).astype(jnp.int32), axis=-1)
    high = jnp.sum((marks[:, None, :] <= tails[:, :, None]).astype(jnp.int32), axis=-1)
    begin = low // LANES * LANES
    need = high - begin
    which = jnp.zeros_like(need)
    for size in sizes[:-1]:
        which = which + (need > size).astype(jnp.int32)
    width = jnp.asarray(sizes, jnp.int32)[which]
    begin = jnp.minimum(begin, length - width)
    return jnp.stack([begin, which], axis=-1).reshape(rows, -1)


def head_lanes(half, shape):
    lane = lax.broadcasted_iota(jnp.int32, shape, 1)
    return (lane >= half * HD) & (lane < (half + 1) * HD)


def attend_kernel(sizes, tile, table, q_ref, k_ref, v_ref, col_ref, row_ref, ctx_ref, log_ref, vt_ref):
    length = k_ref.shape[0]
    row = pl.program_id(0)
    vt_ref[...] = v_ref[...].astype(jnp.float32).T.astype(jnp.bfloat16)

    @pl.loop(0, length // tile)
    def _(step):
        begin = pl.multiple_of(table[row, 2 * step], LANES)
        which = table[row, 2 * step + 1]
        rows = pl.ds(pl.multiple_of(step * tile, tile), tile)
        for number, size in enumerate(sizes):

            @pl.when(which == number)
            def _(size=size):
                keys = k_ref[pl.ds(begin, size), :]
                marks = col_ref[pl.ds(begin, size), :]
                same = jnp.concatenate([marks] * (tile // LANES), axis=1) == row_ref[0, :, rows]
                here = q_ref[rows, :]
                done = []
                for half in range(2):
                    mine = jnp.where(head_lanes(half, here.shape), here * HD ** (-0.5), 0.0).astype(
                        jnp.bfloat16
                    )
                    raw = jnp.where(same, dot_dims(keys, mine, 1, 1), NEG)
                    peak = jnp.max(raw, axis=0, keepdims=True)
                    expo = jnp.exp(raw - peak)
                    total = jnp.sum(expo, axis=0, keepdims=True)
                    mixed = jnp.dot(
                        vt_ref[half * HD : (half + 1) * HD, pl.ds(begin, size)],
                        expo.astype(jnp.bfloat16),
                        preferred_element_type=jnp.float32,
                    )
                    done.append(mixed * (1.0 / total))
                    log_ref[0, half : half + 1, rows] = peak + jnp.log(total)
                ctx_ref[rows, :] = jnp.concatenate(done, axis=0).T.astype(jnp.bfloat16)


def attend(table, project, marks_col, marks_row, rows, length):
    pairs = HEADS * HD // LANES
    tile = min(TILE, length)
    sizes = windows_of(length)
    columns = lambda part: pl.BlockSpec((length, LANES), lambda i, j, t: (i, part * pairs + j))
    flops = 4 * rows * HEADS * length * length * HD
    return pl.pallas_call(
        functools.partial(attend_kernel, sizes, tile),
        out_shape=(
            jax.ShapeDtypeStruct((rows * length, D), jnp.bfloat16),
            jax.ShapeDtypeStruct((rows * pairs, 2, length), jnp.float32),
        ),
        grid_spec=pltpu.PrefetchScalarGridSpec(
            num_scalar_prefetch=1,
            grid=(rows, pairs),
            in_specs=[
                columns(0),
                columns(1),
                columns(2),
                pl.BlockSpec((length, LANES), lambda i, j, t: (i, 0)),
                pl.BlockSpec((1, 1, length), lambda i, j, t: (i, 0, 0)),
            ],
            out_specs=[
                pl.BlockSpec((length, LANES), lambda i, j, t: (i, j)),
                pl.BlockSpec((1, 2, length), lambda i, j, t: (i * pairs + j, 0, 0)),
            ],
            scratch_shapes=[pltpu.VMEM((LANES, length), jnp.bfloat16)],
        ),
        compiler_params=pltpu.CompilerParams(vmem_limit_bytes=VMEM_LIMIT),
        cost_estimate=pl.CostEstimate(
            flops=flops, bytes_accessed=8 * rows * length * D, transcendentals=rows * HEADS * length * length
        ),
        name="attend",
    )(table, project, project, project, marks_col, marks_row)


def attend_back_kernel(
    sizes, tile, table, q_ref, k_ref, v_ref, g_ref, col_ref, row_ref, log_ref, out_ref, kt_ref, dk_ref, dv_ref
):
    length = k_ref.shape[0]
    row = pl.program_id(0)
    kt_ref[...] = k_ref[...].astype(jnp.float32).T.astype(jnp.bfloat16)
    dk_ref[...] = jnp.zeros_like(dk_ref)
    dv_ref[...] = jnp.zeros_like(dv_ref)
    scale = HD ** (-0.5)

    @pl.loop(0, length // tile)
    def _(step):
        begin = pl.multiple_of(table[row, 2 * step], LANES)
        which = table[row, 2 * step + 1]
        rows = pl.ds(pl.multiple_of(step * tile, tile), tile)
        for number, size in enumerate(sizes):

            @pl.when(which == number)
            def _(size=size):
                window = pl.ds(begin, size)
                keys = k_ref[window, :]
                vals = v_ref[window, :]
                marks = col_ref[window, :]
                same = jnp.concatenate([marks] * (tile // LANES), axis=1) == row_ref[0, :, rows]
                here = q_ref[rows, :]
                grad = g_ref[rows, :]
                done = []
                for half in range(2):
                    lanes = head_lanes(half, here.shape)
                    mine = jnp.where(lanes, here * scale, 0.0).astype(jnp.bfloat16)
                    own = jnp.where(lanes, grad, 0.0).astype(jnp.bfloat16)
                    raw = jnp.where(same, dot_dims(keys, mine, 1, 1), NEG)
                    probs = jnp.exp(raw - log_ref[0, half : half + 1, rows])
                    d_probs = dot_dims(vals, own, 1, 1)
                    dv_ref[window, :] += jnp.dot(
                        probs.astype(jnp.bfloat16), own, preferred_element_type=jnp.float32
                    )
                    product = probs * d_probs
                    inner = jnp.sum(product, axis=0, keepdims=True)
                    d_scores = (product - probs * inner).astype(jnp.bfloat16)
                    dk_ref[window, :] += jnp.dot(d_scores, mine, preferred_element_type=jnp.float32)
                    done.append(
                        jnp.dot(
                            kt_ref[half * HD : (half + 1) * HD, window],
                            d_scores,
                            preferred_element_type=jnp.float32,
                        )
                    )
                out_ref[0, rows, :] = (jnp.concatenate(done, axis=0) * scale).T.astype(jnp.bfloat16)

    out_ref[1, :, :] = dk_ref[...].astype(jnp.bfloat16)
    out_ref[2, :, :] = dv_ref[...].astype(jnp.bfloat16)


def attend_back(table, project, grad, marks_col, marks_row, log_sum, rows, length):
    pairs = HEADS * HD // LANES
    tile = min(TILE, length)
    sizes = windows_of(length)
    columns = lambda part: pl.BlockSpec((length, LANES), lambda i, j, t: (i, part * pairs + j))
    flops = 10 * rows * HEADS * length * length * HD
    return pl.pallas_call(
        functools.partial(attend_back_kernel, sizes, tile),
        out_shape=jax.ShapeDtypeStruct((3, rows * length, D), jnp.bfloat16),
        grid_spec=pltpu.PrefetchScalarGridSpec(
            num_scalar_prefetch=1,
            grid=(rows, pairs),
            in_specs=[
                columns(0),
                columns(1),
                columns(2),
                columns(0),
                pl.BlockSpec((length, LANES), lambda i, j, t: (i, 0)),
                pl.BlockSpec((1, 1, length), lambda i, j, t: (i, 0, 0)),
                pl.BlockSpec((1, 2, length), lambda i, j, t: (i * pairs + j, 0, 0)),
            ],
            out_specs=pl.BlockSpec((3, length, LANES), lambda i, j, t: (0, i, j)),
            scratch_shapes=[
                pltpu.VMEM((LANES, length), jnp.bfloat16),
                pltpu.VMEM((length, LANES), jnp.float32),
                pltpu.VMEM((length, LANES), jnp.float32),
            ],
        ),
        compiler_params=pltpu.CompilerParams(vmem_limit_bytes=VMEM_LIMIT),
        cost_estimate=pl.CostEstimate(
            flops=flops, bytes_accessed=14 * rows * length * D, transcendentals=rows * HEADS * length * length
        ),
        name="attend_back",
    )(table, project, project, project, grad, marks_col, marks_row, log_sum)


MESH = pl.DeviceIdType.MESH
ROWS = 48


def partners(me):
    core, along_x, along_y = me % 2, (me // 2) % 2, me // 4
    side_x = me + 2 - 4 * along_x
    return (me + 1 - 2 * core, side_x, me + 4 - 8 * along_y, side_x + 4 - 8 * along_y)


def send(source, target, send_sem, recv_sem, axis, place):
    return pltpu.make_async_remote_copy(
        src_ref=source,
        dst_ref=target,
        send_sem=send_sem,
        recv_sem=recv_sem,
        device_id={axis: place},
        device_id_type=MESH,
    )


def greet(peers):
    barrier = pltpu.get_barrier_semaphore()
    for axis, place in peers:
        pl.semaphore_signal(barrier, inc=1, device_id={axis: place}, device_id_type=MESH)
    pl.semaphore_wait(barrier, len(peers))


def owner_rows(owner, width, part):
    begin = pl.multiple_of(owner * width, 16)
    if part is None:
        return pl.ds(begin, width)
    return pl.ds(pl.multiple_of(begin + part * (width // 2), 16), width // 2)


def gather_kernel(widths, starts, shard_ref, *refs):
    count = len(widths)
    outs = refs[:count]
    send_sem, recv_sem, own_sem = refs[count:]
    me = lax.axis_index("dp")
    sib, side_x, side_y, across = partners(me)
    _, sib_x, sib_y, sib_across = partners(sib)
    greet([("dp", sib), ("dp", side_x), ("dp", side_y)])
    arrivals = [
        (side_x, None),
        (side_y, None),
        (across, 0),
        (across, 1),
        (sib, None),
        (sib_x, None),
        (sib_y, None),
        (sib_across, 0),
        (sib_across, 1),
    ]
    sent = []

    def put(block, kind, slot, source, owner, part, place):
        copy = send(
            source,
            outs[block].at[owner_rows(owner, widths[block], part)],
            send_sem.at[block, slot],
            recv_sem.at[block, kind],
            "dp",
            place,
        )
        copy.start()
        sent.append(copy)

    def arrived(block, kind):
        owner, part = arrivals[kind]
        region = outs[block].at[owner_rows(owner, widths[block], part)]
        send(region, region, send_sem.at[block, 0], recv_sem.at[block, kind], "dp", sib).wait_recv()

    def forward(block, kind, slot, owner, part, place):
        region = outs[block].at[owner_rows(owner, widths[block], part)]
        put(block, kind, slot, region, owner, part, place)

    kept = []
    for block in range(count):
        mine = shard_ref.at[pl.ds(starts[block], widths[block])]
        put(block, 0, 0, mine, me, None, side_x)
        put(block, 1, 1, mine, me, None, side_y)
        put(block, 4, 2, mine, me, None, sib)
        copy = pltpu.make_async_copy(
            mine, outs[block].at[owner_rows(me, widths[block], None)], own_sem.at[block]
        )
        copy.start()
        kept.append(copy)
    for step in range(count + 1):
        if step < count:
            arrived(step, 0)
            forward(step, 2, 3, side_x, 0, side_y)
            forward(step, 5, 4, side_x, None, sib)
            arrived(step, 1)
            forward(step, 3, 5, side_y, 1, side_x)
            forward(step, 6, 6, side_y, None, sib)
        if step > 0:
            arrived(step - 1, 2)
            forward(step - 1, 7, 7, across, 0, sib)
            arrived(step - 1, 3)
            forward(step - 1, 8, 8, across, 1, sib)
    for block in range(count):
        for kind in range(4, 9):
            arrived(block, kind)
    for copy in sent:
        copy.wait_send()
    for copy in kept:
        copy.wait()


def plane_gather(shard, widths, starts):
    count = len(widths)
    depth = shard.shape[1]
    return pl.pallas_call(
        functools.partial(gather_kernel, widths, starts),
        out_shape=tuple(jax.ShapeDtypeStruct((8 * width, depth), shard.dtype) for width in widths),
        in_specs=[pl.BlockSpec(memory_space=pltpu.VMEM)],
        out_specs=tuple(pl.BlockSpec(memory_space=pl.ANY) for _ in widths),
        scratch_shapes=[
            pltpu.SemaphoreType.DMA((count, 9)),
            pltpu.SemaphoreType.DMA((count, 9)),
            pltpu.SemaphoreType.DMA((count,)),
        ],
        compiler_params=pltpu.CompilerParams(
            collective_id=1, has_side_effects=True, vmem_limit_bytes=16 * 1024 * 1024
        ),
        cost_estimate=pl.CostEstimate(
            flops=0, bytes_accessed=8 * 16 * shard.shape[0] * depth, transcendentals=0
        ),
        name="plane_gather",
    )(shard)


def add_rows(target, target_at, terms, count):
    def step(number, carry):
        offset = pl.multiple_of(number * ROWS, 16)
        total = None
        for ref, begin in terms:
            value = ref[pl.ds(begin + offset, ROWS), :].astype(jnp.float32)
            total = value if total is None else total + value
        target[pl.ds(target_at + offset, ROWS), :] = total.astype(target.dtype)
        return carry

    lax.fori_loop(0, count // ROWS, step, 0)


def reduce_kernel(widths, starts, across_planes, *refs):
    count = len(widths)
    share = sum(widths)
    blocks = refs[:count]
    refs = refs[count:]
    if across_planes:
        small_ref, out_ref, small_out = refs[:3]
        refs = refs[3:]
    else:
        out_ref = refs[0]
        refs = refs[1:]
    own, given, from_x, from_y, turn_x, turn_y, total = refs[:7]
    load_sem, sib_send, sib_recv, link_send, link_recv, out_sem = refs[7:13]
    refs = refs[13:]
    if across_planes:
        low_first, high_first, low_second, final, z_send, z_recv = refs[:6]
        small_all, small_planes, small_sum, small_send, small_recv, wide_send, wide_recv = refs[6:]
    me = lax.axis_index("dp")
    plane = lax.axis_index("seq")
    sib, side_x, side_y, across = partners(me)
    _, sib_x, sib_y, sib_across = partners(sib)
    owners = (me, side_x, side_y, across)
    sib_owners = (sib, sib_x, sib_y, sib_across)
    if across_planes:
        others = [(me + step) % 8 for step in range(1, 8)]
        planes = [(plane + step) % 4 for step in range(1, 4)]
        greet([("dp", place) for place in others] + [("seq", place) for place in planes])
    else:
        greet([("dp", sib), ("dp", side_x), ("dp", side_y)])
    order = (3, 1, 2, 0)
    loads, sends = {}, []
    for block in range(count):
        width = widths[block]
        here = pl.ds(starts[block], width)
        for which in order:
            copy = send(
                blocks[block].at[owner_rows(sib_owners[which], width, None)],
                given.at[which, here],
                sib_send.at[block, which],
                sib_recv.at[block, which],
                "dp",
                sib,
            )
            copy.start()
            sends.append(copy)
            load = pltpu.make_async_copy(
                blocks[block].at[owner_rows(owners[which], width, None)],
                own.at[which, here],
                load_sem.at[block, which],
            )
            load.start()
            loads[block, which] = (load, copy)
    if across_planes:
        small_all[me] = small_ref[...]
        for number, place in enumerate(others):
            copy = send(
                small_ref, small_all.at[me], small_send.at[number], small_recv.at[me], "dp", place
            )
            copy.start()
            sends.append(copy)

    def link(block, slot, source, target, place):
        copy = send(source, target, link_send.at[block, slot], link_recv.at[block, slot], "dp", place)
        copy.start()
        sends.append(copy)

    def landed(block, slot, region):
        send(region, region, link_send.at[block, slot], link_recv.at[block, slot], "dp", sib).wait_recv()

    def upper(block):
        return (starts[block], widths[block] // 2)

    def lower(block):
        return (starts[block] + widths[block] // 2, widths[block] // 2)

    def rows_of(part):
        return pl.ds(part[0], part[1])

    def half_of(block):
        return pl.ds(starts[block] // 2, widths[block] // 2)

    def pair_sum(block, which):
        load, copy = loads[block, which]
        load.wait()
        copy.wait_recv()
        add_rows(
            own.at[which],
            starts[block],
            [(own.at[which], starts[block]), (given.at[which], starts[block])],
            widths[block],
        )

    def first_stage(block):
        pair_sum(block, 3)
        link(block, 0, own.at[3, rows_of(upper(block))], turn_x.at[half_of(block)], side_x)
        link(block, 1, own.at[3, rows_of(lower(block))], turn_y.at[half_of(block)], side_y)
        pair_sum(block, 1)
        link(
            block, 2, own.at[1, rows_of(upper(block))], from_x.at[rows_of(upper(block))], side_x
        )
        pair_sum(block, 2)
        link(
            block, 3, own.at[2, rows_of(lower(block))], from_y.at[rows_of(lower(block))], side_y
        )
        pair_sum(block, 0)

    def second_stage(block):
        landed(block, 0, turn_x.at[half_of(block)])
        begin, size = upper(block)
        add_rows(own.at[2], begin, [(own.at[2], begin), (turn_x, starts[block] // 2)], size)
        link(block, 4, own.at[2, rows_of(upper(block))], from_y.at[rows_of(upper(block))], side_y)
        landed(block, 1, turn_y.at[half_of(block)])
        begin, size = lower(block)
        add_rows(own.at[1], begin, [(own.at[1], begin), (turn_y, starts[block] // 2)], size)
        link(block, 5, own.at[1, rows_of(lower(block))], from_x.at[rows_of(lower(block))], side_x)

    def third_stage(block):
        landed(block, 2, from_x.at[rows_of(upper(block))])
        landed(block, 5, from_x.at[rows_of(lower(block))])
        landed(block, 3, from_y.at[rows_of(lower(block))])
        landed(block, 4, from_y.at[rows_of(upper(block))])
        begin = starts[block]
        add_rows(total, begin, [(own.at[0], begin), (from_x, begin), (from_y, begin)], widths[block])

    stages = [first_stage, second_stage, third_stage]
    results = total
    if across_planes:
        results = final

        def z_copy(block, slot, source, target, place):
            return send(source, target, z_send.at[block, slot], z_recv.at[block, slot], "seq", place)

        def z_put(block, slot, source, target, place):
            copy = z_copy(block, slot, source, target, place)
            copy.start()
            return copy

        def z_landed(block, slot, region):
            z_copy(block, slot, region, region, (plane + 1) % 4).wait_recv()

        def fourth_stage(block):
            up, down, half = rows_of(upper(block)), rows_of(lower(block)), half_of(block)

            @pl.when(plane == 0)
            def _():
                z_put(block, 0, total.at[up], low_first.at[half], 1)
                z_put(block, 1, total.at[down], low_second.at[half], 1)

            @pl.when(plane == 2)
            def _():
                z_put(block, 2, total.at[up], high_first.at[half], 1)

        def fifth_stage(block):
            up, down, half = rows_of(upper(block)), rows_of(lower(block)), half_of(block)
            middle = starts[block] // 2

            @pl.when(plane == 1)
            def _():
                z_landed(block, 0, low_first.at[half])
                z_landed(block, 2, high_first.at[half])
                begin, size = upper(block)
                add_rows(
                    final, begin, [(total, begin), (low_first, middle), (high_first, middle)], size
                )
                z_put(block, 3, final.at[up], final.at[up], 0)
                z_put(block, 4, final.at[up], final.at[up], 2)
                z_landed(block, 1, low_second.at[half])
                begin, size = lower(block)
                add_rows(total, begin, [(total, begin), (low_second, middle)], size)
                z_put(block, 5, total.at[down], low_second.at[half], 2)

        def sixth_stage(block):
            up, down, half = rows_of(upper(block)), rows_of(lower(block)), half_of(block)
            middle = starts[block] // 2

            @pl.when(plane == 2)
            def _():
                z_landed(block, 5, low_second.at[half])
                begin, size = lower(block)
                add_rows(final, begin, [(total, begin), (low_second, middle)], size)
                z_put(block, 6, final.at[down], final.at[down], 1)
                z_put(block, 7, final.at[down], final.at[down], 3)
                z_landed(block, 4, final.at[up])
                z_put(block, 8, final.at[up], final.at[up], 3)

        def seventh_stage(block):
            down = rows_of(lower(block))

            @pl.when(plane == 1)
            def _():
                z_landed(block, 6, final.at[down])
                z_put(block, 9, final.at[down], final.at[down], 0)

        def eighth_stage(block):
            up, down, half = rows_of(upper(block)), rows_of(lower(block)), half_of(block)

            @pl.when(plane == 0)
            def _():
                z_landed(block, 3, final.at[up])
                z_landed(block, 9, final.at[down])
                z_copy(block, 0, total.at[up], low_first.at[half], 1).wait_send()
                z_copy(block, 1, total.at[down], low_second.at[half], 1).wait_send()

            @pl.when(plane == 1)
            def _():
                z_copy(block, 3, final.at[up], final.at[up], 0).wait_send()
                z_copy(block, 4, final.at[up], final.at[up], 2).wait_send()
                z_copy(block, 5, total.at[down], low_second.at[half], 2).wait_send()
                z_copy(block, 9, final.at[down], final.at[down], 0).wait_send()

            @pl.when(plane == 2)
            def _():
                z_copy(block, 2, total.at[up], high_first.at[half], 1).wait_send()
                z_copy(block, 6, final.at[down], final.at[down], 1).wait_send()
                z_copy(block, 7, final.at[down], final.at[down], 3).wait_send()
                z_copy(block, 8, final.at[up], final.at[up], 3).wait_send()

            @pl.when(plane == 3)
            def _():
                z_landed(block, 7, final.at[down])
                z_landed(block, 8, final.at[up])

        stages += [fourth_stage, fifth_stage, sixth_stage, seventh_stage, eighth_stage]

    outgoing = []

    def last_stage(block):
        here = pl.ds(starts[block], widths[block])
        copy = pltpu.make_async_copy(results.at[here], out_ref.at[here], out_sem.at[block])
        copy.start()
        outgoing.append(copy)

    stages.append(last_stage)

    def small_first():
        for place in others:
            send(
                small_ref, small_all.at[place], small_send.at[0], small_recv.at[place], "dp", sib
            ).wait_recv()
        total_small = small_all[0]
        for number in range(1, 8):
            total_small = total_small + small_all[number]
        small_sum[...] = total_small
        small_planes[plane] = total_small
        for number, place in enumerate(planes):
            copy = send(
                small_sum, small_planes.at[plane], wide_send.at[number], wide_recv.at[plane], "seq", place
            )
            copy.start()
            sends.append(copy)

    def small_second():
        for place in planes:
            send(
                small_sum, small_planes.at[place], wide_send.at[0], wide_recv.at[place], "seq", place
            ).wait_recv()
        small_out[...] = (small_planes[0] + small_planes[1]) + (small_planes[2] + small_planes[3])

    for tick in range(count + len(stages) - 1):
        for number in range(len(stages) - 1, -1, -1):
            block = tick - number
            if 0 <= block < count:
                stages[number](block)
        if across_planes and tick == 1:
            small_first()
    if across_planes:
        small_second()
    for copy in sends:
        copy.wait_send()
    for copy in outgoing:
        copy.wait()


def plane_reduce(terms, widths, starts, small=None):
    count = len(widths)
    share = sum(widths)
    depth = terms[0].shape[1]
    across_planes = small is not None
    low = terms[0].dtype
    whole = pltpu.VMEM((share, depth), low)
    half = pltpu.VMEM((share // 2, depth), low)
    dma = pltpu.SemaphoreType.DMA
    scratch = [
        pltpu.VMEM((4, share, depth), low),
        pltpu.VMEM((4, share, depth), low),
        whole,
        whole,
        half,
        half,
        whole,
        dma((count, 4)),
        dma((count, 4)),
        dma((count, 4)),
        dma((count, 6)),
        dma((count, 6)),
        dma((count,)),
    ]
    any_spec = pl.BlockSpec(memory_space=pl.ANY)
    vmem_spec = pl.BlockSpec(memory_space=pltpu.VMEM)
    out_shape = [jax.ShapeDtypeStruct((share, depth), low)]
    in_specs = [any_spec] * count
    out_specs = [any_spec]
    operands = list(terms)
    if across_planes:
        scratch += [
            half,
            half,
            half,
            whole,
            dma((count, 10)),
            dma((count, 10)),
            pltpu.VMEM((8,) + small.shape, small.dtype),
            pltpu.VMEM((4,) + small.shape, small.dtype),
            pltpu.VMEM(small.shape, small.dtype),
            dma((7,)),
            dma((8,)),
            dma((3,)),
            dma((4,)),
        ]
        operands.append(small)
        in_specs.append(vmem_spec)
        out_specs.append(vmem_spec)
        out_shape.append(jax.ShapeDtypeStruct(small.shape, small.dtype))
    return pl.pallas_call(
        functools.partial(reduce_kernel, widths, starts, across_planes),
        out_shape=tuple(out_shape),
        in_specs=in_specs,
        out_specs=tuple(out_specs),
        scratch_shapes=scratch,
        compiler_params=pltpu.CompilerParams(
            collective_id=2 if across_planes else 3,
            has_side_effects=True,
            vmem_limit_bytes=48 * 1024 * 1024,
        ),
        cost_estimate=pl.CostEstimate(
            flops=0, bytes_accessed=8 * 20 * share * depth, transcendentals=0
        ),
        name="reduce_all" if across_planes else "plane_reduce",
    )(*operands)


def on_device(
    inputs,
    segments,
    cotangent,
    weights,
    first_moment,
    second_moment,
    bases,
    right_bases,
    small,
    small_first,
    small_second,
):
    number, quarter, width = inputs.shape
    length = segments.shape[1]
    groups = lax.axis_size("seq")
    owners = lax.axis_size("dp")
    place = lax.axis_index("seq")
    rows = -(-number // groups)
    padded = rows * groups
    tokens = rows * length
    block_widths = [3 * D // owners, D // owners, FF // owners, FF // owners]
    block_starts = [sum(block_widths[:which]) for which in range(4)]

    def blocks_of(matrix):
        return [
            matrix[block_starts[which] : block_starts[which] + block_widths[which]]
            for which in range(4)
        ]

    def to_rows(array):
        array = jnp.pad(array, ((0, padded - number), (0, 0), (0, 0)))
        moved = lax.all_to_all(array, "seq", split_axis=0, concat_axis=1, tiled=True)
        return moved.reshape(tokens, width)

    def to_quarters(array):
        array = array.reshape(rows, length, width)
        moved = lax.all_to_all(array, "seq", split_axis=1, concat_axis=0, tiled=True)
        return moved[:number]

    x = to_rows(inputs)
    pull = to_rows(cotangent)
    on_plane = owners == 8 and groups == 4 and number == 3

    def gather_blocks(matrix):
        if on_plane:
            return plane_gather(matrix, block_widths, block_starts)
        return [lax.all_gather(block, "dp", axis=0, tiled=True) for block in blocks_of(matrix)]

    def scatter_blocks(terms):
        if on_plane:
            return plane_reduce(terms, block_widths, block_starts)[0]
        return jnp.concatenate(
            [lax.psum_scatter(term, "dp", scatter_dimension=0, tiled=True) for term in terms], axis=0
        )

    w_qkv, w_out, w_up, w_down = gather_blocks(weights.astype(jnp.bfloat16).T)
    pieces = [small[index * D : (index + 1) * D] for index in range(8)] + [small[8 * D :]]
    (
        gain_one,
        gain_two,
        shift_one,
        shift_two,
        bias_query,
        bias_value,
        bias_out,
        bias_down,
        bias_up,
    ) = pieces

    filler = jnp.broadcast_to(
        (jnp.arange(length, dtype=jnp.int32) // TILE)[None], (padded - number, length)
    )
    marks = lax.dynamic_slice_in_dim(
        jnp.concatenate([segments, filler], axis=0), place * rows, rows, axis=0
    )
    table = key_windows(marks)
    marks_col = jnp.broadcast_to(marks.reshape(tokens, 1), (tokens, LANES))
    marks_row = marks.reshape(rows, 1, length)

    acts = x.astype(jnp.float32)
    bias_qkv = jnp.concatenate([bias_query, jnp.zeros_like(bias_query), bias_value])
    project = (dot_dims(x, w_qkv, 1, 1) + bias_qkv).astype(jnp.bfloat16)
    context, log_sum = attend(table, project, marks_col, marks_row, rows, length)
    attended = dot_dims(context, w_out, 1, 1) + bias_out
    first, scaled_one, inv_one = normalize(acts + attended, gain_one, shift_one)
    first_low = first.astype(jnp.bfloat16)
    upward = dot_dims(first_low, w_up, 1, 1) + bias_up
    active_full, gelu_pull = jax.vjp(lambda value: jax.nn.gelu(value, approximate=False), upward)
    active = active_full.astype(jnp.bfloat16)
    downward = dot_dims(active, w_down, 1, 0) + bias_down
    output, scaled_two, inv_two = normalize(first + downward, gain_two, shift_two)
    grad_out = pull.astype(jnp.float32)
    d_two = norm_back(grad_out, scaled_two, inv_two, gain_two)
    grad_gain_two = jnp.sum(grad_out * scaled_two, axis=0)
    grad_shift_two = jnp.sum(grad_out, axis=0)
    d_down = d_two.astype(jnp.bfloat16)
    grad_bias_down = jnp.sum(d_down.astype(jnp.float32), axis=0)
    grad_down = dot_dims(active, d_down, 0, 0).astype(jnp.bfloat16)
    d_active = dot_dims(d_down, w_down, 1, 1)
    (d_up_full,) = gelu_pull(d_active)
    d_up = d_up_full.astype(jnp.bfloat16)
    grad_bias_up = jnp.sum(d_up.astype(jnp.float32), axis=0)
    grad_up = dot_dims(d_up, first_low, 0, 0).astype(jnp.bfloat16)
    d_first = d_two + dot_dims(d_up, w_up, 1, 0)
    d_one = norm_back(d_first, scaled_one, inv_one, gain_one)
    grad_gain_one = jnp.sum(d_first * scaled_one, axis=0)
    grad_shift_one = jnp.sum(d_first, axis=0)
    d_att = d_one.astype(jnp.bfloat16)
    grad_bias_out = jnp.sum(d_att.astype(jnp.float32), axis=0)
    grad_outw = dot_dims(d_att, context, 0, 0).astype(jnp.bfloat16)
    d_context = dot_dims(d_att, w_out, 1, 0).astype(jnp.bfloat16)
    d_qkv = attend_back(table, project, d_context, marks_col, marks_row, log_sum, rows, length)
    grad_bias_query = jnp.sum(d_qkv[0].astype(jnp.float32), axis=0)
    grad_bias_value = jnp.sum(d_qkv[2].astype(jnp.float32), axis=0)
    grad_qkv = jnp.concatenate([dot_dims(d_qkv[part], x, 0, 0) for part in range(3)], axis=0).astype(
        jnp.bfloat16
    )
    input_grad = d_one
    for part in range(3):
        input_grad = input_grad + dot_dims(d_qkv[part], w_qkv[part * D : (part + 1) * D], 1, 0)
    input_grad = to_quarters(input_grad.astype(jnp.bfloat16))
    output = to_quarters(output.astype(jnp.bfloat16))

    small_local = jnp.concatenate(
        [
            grad_gain_one,
            grad_gain_two,
            grad_shift_one,
            grad_shift_two,
            grad_bias_query,
            grad_bias_value,
            grad_bias_out,
            grad_bias_down,
            grad_bias_up,
        ]
    )
    grads = [grad_qkv, grad_outw, grad_up, grad_down]
    if on_plane:
        mine, small_grad = plane_reduce(
            grads, block_widths, block_starts, small_local.reshape(-1, LANES)
        )
        small_grad = small_grad.reshape(-1)
    else:
        mine = lax.psum(scatter_blocks(grads), "seq")
        small_grad = lax.psum(small_local, ("dp", "seq"))
    reduced = mine.T.astype(jnp.float32)
    bases_low = bases.astype(jnp.bfloat16)
    rights = [
        right_bases[
            block_starts[which] : block_starts[which] + block_widths[which],
            : owners * block_widths[which],
        ].astype(jnp.bfloat16)
        for which in range(4)
    ]
    terms = []
    for which, block in enumerate(blocks_of(mine)):
        turned = dot_dims(block, bases_low[which], 1, 0).astype(jnp.bfloat16)
        terms.append(dot_dims(rights[which], turned, 0, 0).astype(jnp.bfloat16))
    rotated = scatter_blocks(terms).T.astype(jnp.float32)
    first_new, second_new, heading = moments(rotated, first_moment, second_moment)
    heading = heading.astype(jnp.bfloat16)
    steps = [
        dot_dims(
            heading[:, block_starts[which] : block_starts[which] + block_widths[which]],
            bases_low[which],
            0,
            1,
        ).astype(jnp.bfloat16)
        for which in range(4)
    ]
    every = gather_blocks(jnp.concatenate(steps, axis=0))
    update = [dot_dims(every[which], rights[which], 0, 1) for which in range(4)]
    weights_new = weights - learn_rate * jnp.concatenate(update, axis=1)
    small_first_new, small_second_new, small_heading = moments(
        small_grad, small_first, small_second
    )
    small_new = small - small_rate * small_heading
    return (
        output,
        input_grad,
        reduced,
        first_new,
        second_new,
        weights_new,
        weights_new.astype(jnp.bfloat16),
        small_grad,
        small_first_new,
        small_second_new,
        small_new,
    )


def solution(mesh):
    return jax.shard_map(
        on_device,
        mesh=mesh,
        in_specs=(
            P("dp", "seq", None),
            P("dp", None),
            P("dp", "seq", None),
            P(None, "dp"),
            P(None, "dp"),
            P(None, "dp"),
            P(),
            P("dp", None),
            P(),
            P(),
            P(),
        ),
        out_specs=(
            P("dp", "seq", None),
            P("dp", "seq", None),
            P(None, "dp"),
            P(None, "dp"),
            P(None, "dp"),
            P(None, "dp"),
            P(None, "dp"),
            P(),
            P(),
            P(),
            P(),
        ),
        check_vma=False,
    )
```

```python
import functools
import math

import jax
import jax.numpy as jnp
from jax import lax
from jax.experimental import pallas as pl
from jax.experimental.pallas import tpu as pltpu
from jax.sharding import PartitionSpec as P

D = 768
HEADS = 12
HD = 64
FF = 3072
STEP = 10


norm_eps = 1e-12
beta_first = 0.9
beta_second = 0.999
adam_eps = 1e-08
learn_rate = 0.03
small_rate = 0.3

TILE = 256
LANES = 128
WINDOWS = (256, 512, 640, 768, 1024)
NEG = -1e30
VMEM_LIMIT = 60 * 1024 * 1024


def dot_dims(left, right, left_dim, right_dim):
    return lax.dot_general(
        left, right, (((left_dim,), (right_dim,)), ((), ())), preferred_element_type=jnp.float32
    )


def normalize(resid, gain, shift):
    centre = resid - jnp.mean(resid, axis=-1, keepdims=True)
    spread = jnp.mean(centre * centre, axis=-1, keepdims=True)
    inv_std = lax.rsqrt(spread + norm_eps)
    scaled = centre * inv_std
    return (scaled * gain + shift, scaled, inv_std)


def norm_back(grad, scaled, inv_std, gain):
    lifted = grad * gain
    return inv_std * (
        lifted
        - jnp.mean(lifted, axis=-1, keepdims=True)
        - scaled * jnp.mean(lifted * scaled, axis=-1, keepdims=True)
    )


def moments(grad, first, second):
    first_out = beta_first * first + (1.0 - beta_first) * grad
    second_out = beta_second * second + (1.0 - beta_second) * grad * grad
    heading = (
        first_out
        / (1.0 - beta_first**STEP)
        / (jnp.sqrt(second_out / (1.0 - beta_second**STEP)) + adam_eps)
    )
    return (first_out, second_out, heading)


def windows_of(length):
    return tuple(size for size in WINDOWS if size < length) + (length,)


def key_windows(marks):
    rows, length = marks.shape
    tile = min(TILE, length)
    sizes = windows_of(length)
    heads = marks[:, ::tile]
    tails = marks[:, tile - 1 :: tile]
    low = jnp.sum((marks[:, None, :] < heads[:, :, None]).astype(jnp.int32), axis=-1)
    high = jnp.sum((marks[:, None, :] <= tails[:, :, None]).astype(jnp.int32), axis=-1)
    begin = low // LANES * LANES
    need = high - begin
    which = jnp.zeros_like(need)
    for size in sizes[:-1]:
        which = which + (need > size).astype(jnp.int32)
    width = jnp.asarray(sizes, jnp.int32)[which]
    begin = jnp.minimum(begin, length - width)
    return jnp.stack([begin, which], axis=-1).reshape(rows, -1)


def head_lanes(half, shape):
    lane = lax.broadcasted_iota(jnp.int32, shape, 1)
    return (lane >= half * HD) & (lane < (half + 1) * HD)


def attend_kernel(sizes, tile, table, q_ref, k_ref, v_ref, col_ref, row_ref, ctx_ref, log_ref, vt_ref):
    length = k_ref.shape[0]
    row = pl.program_id(0)
    vt_ref[...] = v_ref[...].astype(jnp.float32).T.astype(jnp.bfloat16)

    @pl.loop(0, length // tile)
    def _(step):
        begin = pl.multiple_of(table[row, 2 * step], LANES)
        which = table[row, 2 * step + 1]
        rows = pl.ds(pl.multiple_of(step * tile, tile), tile)
        for number, size in enumerate(sizes):

            @pl.when(which == number)
            def _(size=size):
                keys = k_ref[pl.ds(begin, size), :]
                marks = col_ref[pl.ds(begin, size), :]
                same = jnp.concatenate([marks] * (tile // LANES), axis=1) == row_ref[0, :, rows]
                here = q_ref[rows, :]
                done = []
                for half in range(2):
                    mine = jnp.where(head_lanes(half, here.shape), here * HD ** (-0.5), 0.0).astype(
                        jnp.bfloat16
                    )
                    raw = jnp.where(same, dot_dims(keys, mine, 1, 1), NEG)
                    peak = jnp.max(raw, axis=0, keepdims=True)
                    expo = jnp.exp(raw - peak)
                    total = jnp.sum(expo, axis=0, keepdims=True)
                    mixed = jnp.dot(
                        vt_ref[half * HD : (half + 1) * HD, pl.ds(begin, size)],
                        expo.astype(jnp.bfloat16),
                        preferred_element_type=jnp.float32,
                    )
                    done.append(mixed * (1.0 / total))
                    log_ref[0, half : half + 1, rows] = peak + jnp.log(total)
                ctx_ref[rows, :] = jnp.concatenate(done, axis=0).T.astype(jnp.bfloat16)


def attend(table, project, marks_col, marks_row, rows, length):
    pairs = HEADS * HD // LANES
    tile = min(TILE, length)
    sizes = windows_of(length)
    columns = lambda part: pl.BlockSpec((length, LANES), lambda i, j, t: (i, part * pairs + j))
    flops = 4 * rows * HEADS * length * length * HD
    return pl.pallas_call(
        functools.partial(attend_kernel, sizes, tile),
        out_shape=(
            jax.ShapeDtypeStruct((rows * length, D), jnp.bfloat16),
            jax.ShapeDtypeStruct((rows * pairs, 2, length), jnp.float32),
        ),
        grid_spec=pltpu.PrefetchScalarGridSpec(
            num_scalar_prefetch=1,
            grid=(rows, pairs),
            in_specs=[
                columns(0),
                columns(1),
                columns(2),
                pl.BlockSpec((length, LANES), lambda i, j, t: (i, 0)),
                pl.BlockSpec((1, 1, length), lambda i, j, t: (i, 0, 0)),
            ],
            out_specs=[
                pl.BlockSpec((length, LANES), lambda i, j, t: (i, j)),
                pl.BlockSpec((1, 2, length), lambda i, j, t: (i * pairs + j, 0, 0)),
            ],
            scratch_shapes=[pltpu.VMEM((LANES, length), jnp.bfloat16)],
        ),
        compiler_params=pltpu.CompilerParams(vmem_limit_bytes=VMEM_LIMIT),
        cost_estimate=pl.CostEstimate(
            flops=flops, bytes_accessed=8 * rows * length * D, transcendentals=rows * HEADS * length * length
        ),
        name="attend",
    )(table, project, project, project, marks_col, marks_row)


def attend_back_kernel(
    sizes, tile, table, q_ref, k_ref, v_ref, g_ref, col_ref, row_ref, log_ref, out_ref, kt_ref, dk_ref, dv_ref
):
    length = k_ref.shape[0]
    row = pl.program_id(0)
    kt_ref[...] = k_ref[...].astype(jnp.float32).T.astype(jnp.bfloat16)
    dk_ref[...] = jnp.zeros_like(dk_ref)
    dv_ref[...] = jnp.zeros_like(dv_ref)
    scale = HD ** (-0.5)

    @pl.loop(0, length // tile)
    def _(step):
        begin = pl.multiple_of(table[row, 2 * step], LANES)
        which = table[row, 2 * step + 1]
        rows = pl.ds(pl.multiple_of(step * tile, tile), tile)
        for number, size in enumerate(sizes):

            @pl.when(which == number)
            def _(size=size):
                window = pl.ds(begin, size)
                keys = k_ref[window, :]
                vals = v_ref[window, :]
                marks = col_ref[window, :]
                same = jnp.concatenate([marks] * (tile // LANES), axis=1) == row_ref[0, :, rows]
                here = q_ref[rows, :]
                grad = g_ref[rows, :]
                done = []
                for half in range(2):
                    lanes = head_lanes(half, here.shape)
                    mine = jnp.where(lanes, here * scale, 0.0).astype(jnp.bfloat16)
                    own = jnp.where(lanes, grad, 0.0).astype(jnp.bfloat16)
                    raw = jnp.where(same, dot_dims(keys, mine, 1, 1), NEG)
                    probs = jnp.exp(raw - log_ref[0, half : half + 1, rows])
                    d_probs = dot_dims(vals, own, 1, 1)
                    dv_ref[window, :] += jnp.dot(
                        probs.astype(jnp.bfloat16), own, preferred_element_type=jnp.float32
                    )
                    product = probs * d_probs
                    inner = jnp.sum(product, axis=0, keepdims=True)
                    d_scores = (product - probs * inner).astype(jnp.bfloat16)
                    dk_ref[window, :] += jnp.dot(d_scores, mine, preferred_element_type=jnp.float32)
                    done.append(
                        jnp.dot(
                            kt_ref[half * HD : (half + 1) * HD, window],
                            d_scores,
                            preferred_element_type=jnp.float32,
                        )
                    )
                out_ref[0, rows, :] = (jnp.concatenate(done, axis=0) * scale).T.astype(jnp.bfloat16)

    out_ref[1, :, :] = dk_ref[...].astype(jnp.bfloat16)
    out_ref[2, :, :] = dv_ref[...].astype(jnp.bfloat16)


def attend_back(table, project, grad, marks_col, marks_row, log_sum, rows, length):
    pairs = HEADS * HD // LANES
    tile = min(TILE, length)
    sizes = windows_of(length)
    columns = lambda part: pl.BlockSpec((length, LANES), lambda i, j, t: (i, part * pairs + j))
    flops = 10 * rows * HEADS * length * length * HD
    return pl.pallas_call(
        functools.partial(attend_back_kernel, sizes, tile),
        out_shape=jax.ShapeDtypeStruct((3, rows * length, D), jnp.bfloat16),
        grid_spec=pltpu.PrefetchScalarGridSpec(
            num_scalar_prefetch=1,
            grid=(rows, pairs),
            in_specs=[
                columns(0),
                columns(1),
                columns(2),
                columns(0),
                pl.BlockSpec((length, LANES), lambda i, j, t: (i, 0)),
                pl.BlockSpec((1, 1, length), lambda i, j, t: (i, 0, 0)),
                pl.BlockSpec((1, 2, length), lambda i, j, t: (i * pairs + j, 0, 0)),
            ],
            out_specs=pl.BlockSpec((3, length, LANES), lambda i, j, t: (0, i, j)),
            scratch_shapes=[
                pltpu.VMEM((LANES, length), jnp.bfloat16),
                pltpu.VMEM((length, LANES), jnp.float32),
                pltpu.VMEM((length, LANES), jnp.float32),
            ],
        ),
        compiler_params=pltpu.CompilerParams(vmem_limit_bytes=VMEM_LIMIT),
        cost_estimate=pl.CostEstimate(
            flops=flops, bytes_accessed=14 * rows * length * D, transcendentals=rows * HEADS * length * length
        ),
        name="attend_back",
    )(table, project, project, project, grad, marks_col, marks_row, log_sum)


MESH = pl.DeviceIdType.MESH
ROWS = 48


def partners(me):
    core, along_x, along_y = me % 2, (me // 2) % 2, me // 4
    side_x = me + 2 - 4 * along_x
    return (me + 1 - 2 * core, side_x, me + 4 - 8 * along_y, side_x + 4 - 8 * along_y)


def send(source, target, send_sem, recv_sem, axis, place):
    return pltpu.make_async_remote_copy(
        src_ref=source,
        dst_ref=target,
        send_sem=send_sem,
        recv_sem=recv_sem,
        device_id={axis: place},
        device_id_type=MESH,
    )


def greet(peers):
    barrier = pltpu.get_barrier_semaphore()
    for axis, place in peers:
        pl.semaphore_signal(barrier, inc=1, device_id={axis: place}, device_id_type=MESH)
    pl.semaphore_wait(barrier, len(peers))


def gather_kernel(widths, starts, places, moves, shard_ref, *refs):
    count = len(widths)
    moved_in = refs[: len(moves)]
    refs = refs[len(moves) :]
    arrays = 1 + max(number for number, _ in places)
    outs = refs[:arrays]
    moved_out = refs[arrays : arrays + len(moves)]
    refs = refs[arrays + len(moves) :]
    send_sem, recv_sem, own_sem = refs[:3]
    me = lax.axis_index("dp")
    sib, side_x, side_y, across = partners(me)
    _, sib_x, sib_y, sib_across = partners(sib)
    peers = [("dp", sib), ("dp", side_x), ("dp", side_y)]
    if moves:
        z_send, z_recv, z_own, zeros_ref = refs[3:]
        plane = lax.axis_index("seq")
        planes = [(plane + step) % 4 for step in range(1, 4)]
        peers += [("seq", place) for place in planes]
        zeros_ref[...] = jnp.zeros_like(zeros_ref)
    greet(peers)
    arrivals = [
        (side_x, None),
        (side_y, None),
        (across, 0),
        (across, 1),
        (sib, None),
        (sib_x, None),
        (sib_y, None),
        (sib_across, 0),
        (sib_across, 1),
    ]
    sent = []

    def rows_at(block, owner, part):
        number, first = places[block]
        width = widths[block]
        begin = first + owner * width
        size = width
        if part is not None:
            size = width // 2
            begin = begin + part * size
        return outs[number].at[pl.ds(pl.multiple_of(begin, 16), size)]

    def put(block, kind, slot, source, owner, part, place):
        copy = send(
            source,
            rows_at(block, owner, part),
            send_sem.at[block, slot],
            recv_sem.at[block, kind],
            "dp",
            place,
        )
        copy.start()
        sent.append(copy)

    def arrived(block, kind):
        owner, part = arrivals[kind]
        region = rows_at(block, owner, part)
        send(region, region, send_sem.at[block, 0], recv_sem.at[block, kind], "dp", sib).wait_recv()

    def forward(block, kind, slot, owner, part, place):
        put(block, kind, slot, rows_at(block, owner, part), owner, part, place)

    def each_move(number, act_send, act_own, act_recv):
        source, target = moved_in[number], moved_out[number]
        if moves[number] == "in":
            quarter = source.shape[1]
            part = lambda place: target.at[pl.ds(pl.multiple_of(place * quarter, 16), quarter)]
            for row in range(3):

                @pl.when(plane != row)
                def _(row=row):
                    act_send(
                        send(
                            source.at[row],
                            part(plane),
                            z_send.at[number, row],
                            z_recv.at[number, plane],
                            "seq",
                            row,
                        )
                    )

                @pl.when(plane == row)
                def _(row=row):
                    act_own(pltpu.make_async_copy(source.at[row], part(plane), z_own.at[number, 0]))
                    for place in planes if act_recv else ():
                        act_recv(
                            send(
                                source.at[row],
                                part(place),
                                z_send.at[number, row],
                                z_recv.at[number, place],
                                "seq",
                                place,
                            )
                        )

            @pl.when(plane == 3)
            def _():
                for place in range(4):
                    act_own(pltpu.make_async_copy(zeros_ref, part(place), z_own.at[number, place]))

        else:
            quarter = target.shape[1]
            part = lambda place: source.at[pl.ds(pl.multiple_of(place * quarter, 16), quarter)]

            @pl.when(plane < 3)
            def _():
                for step, place in enumerate(planes):
                    act_send(
                        send(
                            part(place),
                            target.at[plane],
                            z_send.at[number, step],
                            z_recv.at[number, plane],
                            "seq",
                            place,
                        )
                    )
                act_own(pltpu.make_async_copy(part(plane), target.at[plane], z_own.at[number, 0]))

            for row in range(3) if act_recv else ():

                @pl.when(plane != row)
                def _(row=row):
                    act_recv(
                        send(
                            part(plane),
                            target.at[row],
                            z_send.at[number, 0],
                            z_recv.at[number, row],
                            "seq",
                            row,
                        )
                    )

    for number in range(len(moves)):
        each_move(number, lambda copy: copy.start(), lambda copy: copy.start(), None)
    kept = []
    for block in range(count):
        mine = shard_ref.at[pl.ds(starts[block], widths[block])]
        put(block, 0, 0, mine, me, None, side_x)
        put(block, 1, 1, mine, me, None, side_y)
        put(block, 4, 2, mine, me, None, sib)
        copy = pltpu.make_async_copy(mine, rows_at(block, me, None), own_sem.at[block])
        copy.start()
        kept.append(copy)
    for step in range(count + 1):
        if step < count:
            arrived(step, 0)
            forward(step, 2, 3, side_x, 0, side_y)
            forward(step, 5, 4, side_x, None, sib)
            arrived(step, 1)
            forward(step, 3, 5, side_y, 1, side_x)
            forward(step, 6, 6, side_y, None, sib)
        if step > 0:
            arrived(step - 1, 2)
            forward(step - 1, 7, 7, across, 0, sib)
            arrived(step - 1, 3)
            forward(step - 1, 8, 8, across, 1, sib)
    for block in range(count):
        for kind in range(4, 9):
            arrived(block, kind)
    for copy in sent:
        copy.wait_send()
    for copy in kept:
        copy.wait()
    for number in range(len(moves)):
        each_move(
            number,
            lambda copy: copy.wait_send(),
            lambda copy: copy.wait(),
            lambda copy: copy.wait_recv(),
        )


def plane_gather(shard, widths, starts, joined, moves=(), arrays=(), length=0):
    count = len(widths)
    depth = shard.shape[1]
    if joined:
        places = [(0, 8 * start) for start in starts]
        out_shape = [jax.ShapeDtypeStruct((8 * sum(widths), depth), shard.dtype)]
    else:
        places = [(number, 0) for number in range(count)]
        out_shape = [jax.ShapeDtypeStruct((8 * width, depth), shard.dtype) for width in widths]
    scratch = [
        pltpu.SemaphoreType.DMA((count, 9)),
        pltpu.SemaphoreType.DMA((count, 9)),
        pltpu.SemaphoreType.DMA((count,)),
    ]
    if moves:
        quarter = length // 4
        for kind in moves:
            shape = (length, depth) if kind == "in" else (3, quarter, depth)
            out_shape.append(jax.ShapeDtypeStruct(shape, shard.dtype))
        scratch += [
            pltpu.SemaphoreType.DMA((len(moves), 3)),
            pltpu.SemaphoreType.DMA((len(moves), 4)),
            pltpu.SemaphoreType.DMA((len(moves), 4)),
            pltpu.VMEM((quarter, depth), shard.dtype),
        ]
    return pl.pallas_call(
        functools.partial(gather_kernel, widths, starts, places, moves),
        out_shape=tuple(out_shape),
        in_specs=[pl.BlockSpec(memory_space=pltpu.VMEM)] * (1 + len(moves)),
        out_specs=tuple(pl.BlockSpec(memory_space=pl.ANY) for _ in out_shape),
        scratch_shapes=scratch,
        compiler_params=pltpu.CompilerParams(
            collective_id=4 if joined else 1, has_side_effects=True, vmem_limit_bytes=16 * 1024 * 1024
        ),
        cost_estimate=pl.CostEstimate(
            flops=0, bytes_accessed=8 * 16 * shard.shape[0] * depth, transcendentals=0
        ),
        name="gather_steps" if joined else "gather_weights",
    )(shard, *arrays)


def add_rows(target, target_at, terms, count):
    def step(number, carry):
        offset = pl.multiple_of(number * ROWS, 16)
        total = None
        for ref, begin in terms:
            value = ref[pl.ds(begin + offset, ROWS), :].astype(jnp.float32)
            total = value if total is None else total + value
        target[pl.ds(target_at + offset, ROWS), :] = total.astype(target.dtype)
        return carry

    lax.fori_loop(0, count // ROWS, step, 0)


def reduce_kernel(widths, starts, places, across_planes, *refs):
    count = len(widths)
    arrays = 1 + max(number for number, _ in places)
    blocks = refs[:arrays]
    refs = refs[arrays:]
    if across_planes:
        small_ref, out_ref, small_out = refs[:3]
        refs = refs[3:]
    else:
        out_ref = refs[0]
        refs = refs[1:]
    own, given, from_x, from_y, turn_x, turn_y, total = refs[:7]
    load_sem, sib_send, sib_recv, link_send, link_recv, out_sem = refs[7:13]
    refs = refs[13:]
    if across_planes:
        low_first, high_first, low_second, final, z_send, z_recv = refs[:6]
        small_all, small_planes, small_sum, small_send, small_recv, wide_send, wide_recv = refs[6:]
    me = lax.axis_index("dp")
    plane = lax.axis_index("seq")
    sib, side_x, side_y, across = partners(me)
    _, sib_x, sib_y, sib_across = partners(sib)
    owners = (me, side_x, side_y, across)
    sib_owners = (sib, sib_x, sib_y, sib_across)
    if across_planes:
        others = [(me + step) % 8 for step in range(1, 8)]
        planes = [(plane + step) % 4 for step in range(1, 4)]
        greet([("dp", place) for place in others] + [("seq", place) for place in planes])
    else:
        greet([("dp", sib), ("dp", side_x), ("dp", side_y)])
    order = (3, 1, 2, 0)
    loads, sends = {}, []

    def block_rows(block, owner):
        number, first = places[block]
        begin = pl.multiple_of(first + owner * widths[block], 16)
        return blocks[number].at[pl.ds(begin, widths[block])]

    for block in range(count):
        width = widths[block]
        here = pl.ds(starts[block], width)
        for which in order:
            copy = send(
                block_rows(block, sib_owners[which]),
                given.at[which, here],
                sib_send.at[block, which],
                sib_recv.at[block, which],
                "dp",
                sib,
            )
            copy.start()
            sends.append(copy)
            load = pltpu.make_async_copy(
                block_rows(block, owners[which]),
                own.at[which, here],
                load_sem.at[block, which],
            )
            load.start()
            loads[block, which] = (load, copy)
    if across_planes:
        small_all[me] = small_ref[...]
        for number, place in enumerate(others):
            copy = send(
                small_ref, small_all.at[me], small_send.at[number], small_recv.at[me], "dp", place
            )
            copy.start()
            sends.append(copy)

    def link(block, slot, source, target, place):
        copy = send(source, target, link_send.at[block, slot], link_recv.at[block, slot], "dp", place)
        copy.start()
        sends.append(copy)

    def landed(block, slot, region):
        send(region, region, link_send.at[block, slot], link_recv.at[block, slot], "dp", sib).wait_recv()

    def upper(block):
        return (starts[block], widths[block] // 2)

    def lower(block):
        return (starts[block] + widths[block] // 2, widths[block] // 2)

    def rows_of(part):
        return pl.ds(part[0], part[1])

    def half_of(block):
        return pl.ds(starts[block] // 2, widths[block] // 2)

    def pair_sum(block, which):
        load, copy = loads[block, which]
        load.wait()
        copy.wait_recv()
        add_rows(
            own.at[which],
            starts[block],
            [(own.at[which], starts[block]), (given.at[which], starts[block])],
            widths[block],
        )

    def first_stage(block):
        pair_sum(block, 3)
        link(block, 0, own.at[3, rows_of(upper(block))], turn_x.at[half_of(block)], side_x)
        link(block, 1, own.at[3, rows_of(lower(block))], turn_y.at[half_of(block)], side_y)
        pair_sum(block, 1)
        link(
            block, 2, own.at[1, rows_of(upper(block))], from_x.at[rows_of(upper(block))], side_x
        )
        pair_sum(block, 2)
        link(
            block, 3, own.at[2, rows_of(lower(block))], from_y.at[rows_of(lower(block))], side_y
        )
        pair_sum(block, 0)

    def second_stage(block):
        landed(block, 0, turn_x.at[half_of(block)])
        begin, size = upper(block)
        add_rows(own.at[2], begin, [(own.at[2], begin), (turn_x, starts[block] // 2)], size)
        link(block, 4, own.at[2, rows_of(upper(block))], from_y.at[rows_of(upper(block))], side_y)
        landed(block, 1, turn_y.at[half_of(block)])
        begin, size = lower(block)
        add_rows(own.at[1], begin, [(own.at[1], begin), (turn_y, starts[block] // 2)], size)
        link(block, 5, own.at[1, rows_of(lower(block))], from_x.at[rows_of(lower(block))], side_x)

    def third_stage(block):
        landed(block, 2, from_x.at[rows_of(upper(block))])
        landed(block, 5, from_x.at[rows_of(lower(block))])
        landed(block, 3, from_y.at[rows_of(lower(block))])
        landed(block, 4, from_y.at[rows_of(upper(block))])
        begin = starts[block]
        add_rows(total, begin, [(own.at[0], begin), (from_x, begin), (from_y, begin)], widths[block])

    stages = [first_stage, second_stage, third_stage]
    results = total
    if across_planes:
        results = final

        def z_copy(block, slot, source, target, place):
            return send(source, target, z_send.at[block, slot], z_recv.at[block, slot], "seq", place)

        def z_put(block, slot, source, target, place):
            copy = z_copy(block, slot, source, target, place)
            copy.start()
            return copy

        def z_landed(block, slot, region):
            z_copy(block, slot, region, region, (plane + 1) % 4).wait_recv()

        def fourth_stage(block):
            up, down, half = rows_of(upper(block)), rows_of(lower(block)), half_of(block)

            @pl.when(plane == 0)
            def _():
                z_put(block, 0, total.at[up], low_first.at[half], 1)
                z_put(block, 1, total.at[down], low_second.at[half], 1)

            @pl.when(plane == 2)
            def _():
                z_put(block, 2, total.at[up], high_first.at[half], 1)

        def fifth_stage(block):
            up, down, half = rows_of(upper(block)), rows_of(lower(block)), half_of(block)
            middle = starts[block] // 2

            @pl.when(plane == 1)
            def _():
                z_landed(block, 0, low_first.at[half])
                z_landed(block, 2, high_first.at[half])
                begin, size = upper(block)
                add_rows(
                    final, begin, [(total, begin), (low_first, middle), (high_first, middle)], size
                )
                z_put(block, 3, final.at[up], final.at[up], 0)
                z_put(block, 4, final.at[up], final.at[up], 2)
                z_landed(block, 1, low_second.at[half])
                begin, size = lower(block)
                add_rows(total, begin, [(total, begin), (low_second, middle)], size)
                z_put(block, 5, total.at[down], low_second.at[half], 2)

        def sixth_stage(block):
            up, down, half = rows_of(upper(block)), rows_of(lower(block)), half_of(block)
            middle = starts[block] // 2

            @pl.when(plane == 2)
            def _():
                z_landed(block, 5, low_second.at[half])
                begin, size = lower(block)
                add_rows(final, begin, [(total, begin), (low_second, middle)], size)
                z_put(block, 6, final.at[down], final.at[down], 1)
                z_put(block, 7, final.at[down], final.at[down], 3)
                z_landed(block, 4, final.at[up])
                z_put(block, 8, final.at[up], final.at[up], 3)

        def seventh_stage(block):
            down = rows_of(lower(block))

            @pl.when(plane == 1)
            def _():
                z_landed(block, 6, final.at[down])
                z_put(block, 9, final.at[down], final.at[down], 0)

        def eighth_stage(block):
            up, down, half = rows_of(upper(block)), rows_of(lower(block)), half_of(block)

            @pl.when(plane == 0)
            def _():
                z_landed(block, 3, final.at[up])
                z_landed(block, 9, final.at[down])
                z_copy(block, 0, total.at[up], low_first.at[half], 1).wait_send()
                z_copy(block, 1, total.at[down], low_second.at[half], 1).wait_send()

            @pl.when(plane == 1)
            def _():
                z_copy(block, 3, final.at[up], final.at[up], 0).wait_send()
                z_copy(block, 4, final.at[up], final.at[up], 2).wait_send()
                z_copy(block, 5, total.at[down], low_second.at[half], 2).wait_send()
                z_copy(block, 9, final.at[down], final.at[down], 0).wait_send()

            @pl.when(plane == 2)
            def _():
                z_copy(block, 2, total.at[up], high_first.at[half], 1).wait_send()
                z_copy(block, 6, final.at[down], final.at[down], 1).wait_send()
                z_copy(block, 7, final.at[down], final.at[down], 3).wait_send()
                z_copy(block, 8, final.at[up], final.at[up], 3).wait_send()

            @pl.when(plane == 3)
            def _():
                z_landed(block, 7, final.at[down])
                z_landed(block, 8, final.at[up])

        stages += [fourth_stage, fifth_stage, sixth_stage, seventh_stage, eighth_stage]

    outgoing = []

    def last_stage(block):
        here = pl.ds(starts[block], widths[block])
        copy = pltpu.make_async_copy(results.at[here], out_ref.at[here], out_sem.at[block])
        copy.start()
        outgoing.append(copy)

    stages.append(last_stage)

    def small_first():
        for place in others:
            send(
                small_ref, small_all.at[place], small_send.at[0], small_recv.at[place], "dp", sib
            ).wait_recv()
        total_small = small_all[0]
        for number in range(1, 8):
            total_small = total_small + small_all[number]
        small_sum[...] = total_small
        small_planes[plane] = total_small
        for number, place in enumerate(planes):
            copy = send(
                small_sum, small_planes.at[plane], wide_send.at[number], wide_recv.at[plane], "seq", place
            )
            copy.start()
            sends.append(copy)

    def small_second():
        for place in planes:
            send(
                small_sum, small_planes.at[place], wide_send.at[0], wide_recv.at[place], "seq", place
            ).wait_recv()
        small_out[...] = (small_planes[0] + small_planes[1]) + (small_planes[2] + small_planes[3])

    for tick in range(count + len(stages) - 1):
        for number in range(len(stages) - 1, -1, -1):
            block = tick - number
            if 0 <= block < count:
                stages[number](block)
        if across_planes and tick == 1:
            small_first()
    if across_planes:
        small_second()
    for copy in sends:
        copy.wait_send()
    for copy in outgoing:
        copy.wait()


def plane_reduce(terms, widths, starts, small=None):
    count = len(widths)
    share = sum(widths)
    depth = terms[0].shape[1]
    across_planes = small is not None
    if len(terms) == 1:
        places = [(0, 8 * start) for start in starts]
    else:
        places = [(number, 0) for number in range(count)]
    low = terms[0].dtype
    whole = pltpu.VMEM((share, depth), low)
    half = pltpu.VMEM((share // 2, depth), low)
    dma = pltpu.SemaphoreType.DMA
    scratch = [
        pltpu.VMEM((4, share, depth), low),
        pltpu.VMEM((4, share, depth), low),
        whole,
        whole,
        half,
        half,
        whole,
        dma((count, 4)),
        dma((count, 4)),
        dma((count, 4)),
        dma((count, 6)),
        dma((count, 6)),
        dma((count,)),
    ]
    any_spec = pl.BlockSpec(memory_space=pl.ANY)
    vmem_spec = pl.BlockSpec(memory_space=pltpu.VMEM)
    out_shape = [jax.ShapeDtypeStruct((share, depth), low)]
    in_specs = [any_spec] * len(terms)
    out_specs = [any_spec]
    operands = list(terms)
    if across_planes:
        scratch += [
            half,
            half,
            half,
            whole,
            dma((count, 10)),
            dma((count, 10)),
            pltpu.VMEM((8,) + small.shape, small.dtype),
            pltpu.VMEM((4,) + small.shape, small.dtype),
            pltpu.VMEM(small.shape, small.dtype),
            dma((7,)),
            dma((8,)),
            dma((3,)),
            dma((4,)),
        ]
        operands.append(small)
        in_specs.append(vmem_spec)
        out_specs.append(vmem_spec)
        out_shape.append(jax.ShapeDtypeStruct(small.shape, small.dtype))
    return pl.pallas_call(
        functools.partial(reduce_kernel, widths, starts, places, across_planes),
        out_shape=tuple(out_shape),
        in_specs=in_specs,
        out_specs=tuple(out_specs),
        scratch_shapes=scratch,
        compiler_params=pltpu.CompilerParams(
            collective_id=2 if across_planes else 3,
            has_side_effects=True,
            vmem_limit_bytes=48 * 1024 * 1024,
        ),
        cost_estimate=pl.CostEstimate(
            flops=0, bytes_accessed=8 * 20 * share * depth, transcendentals=0
        ),
        name="reduce_all" if across_planes else "plane_reduce",
    )(*operands)


def basis_specs():
    return [
        pl.BlockSpec((1, D, D), lambda g: (g + jnp.minimum(g, 1), 0, 0)),
        pl.BlockSpec((1, D, D), lambda g: (1, 0, 0)),
    ]


def low_of(value):
    return value.astype(jnp.bfloat16)


def turn_kernel(joint, grad_ref, basis_ref, basis_out_ref, right_ref, reduced_ref, term_ref):
    group = pl.program_id(0)
    grad = grad_ref[...]
    reduced_ref[...] = grad.astype(jnp.float32).T
    basis = low_of(basis_ref[0])

    def spread(rows, turned, begin, columns):
        for step in range(columns // D):
            right = low_of(right_ref[rows, step * D : (step + 1) * D].T)
            term_ref[begin + step * D : begin + (step + 1) * D, :] = low_of(
                jnp.dot(right, turned, preferred_element_type=jnp.float32)
            )

    @pl.when(group == 0)
    def _():
        turned = low_of(jnp.dot(grad[:joint], basis, preferred_element_type=jnp.float32))
        spread(slice(0, joint), turned, 0, 3 * D)
        other = low_of(basis_out_ref[0])
        turned = low_of(jnp.dot(grad[joint:], other, preferred_element_type=jnp.float32))
        spread(slice(joint, grad.shape[0]), turned, 3 * D, D)

    @pl.when(group != 0)
    def _():
        turned = low_of(jnp.dot(grad, basis, preferred_element_type=jnp.float32))
        spread(slice(None), turned, 0, FF)


def turn(grad, bases, right_bases, joint):
    share = grad.shape[0]
    part = share // 3
    return pl.pallas_call(
        functools.partial(turn_kernel, joint),
        grid=(3,),
        out_shape=(
            jax.ShapeDtypeStruct((D, share), jnp.float32),
            jax.ShapeDtypeStruct((3 * FF, D), jnp.bfloat16),
        ),
        in_specs=[pl.BlockSpec((part, D), lambda g: (g, 0))]
        + basis_specs()
        + [pl.BlockSpec((part, FF), lambda g: (g, 0))],
        out_specs=(
            pl.BlockSpec((D, part), lambda g: (0, g)),
            pl.BlockSpec((FF, D), lambda g: (g, 0)),
        ),
        compiler_params=pltpu.CompilerParams(vmem_limit_bytes=VMEM_LIMIT),
        cost_estimate=pl.CostEstimate(
            flops=2 * share * D * (D + FF), bytes_accessed=4 * share * (FF + D) + 6 * FF * D, transcendentals=0
        ),
        name="turn",
    )(grad, bases, bases, right_bases)


def adam_kernel(
    joint, rotated_ref, first_ref, second_ref, basis_ref, basis_out_ref, first_out, second_out, step_ref
):
    group = pl.program_id(0)
    rotated = rotated_ref[...].astype(jnp.float32).T
    first, second, heading = moments(rotated, first_ref[...], second_ref[...])
    first_out[...] = first
    second_out[...] = second
    heading = low_of(heading.T)
    basis = low_of(basis_ref[0])

    @pl.when(group == 0)
    def _():
        other = low_of(basis_out_ref[0])
        step_ref[:joint, :] = low_of(dot_dims(heading[:joint], basis, 1, 1))
        step_ref[joint:, :] = low_of(dot_dims(heading[joint:], other, 1, 1))

    @pl.when(group != 0)
    def _():
        step_ref[...] = low_of(dot_dims(heading, basis, 1, 1))


def adam(rotated, first_moment, second_moment, bases, joint):
    share = rotated.shape[0]
    part = share // 3
    rows = pl.BlockSpec((part, D), lambda g: (g, 0))
    columns = pl.BlockSpec((D, part), lambda g: (0, g))
    wide = jax.ShapeDtypeStruct((D, share), jnp.float32)
    return pl.pallas_call(
        functools.partial(adam_kernel, joint),
        grid=(3,),
        out_shape=(wide, wide, jax.ShapeDtypeStruct((share, D), jnp.bfloat16)),
        in_specs=[rows, columns, columns] + basis_specs(),
        out_specs=(columns, columns, rows),
        compiler_params=pltpu.CompilerParams(vmem_limit_bytes=VMEM_LIMIT),
        cost_estimate=pl.CostEstimate(
            flops=2 * share * D * D, bytes_accessed=20 * share * D, transcendentals=share * D
        ),
        name="adam",
    )(rotated, first_moment, second_moment, bases, bases)


def update_kernel(joint, every_ref, right_ref, weights_ref, new_ref, low_ref):
    group = pl.program_id(0)

    def finish(update):
        new = weights_ref[...] - learn_rate * update.T
        new_ref[...] = new
        low_ref[...] = low_of(new)

    @pl.when(group == 0)
    def _():
        upper = jnp.dot(
            low_of(right_ref[:joint, : 3 * D]), every_ref[: 3 * D, :], preferred_element_type=jnp.float32
        )
        lower = jnp.dot(
            low_of(right_ref[joint:, :D]), every_ref[3 * D :, :], preferred_element_type=jnp.float32
        )
        finish(jnp.concatenate([upper, lower], axis=0))

    @pl.when(group != 0)
    def _():
        finish(jnp.dot(low_of(right_ref[...]), every_ref[...], preferred_element_type=jnp.float32))


def apply_update(every, right_bases, weights, joint):
    share = weights.shape[1]
    part = share // 3
    columns = pl.BlockSpec((D, part), lambda g: (0, g))
    return pl.pallas_call(
        functools.partial(update_kernel, joint),
        grid=(3,),
        out_shape=(
            jax.ShapeDtypeStruct((D, share), jnp.float32),
            jax.ShapeDtypeStruct((D, share), jnp.bfloat16),
        ),
        in_specs=[
            pl.BlockSpec((FF, D), lambda g: (g, 0)),
            pl.BlockSpec((part, FF), lambda g: (g, 0)),
            columns,
        ],
        out_specs=(columns, columns),
        compiler_params=pltpu.CompilerParams(vmem_limit_bytes=VMEM_LIMIT),
        cost_estimate=pl.CostEstimate(
            flops=2 * share * D * FF, bytes_accessed=4 * share * FF + 16 * share * D, transcendentals=0
        ),
        name="apply_update",
    )(every, right_bases, weights)


def on_device(
    inputs,
    segments,
    cotangent,
    weights,
    first_moment,
    second_moment,
    bases,
    right_bases,
    small,
    small_first,
    small_second,
):
    number, quarter, width = inputs.shape
    length = segments.shape[1]
    groups = lax.axis_size("seq")
    owners = lax.axis_size("dp")
    place = lax.axis_index("seq")
    rows = -(-number // groups)
    padded = rows * groups
    tokens = rows * length
    block_widths = [3 * D // owners, D // owners, FF // owners, FF // owners]
    block_starts = [sum(block_widths[:which]) for which in range(4)]

    def blocks_of(matrix):
        return [
            matrix[block_starts[which] : block_starts[which] + block_widths[which]]
            for which in range(4)
        ]

    def to_rows(array):
        array = jnp.pad(array, ((0, padded - number), (0, 0), (0, 0)))
        moved = lax.all_to_all(array, "seq", split_axis=0, concat_axis=1, tiled=True)
        return moved.reshape(tokens, width)

    def to_quarters(array):
        array = array.reshape(rows, length, width)
        moved = lax.all_to_all(array, "seq", split_axis=1, concat_axis=0, tiled=True)
        return moved[:number]

    on_plane = owners == 8 and groups == 4 and number == 3
    shard = weights.astype(jnp.bfloat16).T
    if on_plane:
        w_qkv, w_out, w_up, w_down, x, pull = plane_gather(
            shard, block_widths, block_starts, False, ("in", "in"), (inputs, cotangent), length
        )
    else:
        x = to_rows(inputs)
        pull = to_rows(cotangent)
        w_qkv, w_out, w_up, w_down = [
            lax.all_gather(block, "dp", axis=0, tiled=True) for block in blocks_of(shard)
        ]
    pieces = [small[index * D : (index + 1) * D] for index in range(8)] + [small[8 * D :]]
    (
        gain_one,
        gain_two,
        shift_one,
        shift_two,
        bias_query,
        bias_value,
        bias_out,
        bias_down,
        bias_up,
    ) = pieces

    filler = jnp.broadcast_to(
        (jnp.arange(length, dtype=jnp.int32) // TILE)[None], (padded - number, length)
    )
    marks = lax.dynamic_slice_in_dim(
        jnp.concatenate([segments, filler], axis=0), place * rows, rows, axis=0
    )
    table = key_windows(marks)
    marks_col = jnp.broadcast_to(marks.reshape(tokens, 1), (tokens, LANES))
    marks_row = marks.reshape(rows, 1, length)

    acts = x.astype(jnp.float32)
    bias_qkv = jnp.concatenate([bias_query, jnp.zeros_like(bias_query), bias_value])
    project = (dot_dims(x, w_qkv, 1, 1) + bias_qkv).astype(jnp.bfloat16)
    context, log_sum = attend(table, project, marks_col, marks_row, rows, length)
    attended = dot_dims(context, w_out, 1, 1) + bias_out
    first, scaled_one, inv_one = normalize(acts + attended, gain_one, shift_one)
    first_low = first.astype(jnp.bfloat16)
    upward = dot_dims(first_low, w_up, 1, 1) + bias_up
    active_full, gelu_pull = jax.vjp(lambda value: jax.nn.gelu(value, approximate=False), upward)
    active = active_full.astype(jnp.bfloat16)
    downward = dot_dims(active, w_down, 1, 0) + bias_down
    output, scaled_two, inv_two = normalize(first + downward, gain_two, shift_two)
    grad_out = pull.astype(jnp.float32)
    d_two = norm_back(grad_out, scaled_two, inv_two, gain_two)
    grad_gain_two = jnp.sum(grad_out * scaled_two, axis=0)
    grad_shift_two = jnp.sum(grad_out, axis=0)
    d_down = d_two.astype(jnp.bfloat16)
    grad_bias_down = jnp.sum(d_down.astype(jnp.float32), axis=0)
    grad_down = dot_dims(active, d_down, 0, 0).astype(jnp.bfloat16)
    d_active = dot_dims(d_down, w_down, 1, 1)
    (d_up_full,) = gelu_pull(d_active)
    d_up = d_up_full.astype(jnp.bfloat16)
    grad_bias_up = jnp.sum(d_up.astype(jnp.float32), axis=0)
    grad_up = dot_dims(d_up, first_low, 0, 0).astype(jnp.bfloat16)
    d_first = d_two + dot_dims(d_up, w_up, 1, 0)
    d_one = norm_back(d_first, scaled_one, inv_one, gain_one)
    grad_gain_one = jnp.sum(d_first * scaled_one, axis=0)
    grad_shift_one = jnp.sum(d_first, axis=0)
    d_att = d_one.astype(jnp.bfloat16)
    grad_bias_out = jnp.sum(d_att.astype(jnp.float32), axis=0)
    grad_outw = dot_dims(d_att, context, 0, 0).astype(jnp.bfloat16)
    d_context = dot_dims(d_att, w_out, 1, 0).astype(jnp.bfloat16)
    d_qkv = attend_back(table, project, d_context, marks_col, marks_row, log_sum, rows, length)
    grad_bias_query = jnp.sum(d_qkv[0].astype(jnp.float32), axis=0)
    grad_bias_value = jnp.sum(d_qkv[2].astype(jnp.float32), axis=0)
    grad_qkv = jnp.concatenate([dot_dims(d_qkv[part], x, 0, 0) for part in range(3)], axis=0).astype(
        jnp.bfloat16
    )
    input_grad = d_one
    for part in range(3):
        input_grad = input_grad + dot_dims(d_qkv[part], w_qkv[part * D : (part + 1) * D], 1, 0)
    input_grad = input_grad.astype(jnp.bfloat16)
    output = output.astype(jnp.bfloat16)

    small_local = jnp.concatenate(
        [
            grad_gain_one,
            grad_gain_two,
            grad_shift_one,
            grad_shift_two,
            grad_bias_query,
            grad_bias_value,
            grad_bias_out,
            grad_bias_down,
            grad_bias_up,
        ]
    )
    grads = [grad_qkv, grad_outw, grad_up, grad_down]
    if on_plane:
        joint = block_widths[0]
        mine, small_grad = plane_reduce(
            grads, block_widths, block_starts, small_local.reshape(-1, LANES)
        )
        small_grad = small_grad.reshape(-1)
        reduced, term = turn(mine, bases, right_bases, joint)
        (rotated,) = plane_reduce([term], block_widths, block_starts)
        first_new, second_new, step = adam(rotated, first_moment, second_moment, bases, joint)
        every, output, input_grad = plane_gather(
            step, block_widths, block_starts, True, ("out", "out"), (output, input_grad), length
        )
        weights_new, weights_low = apply_update(every, right_bases, weights, joint)
    else:
        output = to_quarters(output)
        input_grad = to_quarters(input_grad)
        scatter = lambda array: lax.psum_scatter(array, "dp", scatter_dimension=0, tiled=True)
        mine = lax.psum(jnp.concatenate([scatter(grad) for grad in grads], axis=0), "seq")
        small_grad = lax.psum(small_local, ("dp", "seq"))
        reduced = mine.T.astype(jnp.float32)
        bases_low = bases.astype(jnp.bfloat16)
        rights = [
            right_bases[
                block_starts[which] : block_starts[which] + block_widths[which],
                : owners * block_widths[which],
            ].astype(jnp.bfloat16)
            for which in range(4)
        ]
        rotated = []
        for which, block in enumerate(blocks_of(mine)):
            turned = low_of(dot_dims(block, bases_low[which], 1, 0))
            rotated.append(scatter(low_of(dot_dims(rights[which], turned, 0, 0))))
        rotated = jnp.concatenate(rotated, axis=0).T.astype(jnp.float32)
        first_new, second_new, heading = moments(rotated, first_moment, second_moment)
        heading = low_of(heading)
        update = []
        for which in range(4):
            block = heading[:, block_starts[which] : block_starts[which] + block_widths[which]]
            step = low_of(dot_dims(block, bases_low[which], 0, 1))
            every = lax.all_gather(step, "dp", axis=0, tiled=True)
            update.append(dot_dims(every, rights[which], 0, 1))
        weights_new = weights - learn_rate * jnp.concatenate(update, axis=1)
        weights_low = low_of(weights_new)
    small_first_new, small_second_new, small_heading = moments(
        small_grad, small_first, small_second
    )
    small_new = small - small_rate * small_heading
    return (
        output,
        input_grad,
        reduced,
        first_new,
        second_new,
        weights_new,
        weights_low,
        small_grad,
        small_first_new,
        small_second_new,
        small_new,
    )


def solution(mesh):
    return jax.shard_map(
        on_device,
        mesh=mesh,
        in_specs=(
            P("dp", "seq", None),
            P("dp", None),
            P("dp", "seq", None),
            P(None, "dp"),
            P(None, "dp"),
            P(None, "dp"),
            P(),
            P("dp", None),
            P(),
            P(),
            P(),
        ),
        out_specs=(
            P("dp", "seq", None),
            P("dp", "seq", None),
            P(None, "dp"),
            P(None, "dp"),
            P(None, "dp"),
            P(None, "dp"),
            P(None, "dp"),
            P(),
            P(),
            P(),
            P(),
        ),
        check_vma=False,
    )
```

```python
import functools
import math

import jax
import jax.numpy as jnp
from jax import lax
from jax.experimental import pallas as pl
from jax.experimental.pallas import tpu as pltpu
from jax.sharding import PartitionSpec as P

D = 768
HEADS = 12
HD = 64
FF = 3072
STEP = 10


norm_eps = 1e-12
beta_first = 0.9
beta_second = 0.999
adam_eps = 1e-08
learn_rate = 0.03
small_rate = 0.3

TILE = 256
LANES = 128
WINDOWS = (256, 512, 640, 768, 1024)
NEG = -1e30
VMEM_LIMIT = 60 * 1024 * 1024


def dot_dims(left, right, left_dim, right_dim):
    return lax.dot_general(
        left, right, (((left_dim,), (right_dim,)), ((), ())), preferred_element_type=jnp.float32
    )


def low_of(value):
    return value.astype(jnp.bfloat16)


def normalize(resid, gain, shift):
    centre = resid - jnp.mean(resid, axis=-1, keepdims=True)
    spread = jnp.mean(centre * centre, axis=-1, keepdims=True)
    inv_std = lax.rsqrt(spread + norm_eps)
    scaled = centre * inv_std
    return (scaled * gain + shift, scaled, inv_std)


def norm_back(grad, scaled, inv_std, gain):
    lifted = grad * gain
    return inv_std * (
        lifted
        - jnp.mean(lifted, axis=-1, keepdims=True)
        - scaled * jnp.mean(lifted * scaled, axis=-1, keepdims=True)
    )


def moments(grad, first, second):
    first_out = beta_first * first + (1.0 - beta_first) * grad
    second_out = beta_second * second + (1.0 - beta_second) * grad * grad
    heading = (
        first_out
        / (1.0 - beta_first**STEP)
        / (jnp.sqrt(second_out / (1.0 - beta_second**STEP)) + adam_eps)
    )
    return (first_out, second_out, heading)


def windows_of(length):
    return tuple(size for size in WINDOWS if size < length) + (length,)


def key_windows(marks):
    rows, length = marks.shape
    tile = min(TILE, length)
    sizes = windows_of(length)
    heads = marks[:, ::tile]
    tails = marks[:, tile - 1 :: tile]
    low = jnp.sum((marks[:, None, :] < heads[:, :, None]).astype(jnp.int32), axis=-1)
    high = jnp.sum((marks[:, None, :] <= tails[:, :, None]).astype(jnp.int32), axis=-1)
    begin = low // LANES * LANES
    need = high - begin
    which = jnp.zeros_like(need)
    for size in sizes[:-1]:
        which = which + (need > size).astype(jnp.int32)
    width = jnp.asarray(sizes, jnp.int32)[which]
    begin = jnp.minimum(begin, length - width)
    return jnp.stack([begin, which], axis=-1).reshape(rows, -1)


def head_lanes(half, shape):
    lane = lax.broadcasted_iota(jnp.int32, shape, 1)
    return (lane >= half * HD) & (lane < (half + 1) * HD)


def attend_kernel(sizes, tile, table, q_ref, k_ref, v_ref, col_ref, row_ref, ctx_ref, log_ref, vt_ref):
    length = k_ref.shape[0]
    row = pl.program_id(0)
    vt_ref[...] = v_ref[...].astype(jnp.float32).T.astype(jnp.bfloat16)

    @pl.loop(0, length // tile)
    def _(step):
        begin = pl.multiple_of(table[row, 2 * step], LANES)
        which = table[row, 2 * step + 1]
        rows = pl.ds(pl.multiple_of(step * tile, tile), tile)
        for number, size in enumerate(sizes):

            @pl.when(which == number)
            def _(size=size):
                keys = k_ref[pl.ds(begin, size), :]
                marks = col_ref[pl.ds(begin, size), :]
                same = jnp.concatenate([marks] * (tile // LANES), axis=1) == row_ref[0, :, rows]
                here = q_ref[rows, :]
                done = []
                for half in range(2):
                    mine = jnp.where(head_lanes(half, here.shape), here * HD ** (-0.5), 0.0).astype(
                        jnp.bfloat16
                    )
                    raw = jnp.where(same, dot_dims(keys, mine, 1, 1), NEG)
                    peak = jnp.max(raw, axis=0, keepdims=True)
                    expo = jnp.exp(raw - peak)
                    total = jnp.sum(expo, axis=0, keepdims=True)
                    mixed = jnp.dot(
                        vt_ref[half * HD : (half + 1) * HD, pl.ds(begin, size)],
                        expo.astype(jnp.bfloat16),
                        preferred_element_type=jnp.float32,
                    )
                    done.append(mixed * (1.0 / total))
                    log_ref[0, half : half + 1, rows] = peak + jnp.log(total)
                ctx_ref[rows, :] = jnp.concatenate(done, axis=0).T.astype(jnp.bfloat16)


def attend(table, project, marks_col, marks_row, rows, length):
    pairs = HEADS * HD // LANES
    tile = min(TILE, length)
    sizes = windows_of(length)
    columns = lambda part: pl.BlockSpec((length, LANES), lambda i, j, t: (i, part * pairs + j))
    flops = 4 * rows * HEADS * length * length * HD
    return pl.pallas_call(
        functools.partial(attend_kernel, sizes, tile),
        out_shape=(
            jax.ShapeDtypeStruct((rows * length, D), jnp.bfloat16),
            jax.ShapeDtypeStruct((rows * pairs, 2, length), jnp.float32),
        ),
        grid_spec=pltpu.PrefetchScalarGridSpec(
            num_scalar_prefetch=1,
            grid=(rows, pairs),
            in_specs=[
                columns(0),
                columns(1),
                columns(2),
                pl.BlockSpec((length, LANES), lambda i, j, t: (i, 0)),
                pl.BlockSpec((1, 1, length), lambda i, j, t: (i, 0, 0)),
            ],
            out_specs=[
                pl.BlockSpec((length, LANES), lambda i, j, t: (i, j)),
                pl.BlockSpec((1, 2, length), lambda i, j, t: (i * pairs + j, 0, 0)),
            ],
            scratch_shapes=[pltpu.VMEM((LANES, length), jnp.bfloat16)],
        ),
        compiler_params=pltpu.CompilerParams(vmem_limit_bytes=VMEM_LIMIT),
        cost_estimate=pl.CostEstimate(
            flops=flops, bytes_accessed=8 * rows * length * D, transcendentals=rows * HEADS * length * length
        ),
        name="attend",
    )(table, project, project, project, marks_col, marks_row)


def attend_back_kernel(
    sizes, tile, table, q_ref, k_ref, v_ref, g_ref, col_ref, row_ref, log_ref, out_ref, kt_ref, dk_ref, dv_ref
):
    length = k_ref.shape[0]
    row = pl.program_id(0)
    kt_ref[...] = k_ref[...].astype(jnp.float32).T.astype(jnp.bfloat16)
    dk_ref[...] = jnp.zeros_like(dk_ref)
    dv_ref[...] = jnp.zeros_like(dv_ref)
    scale = HD ** (-0.5)

    @pl.loop(0, length // tile)
    def _(step):
        begin = pl.multiple_of(table[row, 2 * step], LANES)
        which = table[row, 2 * step + 1]
        rows = pl.ds(pl.multiple_of(step * tile, tile), tile)
        for number, size in enumerate(sizes):

            @pl.when(which == number)
            def _(size=size):
                window = pl.ds(begin, size)
                keys = k_ref[window, :]
                vals = v_ref[window, :]
                marks = col_ref[window, :]
                same = jnp.concatenate([marks] * (tile // LANES), axis=1) == row_ref[0, :, rows]
                here = q_ref[rows, :]
                grad = g_ref[rows, :]
                done = []
                for half in range(2):
                    lanes = head_lanes(half, here.shape)
                    mine = jnp.where(lanes, here * scale, 0.0).astype(jnp.bfloat16)
                    own = jnp.where(lanes, grad, 0.0).astype(jnp.bfloat16)
                    raw = jnp.where(same, dot_dims(keys, mine, 1, 1), NEG)
                    probs = jnp.exp(raw - log_ref[0, half : half + 1, rows])
                    d_probs = dot_dims(vals, own, 1, 1)
                    dv_ref[window, :] += jnp.dot(
                        probs.astype(jnp.bfloat16), own, preferred_element_type=jnp.float32
                    )
                    product = probs * d_probs
                    inner = jnp.sum(product, axis=0, keepdims=True)
                    d_scores = (product - probs * inner).astype(jnp.bfloat16)
                    dk_ref[window, :] += jnp.dot(d_scores, mine, preferred_element_type=jnp.float32)
                    done.append(
                        jnp.dot(
                            kt_ref[half * HD : (half + 1) * HD, window],
                            d_scores,
                            preferred_element_type=jnp.float32,
                        )
                    )
                out_ref[0, rows, :] = (jnp.concatenate(done, axis=0) * scale).T.astype(jnp.bfloat16)

    out_ref[1, :, :] = dk_ref[...].astype(jnp.bfloat16)
    out_ref[2, :, :] = dv_ref[...].astype(jnp.bfloat16)


def attend_back(table, project, grad, marks_col, marks_row, log_sum, rows, length):
    pairs = HEADS * HD // LANES
    tile = min(TILE, length)
    sizes = windows_of(length)
    columns = lambda part: pl.BlockSpec((length, LANES), lambda i, j, t: (i, part * pairs + j))
    flops = 10 * rows * HEADS * length * length * HD
    return pl.pallas_call(
        functools.partial(attend_back_kernel, sizes, tile),
        out_shape=jax.ShapeDtypeStruct((3, rows * length, D), jnp.bfloat16),
        grid_spec=pltpu.PrefetchScalarGridSpec(
            num_scalar_prefetch=1,
            grid=(rows, pairs),
            in_specs=[
                columns(0),
                columns(1),
                columns(2),
                columns(0),
                pl.BlockSpec((length, LANES), lambda i, j, t: (i, 0)),
                pl.BlockSpec((1, 1, length), lambda i, j, t: (i, 0, 0)),
                pl.BlockSpec((1, 2, length), lambda i, j, t: (i * pairs + j, 0, 0)),
            ],
            out_specs=pl.BlockSpec((3, length, LANES), lambda i, j, t: (0, i, j)),
            scratch_shapes=[
                pltpu.VMEM((LANES, length), jnp.bfloat16),
                pltpu.VMEM((length, LANES), jnp.float32),
                pltpu.VMEM((length, LANES), jnp.float32),
            ],
        ),
        compiler_params=pltpu.CompilerParams(vmem_limit_bytes=VMEM_LIMIT),
        cost_estimate=pl.CostEstimate(
            flops=flops, bytes_accessed=14 * rows * length * D, transcendentals=rows * HEADS * length * length
        ),
        name="attend_back",
    )(table, project, project, project, grad, marks_col, marks_row, log_sum)


TOKENS = 256
PIECE = 768


def gelu_and_slope(value):
    size = jnp.abs(value)
    turn_at = 1.0 / (1.0 + size * (0.3275911 * 0.5**0.5))
    bell = jnp.exp(value * value * -0.5)
    tail = turn_at * (
        0.5 * 0.254829592
        + turn_at
        * (
            0.5 * -0.284496736
            + turn_at
            * (0.5 * 1.421413741 + turn_at * (0.5 * -1.453152027 + turn_at * (0.5 * 1.061405429)))
        )
    )
    tail = tail * bell
    chance = jnp.where(value >= 0.0, 1.0 - tail, tail)
    return (value * chance, chance + value * bell * (2.0 * math.pi) ** (-0.5))


def layer_kernel(
    context_ref,
    x_ref,
    pull_ref,
    out_w,
    up_w,
    down_w,
    small_ref,
    bias_up_ref,
    output_ref,
    first_ref,
    active_ref,
    d_down_ref,
    d_up_ref,
    d_att_ref,
    d_context_ref,
    sums_ref,
    up_sums_ref,
    slope_ref,
):
    parameter = lambda row: small_ref[row : row + 1, :]
    gain_one, gain_two, shift_one, shift_two = [parameter(row) for row in range(4)]
    bias_out, bias_down = parameter(6), parameter(7)
    attended = dot_dims(context_ref[...], out_w[...], 1, 1) + bias_out
    first, scaled_one, inv_one = normalize(
        x_ref[...].astype(jnp.float32) + attended, gain_one, shift_one
    )
    first_low = low_of(first)
    first_ref[...] = first_low
    downward = bias_down
    for begin in range(0, FF, PIECE):
        units = slice(begin, begin + PIECE)
        upward = dot_dims(first_low, up_w[units, :], 1, 1) + bias_up_ref[:, units]
        active, slope = gelu_and_slope(upward)
        active = low_of(active)
        active_ref[:, units] = active
        slope_ref[:, units] = slope
        downward = downward + jnp.dot(active, down_w[units, :], preferred_element_type=jnp.float32)
    output, scaled_two, inv_two = normalize(first + downward, gain_two, shift_two)
    output_ref[...] = low_of(output)
    grad_out = pull_ref[...].astype(jnp.float32)
    d_two = norm_back(grad_out, scaled_two, inv_two, gain_two)
    d_down = low_of(d_two)
    d_down_ref[...] = d_down
    d_first = d_two
    up_sums = []
    for begin in range(0, FF, PIECE):
        units = slice(begin, begin + PIECE)
        d_active = dot_dims(d_down, down_w[units, :], 1, 1)
        d_up = low_of(d_active * slope_ref[:, units])
        d_up_ref[:, units] = d_up
        up_sums.append(jnp.sum(d_up.astype(jnp.float32), axis=0, keepdims=True))
        d_first = d_first + jnp.dot(d_up, up_w[units, :], preferred_element_type=jnp.float32)
    d_one = norm_back(d_first, scaled_one, inv_one, gain_one)
    d_att = low_of(d_one)
    d_att_ref[...] = d_att
    d_context_ref[...] = low_of(jnp.dot(d_att, out_w[...], preferred_element_type=jnp.float32))
    total = lambda value: jnp.sum(value, axis=0, keepdims=True)
    nothing = jnp.zeros_like(gain_one)
    sums = jnp.concatenate(
        [
            total(d_first * scaled_one),
            total(grad_out * scaled_two),
            total(d_first),
            total(grad_out),
            nothing,
            nothing,
            total(d_att.astype(jnp.float32)),
            total(d_down.astype(jnp.float32)),
        ],
        axis=0,
    )
    up_sums = jnp.concatenate(up_sums, axis=1)

    @pl.when(pl.program_id(0) == 0)
    def _():
        sums_ref[...] = sums
        up_sums_ref[...] = up_sums

    @pl.when(pl.program_id(0) != 0)
    def _():
        sums_ref[...] += sums
        up_sums_ref[...] += up_sums


def layer(context, x, pull, w_out, w_up, w_down, small):
    tokens = context.shape[0]
    tile = min(TOKENS, tokens)
    narrow = pl.BlockSpec((tile, D), lambda i: (i, 0))
    broad = pl.BlockSpec((tile, FF), lambda i: (i, 0))
    fixed = lambda shape: pl.BlockSpec(shape, lambda i: (0, 0), pipeline_mode=pl.Buffered(1))
    low_narrow = jax.ShapeDtypeStruct((tokens, D), jnp.bfloat16)
    low_broad = jax.ShapeDtypeStruct((tokens, FF), jnp.bfloat16)
    return pl.pallas_call(
        layer_kernel,
        grid=(tokens // tile,),
        out_shape=(
            low_narrow,
            low_narrow,
            low_broad,
            low_narrow,
            low_broad,
            low_narrow,
            low_narrow,
            jax.ShapeDtypeStruct((8, D), jnp.float32),
            jax.ShapeDtypeStruct((1, FF), jnp.float32),
        ),
        in_specs=[
            narrow,
            narrow,
            narrow,
            fixed((D, D)),
            fixed((FF, D)),
            fixed((FF, D)),
            fixed((8, D)),
            fixed((1, FF)),
        ],
        out_specs=(
            narrow,
            narrow,
            broad,
            narrow,
            broad,
            narrow,
            narrow,
            pl.BlockSpec((8, D), lambda i: (0, 0)),
            pl.BlockSpec((1, FF), lambda i: (0, 0)),
        ),
        scratch_shapes=[pltpu.VMEM((tile, FF), jnp.float32)],
        compiler_params=pltpu.CompilerParams(vmem_limit_bytes=VMEM_LIMIT),
        cost_estimate=pl.CostEstimate(
            flops=4 * tokens * D * (D + 2 * FF),
            bytes_accessed=2 * (tokens * (7 * D + 2 * FF) + D * (D + 2 * FF)),
            transcendentals=2 * tokens * FF,
        ),
        name="layer",
    )(context, x, pull, w_out, w_up, w_down, small[: 8 * D].reshape(8, D), small[8 * D :].reshape(1, FF))


MESH = pl.DeviceIdType.MESH
ROWS = 48


def partners(me):
    core, along_x, along_y = me % 2, (me // 2) % 2, me // 4
    side_x = me + 2 - 4 * along_x
    return (me + 1 - 2 * core, side_x, me + 4 - 8 * along_y, side_x + 4 - 8 * along_y)


def send(source, target, send_sem, recv_sem, axis, place):
    return pltpu.make_async_remote_copy(
        src_ref=source,
        dst_ref=target,
        send_sem=send_sem,
        recv_sem=recv_sem,
        device_id={axis: place},
        device_id_type=MESH,
    )


def greet(peers):
    barrier = pltpu.get_barrier_semaphore()
    for axis, place in peers:
        pl.semaphore_signal(barrier, inc=1, device_id={axis: place}, device_id_type=MESH)
    pl.semaphore_wait(barrier, len(peers))


def gather_kernel(widths, starts, places, moves, shard_ref, *refs):
    count = len(widths)
    moved_in = refs[: len(moves)]
    refs = refs[len(moves) :]
    arrays = 1 + max(number for number, _ in places)
    outs = refs[:arrays]
    moved_out = refs[arrays : arrays + len(moves)]
    refs = refs[arrays + len(moves) :]
    send_sem, recv_sem, own_sem = refs[:3]
    me = lax.axis_index("dp")
    sib, side_x, side_y, across = partners(me)
    _, sib_x, sib_y, sib_across = partners(sib)
    peers = [("dp", sib), ("dp", side_x), ("dp", side_y)]
    if moves:
        z_send, z_recv, z_own, zeros_ref = refs[3:]
        plane = lax.axis_index("seq")
        planes = [(plane + step) % 4 for step in range(1, 4)]
        peers += [("seq", place) for place in planes]
        zeros_ref[...] = jnp.zeros_like(zeros_ref)
    greet(peers)
    arrivals = [
        (side_x, None),
        (side_y, None),
        (across, 0),
        (across, 1),
        (sib, None),
        (sib_x, None),
        (sib_y, None),
        (sib_across, 0),
        (sib_across, 1),
    ]
    sent = []

    def rows_at(block, owner, part):
        number, first = places[block]
        width = widths[block]
        begin = first + owner * width
        size = width
        if part is not None:
            size = width // 2
            begin = begin + part * size
        return outs[number].at[pl.ds(pl.multiple_of(begin, 16), size)]

    def put(block, kind, slot, source, owner, part, place):
        copy = send(
            source,
            rows_at(block, owner, part),
            send_sem.at[block, slot],
            recv_sem.at[block, kind],
            "dp",
            place,
        )
        copy.start()
        sent.append(copy)

    def arrived(block, kind):
        owner, part = arrivals[kind]
        region = rows_at(block, owner, part)
        send(region, region, send_sem.at[block, 0], recv_sem.at[block, kind], "dp", sib).wait_recv()

    def forward(block, kind, slot, owner, part, place):
        put(block, kind, slot, rows_at(block, owner, part), owner, part, place)

    def each_move(number, act_send, act_own, act_recv):
        source, target = moved_in[number], moved_out[number]
        if moves[number] == "in":
            quarter = source.shape[1]
            part = lambda place: target.at[pl.ds(pl.multiple_of(place * quarter, 16), quarter)]
            for row in range(3):

                @pl.when(plane != row)
                def _(row=row):
                    act_send(
                        send(
                            source.at[row],
                            part(plane),
                            z_send.at[number, row],
                            z_recv.at[number, plane],
                            "seq",
                            row,
                        )
                    )

                @pl.when(plane == row)
                def _(row=row):
                    act_own(pltpu.make_async_copy(source.at[row], part(plane), z_own.at[number, 0]))
                    for place in planes if act_recv else ():
                        act_recv(
                            send(
                                source.at[row],
                                part(place),
                                z_send.at[number, row],
                                z_recv.at[number, place],
                                "seq",
                                place,
                            )
                        )

            @pl.when(plane == 3)
            def _():
                for place in range(4):
                    act_own(pltpu.make_async_copy(zeros_ref, part(place), z_own.at[number, place]))

        else:
            quarter = target.shape[1]
            part = lambda place: source.at[pl.ds(pl.multiple_of(place * quarter, 16), quarter)]

            @pl.when(plane < 3)
            def _():
                for step, place in enumerate(planes):
                    act_send(
                        send(
                            part(place),
                            target.at[plane],
                            z_send.at[number, step],
                            z_recv.at[number, plane],
                            "seq",
                            place,
                        )
                    )
                act_own(pltpu.make_async_copy(part(plane), target.at[plane], z_own.at[number, 0]))

            for row in range(3) if act_recv else ():

                @pl.when(plane != row)
                def _(row=row):
                    act_recv(
                        send(
                            part(plane),
                            target.at[row],
                            z_send.at[number, 0],
                            z_recv.at[number, row],
                            "seq",
                            row,
                        )
                    )

    for number in range(len(moves)):
        each_move(number, lambda copy: copy.start(), lambda copy: copy.start(), None)
    kept = []
    for block in range(count):
        mine = shard_ref.at[pl.ds(starts[block], widths[block])]
        put(block, 0, 0, mine, me, None, side_x)
        put(block, 1, 1, mine, me, None, side_y)
        put(block, 4, 2, mine, me, None, sib)
        copy = pltpu.make_async_copy(mine, rows_at(block, me, None), own_sem.at[block])
        copy.start()
        kept.append(copy)
    for step in range(count + 1):
        if step < count:
            arrived(step, 0)
            forward(step, 2, 3, side_x, 0, side_y)
            forward(step, 5, 4, side_x, None, sib)
            arrived(step, 1)
            forward(step, 3, 5, side_y, 1, side_x)
            forward(step, 6, 6, side_y, None, sib)
        if step > 0:
            arrived(step - 1, 2)
            forward(step - 1, 7, 7, across, 0, sib)
            arrived(step - 1, 3)
            forward(step - 1, 8, 8, across, 1, sib)
    for block in range(count):
        for kind in range(4, 9):
            arrived(block, kind)
    for copy in sent:
        copy.wait_send()
    for copy in kept:
        copy.wait()
    for number in range(len(moves)):
        each_move(
            number,
            lambda copy: copy.wait_send(),
            lambda copy: copy.wait(),
            lambda copy: copy.wait_recv(),
        )


def plane_gather(shard, widths, starts, joined, moves=(), arrays=(), length=0):
    count = len(widths)
    depth = shard.shape[1]
    if joined:
        places = [(0, 8 * start) for start in starts]
        out_shape = [jax.ShapeDtypeStruct((8 * sum(widths), depth), shard.dtype)]
    else:
        places = [(number, 0) for number in range(count)]
        out_shape = [jax.ShapeDtypeStruct((8 * width, depth), shard.dtype) for width in widths]
    scratch = [
        pltpu.SemaphoreType.DMA((count, 9)),
        pltpu.SemaphoreType.DMA((count, 9)),
        pltpu.SemaphoreType.DMA((count,)),
    ]
    if moves:
        quarter = length // 4
        for kind in moves:
            shape = (length, depth) if kind == "in" else (3, quarter, depth)
            out_shape.append(jax.ShapeDtypeStruct(shape, shard.dtype))
        scratch += [
            pltpu.SemaphoreType.DMA((len(moves), 3)),
            pltpu.SemaphoreType.DMA((len(moves), 4)),
            pltpu.SemaphoreType.DMA((len(moves), 4)),
            pltpu.VMEM((quarter, depth), shard.dtype),
        ]
    return pl.pallas_call(
        functools.partial(gather_kernel, widths, starts, places, moves),
        out_shape=tuple(out_shape),
        in_specs=[pl.BlockSpec(memory_space=pltpu.VMEM)] * (1 + len(moves)),
        out_specs=tuple(pl.BlockSpec(memory_space=pl.ANY) for _ in out_shape),
        scratch_shapes=scratch,
        compiler_params=pltpu.CompilerParams(
            collective_id=4 if joined else 1, has_side_effects=True, vmem_limit_bytes=16 * 1024 * 1024
        ),
        cost_estimate=pl.CostEstimate(
            flops=0, bytes_accessed=8 * 16 * shard.shape[0] * depth, transcendentals=0
        ),
        name="gather_steps" if joined else "gather_weights",
    )(shard, *arrays)


def add_rows(target, target_at, terms, count):
    def step(number, carry):
        offset = pl.multiple_of(number * ROWS, 16)
        total = None
        for ref, begin in terms:
            value = ref[pl.ds(begin + offset, ROWS), :].astype(jnp.float32)
            total = value if total is None else total + value
        target[pl.ds(target_at + offset, ROWS), :] = total.astype(target.dtype)
        return carry

    lax.fori_loop(0, count // ROWS, step, 0)


def reduce_kernel(widths, starts, places, across_planes, *refs):
    count = len(widths)
    arrays = 1 + max(place[0] for place in places)
    blocks = refs[:arrays]
    refs = refs[arrays:]
    if across_planes:
        small_ref, out_ref, small_out = refs[:3]
        refs = refs[3:]
    else:
        out_ref = refs[0]
        refs = refs[1:]
    own, given, from_x, from_y, turn_x, turn_y, total = refs[:7]
    load_sem, sib_send, sib_recv, link_send, link_recv, out_sem = refs[7:13]
    refs = refs[13:]
    if across_planes:
        low_first, high_first, low_second, final, z_send, z_recv = refs[:6]
        small_all, small_planes, small_sum, small_send, small_recv, wide_send, wide_recv = refs[6:]
    me = lax.axis_index("dp")
    plane = lax.axis_index("seq")
    sib, side_x, side_y, across = partners(me)
    _, sib_x, sib_y, sib_across = partners(sib)
    owners = (me, side_x, side_y, across)
    sib_owners = (sib, sib_x, sib_y, sib_across)
    if across_planes:
        others = [(me + step) % 8 for step in range(1, 8)]
        planes = [(plane + step) % 4 for step in range(1, 4)]
        greet([("dp", place) for place in others] + [("seq", place) for place in planes])
    else:
        greet([("dp", sib), ("dp", side_x), ("dp", side_y)])
    order = (3, 1, 2, 0)
    loads, sends = {}, []

    def block_rows(block, owner):
        number, first, stride = places[block]
        begin = pl.multiple_of(first + owner * stride, 16)
        return blocks[number].at[pl.ds(begin, widths[block])]

    for block in range(count):
        width = widths[block]
        here = pl.ds(starts[block], width)
        for which in order:
            copy = send(
                block_rows(block, sib_owners[which]),
                given.at[which, here],
                sib_send.at[block, which],
                sib_recv.at[block, which],
                "dp",
                sib,
            )
            copy.start()
            sends.append(copy)
            load = pltpu.make_async_copy(
                block_rows(block, owners[which]),
                own.at[which, here],
                load_sem.at[block, which],
            )
            load.start()
            loads[block, which] = (load, copy)
    if across_planes:
        small_all[me] = small_ref[...]
        for number, place in enumerate(others):
            copy = send(
                small_ref, small_all.at[me], small_send.at[number], small_recv.at[me], "dp", place
            )
            copy.start()
            sends.append(copy)

    def link(block, slot, source, target, place):
        copy = send(source, target, link_send.at[block, slot], link_recv.at[block, slot], "dp", place)
        copy.start()
        sends.append(copy)

    def landed(block, slot, region):
        send(region, region, link_send.at[block, slot], link_recv.at[block, slot], "dp", sib).wait_recv()

    def upper(block):
        return (starts[block], widths[block] // 2)

    def lower(block):
        return (starts[block] + widths[block] // 2, widths[block] // 2)

    def rows_of(part):
        return pl.ds(part[0], part[1])

    def half_of(block):
        return pl.ds(starts[block] // 2, widths[block] // 2)

    def pair_sum(block, which):
        load, copy = loads[block, which]
        load.wait()
        copy.wait_recv()
        add_rows(
            own.at[which],
            starts[block],
            [(own.at[which], starts[block]), (given.at[which], starts[block])],
            widths[block],
        )

    def first_stage(block):
        pair_sum(block, 3)
        link(block, 0, own.at[3, rows_of(upper(block))], turn_x.at[half_of(block)], side_x)
        link(block, 1, own.at[3, rows_of(lower(block))], turn_y.at[half_of(block)], side_y)
        pair_sum(block, 1)
        link(
            block, 2, own.at[1, rows_of(upper(block))], from_x.at[rows_of(upper(block))], side_x
        )
        pair_sum(block, 2)
        link(
            block, 3, own.at[2, rows_of(lower(block))], from_y.at[rows_of(lower(block))], side_y
        )
        pair_sum(block, 0)

    def second_stage(block):
        landed(block, 0, turn_x.at[half_of(block)])
        begin, size = upper(block)
        add_rows(own.at[2], begin, [(own.at[2], begin), (turn_x, starts[block] // 2)], size)
        link(block, 4, own.at[2, rows_of(upper(block))], from_y.at[rows_of(upper(block))], side_y)
        landed(block, 1, turn_y.at[half_of(block)])
        begin, size = lower(block)
        add_rows(own.at[1], begin, [(own.at[1], begin), (turn_y, starts[block] // 2)], size)
        link(block, 5, own.at[1, rows_of(lower(block))], from_x.at[rows_of(lower(block))], side_x)

    def third_stage(block):
        landed(block, 2, from_x.at[rows_of(upper(block))])
        landed(block, 5, from_x.at[rows_of(lower(block))])
        landed(block, 3, from_y.at[rows_of(lower(block))])
        landed(block, 4, from_y.at[rows_of(upper(block))])
        begin = starts[block]
        add_rows(total, begin, [(own.at[0], begin), (from_x, begin), (from_y, begin)], widths[block])

    stages = [first_stage, second_stage, third_stage]
    results = total
    if across_planes:
        results = final

        def z_copy(block, slot, source, target, place):
            return send(source, target, z_send.at[block, slot], z_recv.at[block, slot], "seq", place)

        def z_put(block, slot, source, target, place):
            copy = z_copy(block, slot, source, target, place)
            copy.start()
            return copy

        def z_landed(block, slot, region):
            z_copy(block, slot, region, region, (plane + 1) % 4).wait_recv()

        def fourth_stage(block):
            up, down, half = rows_of(upper(block)), rows_of(lower(block)), half_of(block)

            @pl.when(plane == 0)
            def _():
                z_put(block, 0, total.at[up], low_first.at[half], 1)
                z_put(block, 1, total.at[down], low_second.at[half], 1)

            @pl.when(plane == 2)
            def _():
                z_put(block, 2, total.at[up], high_first.at[half], 1)

        def fifth_stage(block):
            up, down, half = rows_of(upper(block)), rows_of(lower(block)), half_of(block)
            middle = starts[block] // 2

            @pl.when(plane == 1)
            def _():
                z_landed(block, 0, low_first.at[half])
                z_landed(block, 2, high_first.at[half])
                begin, size = upper(block)
                add_rows(
                    final, begin, [(total, begin), (low_first, middle), (high_first, middle)], size
                )
                z_put(block, 3, final.at[up], final.at[up], 0)
                z_put(block, 4, final.at[up], final.at[up], 2)
                z_landed(block, 1, low_second.at[half])
                begin, size = lower(block)
                add_rows(total, begin, [(total, begin), (low_second, middle)], size)
                z_put(block, 5, total.at[down], low_second.at[half], 2)

        def sixth_stage(block):
            up, down, half = rows_of(upper(block)), rows_of(lower(block)), half_of(block)
            middle = starts[block] // 2

            @pl.when(plane == 2)
            def _():
                z_landed(block, 5, low_second.at[half])
                begin, size = lower(block)
                add_rows(final, begin, [(total, begin), (low_second, middle)], size)
                z_put(block, 6, final.at[down], final.at[down], 1)
                z_put(block, 7, final.at[down], final.at[down], 3)
                z_landed(block, 4, final.at[up])
                z_put(block, 8, final.at[up], final.at[up], 3)

        def seventh_stage(block):
            down = rows_of(lower(block))

            @pl.when(plane == 1)
            def _():
                z_landed(block, 6, final.at[down])
                z_put(block, 9, final.at[down], final.at[down], 0)

        def eighth_stage(block):
            up, down, half = rows_of(upper(block)), rows_of(lower(block)), half_of(block)

            @pl.when(plane == 0)
            def _():
                z_landed(block, 3, final.at[up])
                z_landed(block, 9, final.at[down])
                z_copy(block, 0, total.at[up], low_first.at[half], 1).wait_send()
                z_copy(block, 1, total.at[down], low_second.at[half], 1).wait_send()

            @pl.when(plane == 1)
            def _():
                z_copy(block, 3, final.at[up], final.at[up], 0).wait_send()
                z_copy(block, 4, final.at[up], final.at[up], 2).wait_send()
                z_copy(block, 5, total.at[down], low_second.at[half], 2).wait_send()
                z_copy(block, 9, final.at[down], final.at[down], 0).wait_send()

            @pl.when(plane == 2)
            def _():
                z_copy(block, 2, total.at[up], high_first.at[half], 1).wait_send()
                z_copy(block, 6, final.at[down], final.at[down], 1).wait_send()
                z_copy(block, 7, final.at[down], final.at[down], 3).wait_send()
                z_copy(block, 8, final.at[up], final.at[up], 3).wait_send()

            @pl.when(plane == 3)
            def _():
                z_landed(block, 7, final.at[down])
                z_landed(block, 8, final.at[up])

        stages += [fourth_stage, fifth_stage, sixth_stage, seventh_stage, eighth_stage]

    outgoing = []

    def last_stage(block):
        here = pl.ds(starts[block], widths[block])
        copy = pltpu.make_async_copy(results.at[here], out_ref.at[here], out_sem.at[block])
        copy.start()
        outgoing.append(copy)

    stages.append(last_stage)

    def small_first():
        for place in others:
            send(
                small_ref, small_all.at[place], small_send.at[0], small_recv.at[place], "dp", sib
            ).wait_recv()
        total_small = small_all[0]
        for number in range(1, 8):
            total_small = total_small + small_all[number]
        small_sum[...] = total_small
        small_planes[plane] = total_small
        for number, place in enumerate(planes):
            copy = send(
                small_sum, small_planes.at[plane], wide_send.at[number], wide_recv.at[plane], "seq", place
            )
            copy.start()
            sends.append(copy)

    def small_second():
        for place in planes:
            send(
                small_sum, small_planes.at[place], wide_send.at[0], wide_recv.at[place], "seq", place
            ).wait_recv()
        small_out[...] = (small_planes[0] + small_planes[1]) + (small_planes[2] + small_planes[3])

    for tick in range(count + len(stages) - 1):
        for number in range(len(stages) - 1, -1, -1):
            block = tick - number
            if 0 <= block < count:
                stages[number](block)
        if across_planes and tick == 1:
            small_first()
    if across_planes:
        small_second()
    for copy in sends:
        copy.wait_send()
    for copy in outgoing:
        copy.wait()


def plane_reduce(terms, widths, starts, small=None):
    share = sum(widths)
    depth = terms[0].shape[1]
    across_planes = small is not None
    pieces = []
    for which in (2, 3, 0, 1):
        width, start = widths[which], starts[which]
        number, first = (0, 8 * start) if len(terms) == 1 else (which, 0)
        size = next(size for size in (192, 96, width) if width % size == 0)
        pieces += [(size, start + cut, (number, first + cut, width)) for cut in range(0, width, size)]
    widths, starts, places = [list(part) for part in zip(*pieces)]
    count = len(pieces)
    low = terms[0].dtype
    whole = pltpu.VMEM((share, depth), low)
    half = pltpu.VMEM((share // 2, depth), low)
    dma = pltpu.SemaphoreType.DMA
    scratch = [
        pltpu.VMEM((4, share, depth), low),
        pltpu.VMEM((4, share, depth), low),
        whole,
        whole,
        half,
        half,
        whole,
        dma((count, 4)),
        dma((count, 4)),
        dma((count, 4)),
        dma((count, 6)),
        dma((count, 6)),
        dma((count,)),
    ]
    any_spec = pl.BlockSpec(memory_space=pl.ANY)
    vmem_spec = pl.BlockSpec(memory_space=pltpu.VMEM)
    out_shape = [jax.ShapeDtypeStruct((share, depth), low)]
    in_specs = [any_spec] * len(terms)
    out_specs = [any_spec]
    operands = list(terms)
    if across_planes:
        scratch += [
            half,
            half,
            half,
            whole,
            dma((count, 10)),
            dma((count, 10)),
            pltpu.VMEM((8,) + small.shape, small.dtype),
            pltpu.VMEM((4,) + small.shape, small.dtype),
            pltpu.VMEM(small.shape, small.dtype),
            dma((7,)),
            dma((8,)),
            dma((3,)),
            dma((4,)),
        ]
        operands.append(small)
        in_specs.append(vmem_spec)
        out_specs.append(vmem_spec)
        out_shape.append(jax.ShapeDtypeStruct(small.shape, small.dtype))
    return pl.pallas_call(
        functools.partial(reduce_kernel, widths, starts, places, across_planes),
        out_shape=tuple(out_shape),
        in_specs=in_specs,
        out_specs=tuple(out_specs),
        scratch_shapes=scratch,
        compiler_params=pltpu.CompilerParams(
            collective_id=2 if across_planes else 3,
            has_side_effects=True,
            vmem_limit_bytes=48 * 1024 * 1024,
        ),
        cost_estimate=pl.CostEstimate(
            flops=0, bytes_accessed=8 * 20 * share * depth, transcendentals=0
        ),
        name="reduce_all" if across_planes else "plane_reduce",
    )(*operands)


def basis_specs():
    return [
        pl.BlockSpec((1, D, D), lambda g: (g + jnp.minimum(g, 1), 0, 0)),
        pl.BlockSpec((1, D, D), lambda g: (1, 0, 0)),
    ]


def turn_kernel(joint, grad_ref, basis_ref, basis_out_ref, right_ref, reduced_ref, term_ref):
    group = pl.program_id(0)
    grad = grad_ref[...]
    reduced_ref[...] = grad.astype(jnp.float32).T
    basis = low_of(basis_ref[0])

    def spread(rows, turned, begin, columns):
        for step in range(columns // D):
            right = low_of(right_ref[rows, step * D : (step + 1) * D].T)
            term_ref[begin + step * D : begin + (step + 1) * D, :] = low_of(
                jnp.dot(right, turned, preferred_element_type=jnp.float32)
            )

    @pl.when(group == 0)
    def _():
        turned = low_of(jnp.dot(grad[:joint], basis, preferred_element_type=jnp.float32))
        spread(slice(0, joint), turned, 0, 3 * D)
        other = low_of(basis_out_ref[0])
        turned = low_of(jnp.dot(grad[joint:], other, preferred_element_type=jnp.float32))
        spread(slice(joint, grad.shape[0]), turned, 3 * D, D)

    @pl.when(group != 0)
    def _():
        turned = low_of(jnp.dot(grad, basis, preferred_element_type=jnp.float32))
        spread(slice(None), turned, 0, FF)


def turn(grad, bases, right_bases, joint):
    share = grad.shape[0]
    part = share // 3
    return pl.pallas_call(
        functools.partial(turn_kernel, joint),
        grid=(3,),
        out_shape=(
            jax.ShapeDtypeStruct((D, share), jnp.float32),
            jax.ShapeDtypeStruct((3 * FF, D), jnp.bfloat16),
        ),
        in_specs=[pl.BlockSpec((part, D), lambda g: (g, 0))]
        + basis_specs()
        + [pl.BlockSpec((part, FF), lambda g: (g, 0))],
        out_specs=(
            pl.BlockSpec((D, part), lambda g: (0, g)),
            pl.BlockSpec((FF, D), lambda g: (g, 0)),
        ),
        compiler_params=pltpu.CompilerParams(vmem_limit_bytes=VMEM_LIMIT),
        cost_estimate=pl.CostEstimate(
            flops=2 * share * D * (D + FF), bytes_accessed=4 * share * (FF + D) + 6 * FF * D, transcendentals=0
        ),
        name="turn",
    )(grad, bases, bases, right_bases)


def adam_kernel(
    joint, rotated_ref, first_ref, second_ref, basis_ref, basis_out_ref, first_out, second_out, step_ref
):
    group = pl.program_id(0)
    rotated = rotated_ref[...].astype(jnp.float32).T
    first, second, heading = moments(rotated, first_ref[...], second_ref[...])
    first_out[...] = first
    second_out[...] = second
    heading = low_of(heading.T)
    basis = low_of(basis_ref[0])

    @pl.when(group == 0)
    def _():
        other = low_of(basis_out_ref[0])
        step_ref[:joint, :] = low_of(dot_dims(heading[:joint], basis, 1, 1))
        step_ref[joint:, :] = low_of(dot_dims(heading[joint:], other, 1, 1))

    @pl.when(group != 0)
    def _():
        step_ref[...] = low_of(dot_dims(heading, basis, 1, 1))


def adam(rotated, first_moment, second_moment, bases, joint):
    share = rotated.shape[0]
    part = share // 3
    rows = pl.BlockSpec((part, D), lambda g: (g, 0))
    columns = pl.BlockSpec((D, part), lambda g: (0, g))
    wide = jax.ShapeDtypeStruct((D, share), jnp.float32)
    return pl.pallas_call(
        functools.partial(adam_kernel, joint),
        grid=(3,),
        out_shape=(wide, wide, jax.ShapeDtypeStruct((share, D), jnp.bfloat16)),
        in_specs=[rows, columns, columns] + basis_specs(),
        out_specs=(columns, columns, rows),
        compiler_params=pltpu.CompilerParams(vmem_limit_bytes=VMEM_LIMIT),
        cost_estimate=pl.CostEstimate(
            flops=2 * share * D * D, bytes_accessed=20 * share * D, transcendentals=share * D
        ),
        name="adam",
    )(rotated, first_moment, second_moment, bases, bases)


def update_kernel(joint, every_ref, right_ref, weights_ref, new_ref, low_ref):
    group = pl.program_id(0)

    def finish(update):
        new = weights_ref[...] - learn_rate * update.T
        new_ref[...] = new
        low_ref[...] = low_of(new)

    @pl.when(group == 0)
    def _():
        upper = jnp.dot(
            low_of(right_ref[:joint, : 3 * D]), every_ref[: 3 * D, :], preferred_element_type=jnp.float32
        )
        lower = jnp.dot(
            low_of(right_ref[joint:, :D]), every_ref[3 * D :, :], preferred_element_type=jnp.float32
        )
        finish(jnp.concatenate([upper, lower], axis=0))

    @pl.when(group != 0)
    def _():
        finish(jnp.dot(low_of(right_ref[...]), every_ref[...], preferred_element_type=jnp.float32))


def apply_update(every, right_bases, weights, joint):
    share = weights.shape[1]
    part = share // 3
    columns = pl.BlockSpec((D, part), lambda g: (0, g))
    return pl.pallas_call(
        functools.partial(update_kernel, joint),
        grid=(3,),
        out_shape=(
            jax.ShapeDtypeStruct((D, share), jnp.float32),
            jax.ShapeDtypeStruct((D, share), jnp.bfloat16),
        ),
        in_specs=[
            pl.BlockSpec((FF, D), lambda g: (g, 0)),
            pl.BlockSpec((part, FF), lambda g: (g, 0)),
            columns,
        ],
        out_specs=(columns, columns),
        compiler_params=pltpu.CompilerParams(vmem_limit_bytes=VMEM_LIMIT),
        cost_estimate=pl.CostEstimate(
            flops=2 * share * D * FF, bytes_accessed=4 * share * FF + 16 * share * D, transcendentals=0
        ),
        name="apply_update",
    )(every, right_bases, weights)


def on_device(
    inputs,
    segments,
    cotangent,
    weights,
    first_moment,
    second_moment,
    bases,
    right_bases,
    small,
    small_first,
    small_second,
):
    number, quarter, width = inputs.shape
    length = segments.shape[1]
    groups = lax.axis_size("seq")
    owners = lax.axis_size("dp")
    place = lax.axis_index("seq")
    rows = -(-number // groups)
    padded = rows * groups
    tokens = rows * length
    block_widths = [3 * D // owners, D // owners, FF // owners, FF // owners]
    block_starts = [sum(block_widths[:which]) for which in range(4)]

    def blocks_of(matrix):
        return [
            matrix[block_starts[which] : block_starts[which] + block_widths[which]]
            for which in range(4)
        ]

    def to_rows(array):
        array = jnp.pad(array, ((0, padded - number), (0, 0), (0, 0)))
        moved = lax.all_to_all(array, "seq", split_axis=0, concat_axis=1, tiled=True)
        return moved.reshape(tokens, width)

    def to_quarters(array):
        array = array.reshape(rows, length, width)
        moved = lax.all_to_all(array, "seq", split_axis=1, concat_axis=0, tiled=True)
        return moved[:number]

    on_plane = owners == 8 and groups == 4 and number == 3
    shard = weights.astype(jnp.bfloat16).T
    if on_plane:
        w_qkv, w_out, w_up, w_down, x, pull = plane_gather(
            shard, block_widths, block_starts, False, ("in", "in"), (inputs, cotangent), length
        )
    else:
        x = to_rows(inputs)
        pull = to_rows(cotangent)
        w_qkv, w_out, w_up, w_down = [
            lax.all_gather(block, "dp", axis=0, tiled=True) for block in blocks_of(shard)
        ]
    bias_query, bias_value = small[4 * D : 5 * D], small[5 * D : 6 * D]
    filler = jnp.broadcast_to(
        (jnp.arange(length, dtype=jnp.int32) // TILE)[None], (padded - number, length)
    )
    marks = lax.dynamic_slice_in_dim(
        jnp.concatenate([segments, filler], axis=0), place * rows, rows, axis=0
    )
    table = key_windows(marks)
    marks_col = jnp.broadcast_to(marks.reshape(tokens, 1), (tokens, LANES))
    marks_row = marks.reshape(rows, 1, length)

    bias_qkv = jnp.concatenate([bias_query, jnp.zeros_like(bias_query), bias_value])
    project = (dot_dims(x, w_qkv, 1, 1) + bias_qkv).astype(jnp.bfloat16)
    context, log_sum = attend(table, project, marks_col, marks_row, rows, length)
    output, first_low, active, d_down, d_up, d_att, d_context, sums, up_sums = layer(
        context, x, pull, w_out, w_up, w_down, small
    )
    grad_down = low_of(dot_dims(active, d_down, 0, 0))
    grad_up = low_of(dot_dims(d_up, first_low, 0, 0))
    grad_outw = low_of(dot_dims(d_att, context, 0, 0))
    d_qkv = attend_back(table, project, d_context, marks_col, marks_row, log_sum, rows, length)
    grad_bias_query = jnp.sum(d_qkv[0].astype(jnp.float32), axis=0)
    grad_bias_value = jnp.sum(d_qkv[2].astype(jnp.float32), axis=0)
    grad_qkv = jnp.concatenate([dot_dims(d_qkv[part], x, 0, 0) for part in range(3)], axis=0).astype(
        jnp.bfloat16
    )
    input_grad = d_att.astype(jnp.float32)
    for part in range(3):
        input_grad = input_grad + dot_dims(d_qkv[part], w_qkv[part * D : (part + 1) * D], 1, 0)
    input_grad = input_grad.astype(jnp.bfloat16)

    small_local = jnp.concatenate(
        [
            sums[:4].reshape(-1),
            grad_bias_query,
            grad_bias_value,
            sums[6:].reshape(-1),
            up_sums.reshape(-1),
        ]
    )
    grads = [grad_qkv, grad_outw, grad_up, grad_down]
    if on_plane:
        joint = block_widths[0]
        mine, small_grad = plane_reduce(
            grads, block_widths, block_starts, small_local.reshape(-1, LANES)
        )
        small_grad = small_grad.reshape(-1)
        reduced, term = turn(mine, bases, right_bases, joint)
        (rotated,) = plane_reduce([term], block_widths, block_starts)
        first_new, second_new, step = adam(rotated, first_moment, second_moment, bases, joint)
        every, output, input_grad = plane_gather(
            step, block_widths, block_starts, True, ("out", "out"), (output, input_grad), length
        )
        weights_new, weights_low = apply_update(every, right_bases, weights, joint)
    else:
        output = to_quarters(output)
        input_grad = to_quarters(input_grad)
        scatter = lambda array: lax.psum_scatter(array, "dp", scatter_dimension=0, tiled=True)
        mine = lax.psum(jnp.concatenate([scatter(grad) for grad in grads], axis=0), "seq")
        small_grad = lax.psum(small_local, ("dp", "seq"))
        reduced = mine.T.astype(jnp.float32)
        bases_low = bases.astype(jnp.bfloat16)
        rights = [
            right_bases[
                block_starts[which] : block_starts[which] + block_widths[which],
                : owners * block_widths[which],
            ].astype(jnp.bfloat16)
            for which in range(4)
        ]
        rotated = []
        for which, block in enumerate(blocks_of(mine)):
            turned = low_of(dot_dims(block, bases_low[which], 1, 0))
            rotated.append(scatter(low_of(dot_dims(rights[which], turned, 0, 0))))
        rotated = jnp.concatenate(rotated, axis=0).T.astype(jnp.float32)
        first_new, second_new, heading = moments(rotated, first_moment, second_moment)
        heading = low_of(heading)
        update = []
        for which in range(4):
            block = heading[:, block_starts[which] : block_starts[which] + block_widths[which]]
            step = low_of(dot_dims(block, bases_low[which], 0, 1))
            every = lax.all_gather(step, "dp", axis=0, tiled=True)
            update.append(dot_dims(every, rights[which], 0, 1))
        weights_new = weights - learn_rate * jnp.concatenate(update, axis=1)
        weights_low = low_of(weights_new)
    small_first_new, small_second_new, small_heading = moments(
        small_grad, small_first, small_second
    )
    small_new = small - small_rate * small_heading
    return (
        output,
        input_grad,
        reduced,
        first_new,
        second_new,
        weights_new,
        weights_low,
        small_grad,
        small_first_new,
        small_second_new,
        small_new,
    )


def solution(mesh):
    return jax.shard_map(
        on_device,
        mesh=mesh,
        in_specs=(
            P("dp", "seq", None),
            P("dp", None),
            P("dp", "seq", None),
            P(None, "dp"),
            P(None, "dp"),
            P(None, "dp"),
            P(),
            P("dp", None),
            P(),
            P(),
            P(),
        ),
        out_specs=(
            P("dp", "seq", None),
            P("dp", "seq", None),
            P(None, "dp"),
            P(None, "dp"),
            P(None, "dp"),
            P(None, "dp"),
            P(None, "dp"),
            P(),
            P(),
            P(),
            P(),
        ),
        check_vma=False,
    )
```

```python
import functools
import math

import jax
import jax.numpy as jnp
from jax import lax
from jax.experimental import pallas as pl
from jax.experimental.pallas import tpu as pltpu
from jax.sharding import PartitionSpec as P

D = 768
HEADS = 12
HD = 64
FF = 3072
STEP = 10


norm_eps = 1e-12
beta_first = 0.9
beta_second = 0.999
adam_eps = 1e-08
learn_rate = 0.03
small_rate = 0.3

TILE = 256
LANES = 128
SIDE = 4
WINDOWS = (256, 512, 640, 768, 1024)
NEG = -1e30
VMEM_LIMIT = 60 * 1024 * 1024


def dot_dims(left, right, left_dim, right_dim):
    return lax.dot_general(
        left, right, (((left_dim,), (right_dim,)), ((), ())), preferred_element_type=jnp.float32
    )


def low_of(value):
    return value.astype(jnp.bfloat16)


def normalize(resid, gain, shift):
    centre = resid - jnp.mean(resid, axis=-1, keepdims=True)
    spread = jnp.mean(centre * centre, axis=-1, keepdims=True)
    inv_std = lax.rsqrt(spread + norm_eps)
    scaled = centre * inv_std
    return (scaled * gain + shift, scaled, inv_std)


def norm_back(grad, scaled, inv_std, gain):
    lifted = grad * gain
    return inv_std * (
        lifted
        - jnp.mean(lifted, axis=-1, keepdims=True)
        - scaled * jnp.mean(lifted * scaled, axis=-1, keepdims=True)
    )


def moments(grad, first, second):
    first_out = beta_first * first + (1.0 - beta_first) * grad
    second_out = beta_second * second + (1.0 - beta_second) * grad * grad
    heading = (
        first_out
        / (1.0 - beta_first**STEP)
        / (jnp.sqrt(second_out / (1.0 - beta_second**STEP)) + adam_eps)
    )
    return (first_out, second_out, heading)


def windows_of(length):
    return tuple(size for size in WINDOWS if size < length) + (length,)


def key_windows(marks):
    rows, length = marks.shape
    tile = min(TILE, length)
    sizes = windows_of(length)
    heads = marks[:, ::tile]
    tails = marks[:, tile - 1 :: tile]
    low = jnp.sum((marks[:, None, :] < heads[:, :, None]).astype(jnp.int32), axis=-1)
    high = jnp.sum((marks[:, None, :] <= tails[:, :, None]).astype(jnp.int32), axis=-1)
    begin = low // LANES * LANES
    need = high - begin
    which = jnp.zeros_like(need)
    for size in sizes[:-1]:
        which = which + (need > size).astype(jnp.int32)
    width = jnp.asarray(sizes, jnp.int32)[which]
    begin = jnp.minimum(begin, length - width)
    return jnp.stack([begin, which], axis=-1).reshape(rows, -1)


def head_lanes(half, shape):
    lane = lax.broadcasted_iota(jnp.int32, shape, 1)
    return (lane >= half * HD) & (lane < (half + 1) * HD)


def attend_kernel(sizes, tile, table, q_ref, k_ref, v_ref, col_ref, row_ref, ctx_ref, log_ref, vt_ref):
    length = k_ref.shape[0]
    row = pl.program_id(0)
    vt_ref[...] = v_ref[...].astype(jnp.float32).T.astype(jnp.bfloat16)

    @pl.loop(0, length // tile)
    def _(step):
        begin = pl.multiple_of(table[row, 2 * step], LANES)
        which = table[row, 2 * step + 1]
        rows = pl.ds(pl.multiple_of(step * tile, tile), tile)
        for number, size in enumerate(sizes):

            @pl.when(which == number)
            def _(size=size):
                keys = k_ref[pl.ds(begin, size), :]
                marks = col_ref[pl.ds(begin, size), :]
                same = jnp.concatenate([marks] * (tile // LANES), axis=1) == row_ref[0, :, rows]
                here = q_ref[rows, :]
                done = []
                for half in range(SIDE):
                    mine = jnp.where(head_lanes(half, here.shape), here * HD ** (-0.5), 0.0).astype(
                        jnp.bfloat16
                    )
                    raw = jnp.where(same, dot_dims(keys, mine, 1, 1), NEG)
                    peak = jnp.max(raw, axis=0, keepdims=True)
                    expo = jnp.exp(raw - peak)
                    total = jnp.sum(expo, axis=0, keepdims=True)
                    mixed = jnp.dot(
                        vt_ref[half * HD : (half + 1) * HD, pl.ds(begin, size)],
                        expo.astype(jnp.bfloat16),
                        preferred_element_type=jnp.float32,
                    )
                    done.append(mixed * (1.0 / total))
                    log_ref[0, half : half + 1, rows] = peak + jnp.log(total)
                ctx_ref[rows, :] = jnp.concatenate(done, axis=0).T.astype(jnp.bfloat16)


def attend(table, project, marks_col, marks_row, rows, length):
    pairs = HEADS // SIDE
    tile = min(TILE, length)
    sizes = windows_of(length)
    columns = lambda part: pl.BlockSpec((length, SIDE * HD), lambda i, j, t: (i, part * pairs + j))
    flops = 4 * rows * HEADS * length * length * HD
    return pl.pallas_call(
        functools.partial(attend_kernel, sizes, tile),
        out_shape=(
            jax.ShapeDtypeStruct((rows * length, D), jnp.bfloat16),
            jax.ShapeDtypeStruct((rows * pairs, SIDE, length), jnp.float32),
        ),
        grid_spec=pltpu.PrefetchScalarGridSpec(
            num_scalar_prefetch=1,
            grid=(rows, pairs),
            in_specs=[
                columns(0),
                columns(1),
                columns(2),
                pl.BlockSpec((length, LANES), lambda i, j, t: (i, 0)),
                pl.BlockSpec((1, 1, length), lambda i, j, t: (i, 0, 0)),
            ],
            out_specs=[
                pl.BlockSpec((length, SIDE * HD), lambda i, j, t: (i, j)),
                pl.BlockSpec((1, SIDE, length), lambda i, j, t: (i * pairs + j, 0, 0)),
            ],
            scratch_shapes=[pltpu.VMEM((SIDE * HD, length), jnp.bfloat16)],
        ),
        compiler_params=pltpu.CompilerParams(vmem_limit_bytes=VMEM_LIMIT),
        cost_estimate=pl.CostEstimate(
            flops=flops, bytes_accessed=8 * rows * length * D, transcendentals=rows * HEADS * length * length
        ),
        name="attend",
    )(table, project, project, project, marks_col, marks_row)


def attend_back_kernel(
    sizes, tile, table, q_ref, k_ref, v_ref, g_ref, col_ref, row_ref, log_ref, out_ref, kt_ref, dk_ref, dv_ref
):
    length = k_ref.shape[0]
    row = pl.program_id(0)
    kt_ref[...] = k_ref[...].astype(jnp.float32).T.astype(jnp.bfloat16)
    dk_ref[...] = jnp.zeros_like(dk_ref)
    dv_ref[...] = jnp.zeros_like(dv_ref)
    scale = HD ** (-0.5)

    @pl.loop(0, length // tile)
    def _(step):
        begin = pl.multiple_of(table[row, 2 * step], LANES)
        which = table[row, 2 * step + 1]
        rows = pl.ds(pl.multiple_of(step * tile, tile), tile)
        for number, size in enumerate(sizes):

            @pl.when(which == number)
            def _(size=size):
                window = pl.ds(begin, size)
                keys = k_ref[window, :]
                vals = v_ref[window, :]
                marks = col_ref[window, :]
                same = jnp.concatenate([marks] * (tile // LANES), axis=1) == row_ref[0, :, rows]
                here = q_ref[rows, :]
                grad = g_ref[rows, :]
                done = []
                for half in range(SIDE):
                    lanes = head_lanes(half, here.shape)
                    mine = jnp.where(lanes, here * scale, 0.0).astype(jnp.bfloat16)
                    own = jnp.where(lanes, grad, 0.0).astype(jnp.bfloat16)
                    raw = jnp.where(same, dot_dims(keys, mine, 1, 1), NEG)
                    probs = jnp.exp(raw - log_ref[0, half : half + 1, rows])
                    d_probs = dot_dims(vals, own, 1, 1)
                    dv_ref[window, :] += jnp.dot(
                        probs.astype(jnp.bfloat16), own, preferred_element_type=jnp.float32
                    )
                    product = probs * d_probs
                    inner = jnp.sum(product, axis=0, keepdims=True)
                    d_scores = (product - probs * inner).astype(jnp.bfloat16)
                    dk_ref[window, :] += jnp.dot(d_scores, mine, preferred_element_type=jnp.float32)
                    done.append(
                        jnp.dot(
                            kt_ref[half * HD : (half + 1) * HD, window],
                            d_scores,
                            preferred_element_type=jnp.float32,
                        )
                    )
                out_ref[0, rows, :] = (jnp.concatenate(done, axis=0) * scale).T.astype(jnp.bfloat16)

    out_ref[1, :, :] = dk_ref[...].astype(jnp.bfloat16)
    out_ref[2, :, :] = dv_ref[...].astype(jnp.bfloat16)


def attend_back(table, project, grad, marks_col, marks_row, log_sum, rows, length):
    pairs = HEADS // SIDE
    tile = min(TILE, length)
    sizes = windows_of(length)
    columns = lambda part: pl.BlockSpec((length, SIDE * HD), lambda i, j, t: (i, part * pairs + j))
    flops = 10 * rows * HEADS * length * length * HD
    return pl.pallas_call(
        functools.partial(attend_back_kernel, sizes, tile),
        out_shape=jax.ShapeDtypeStruct((3, rows * length, D), jnp.bfloat16),
        grid_spec=pltpu.PrefetchScalarGridSpec(
            num_scalar_prefetch=1,
            grid=(rows, pairs),
            in_specs=[
                columns(0),
                columns(1),
                columns(2),
                columns(0),
                pl.BlockSpec((length, LANES), lambda i, j, t: (i, 0)),
                pl.BlockSpec((1, 1, length), lambda i, j, t: (i, 0, 0)),
                pl.BlockSpec((1, SIDE, length), lambda i, j, t: (i * pairs + j, 0, 0)),
            ],
            out_specs=pl.BlockSpec((3, length, SIDE * HD), lambda i, j, t: (0, i, j)),
            scratch_shapes=[
                pltpu.VMEM((SIDE * HD, length), jnp.bfloat16),
                pltpu.VMEM((length, SIDE * HD), jnp.float32),
                pltpu.VMEM((length, SIDE * HD), jnp.float32),
            ],
        ),
        compiler_params=pltpu.CompilerParams(vmem_limit_bytes=VMEM_LIMIT),
        cost_estimate=pl.CostEstimate(
            flops=flops, bytes_accessed=14 * rows * length * D, transcendentals=rows * HEADS * length * length
        ),
        name="attend_back",
    )(table, project, project, project, grad, marks_col, marks_row, log_sum)


TOKENS = 256
PIECE = 768


def gelu_and_slope(value):
    size = jnp.abs(value)
    turn_at = 1.0 / (1.0 + size * (0.3275911 * 0.5**0.5))
    bell = jnp.exp(value * value * -0.5)
    tail = turn_at * (
        0.5 * 0.254829592
        + turn_at
        * (
            0.5 * -0.284496736
            + turn_at
            * (0.5 * 1.421413741 + turn_at * (0.5 * -1.453152027 + turn_at * (0.5 * 1.061405429)))
        )
    )
    tail = tail * bell
    chance = jnp.where(value >= 0.0, 1.0 - tail, tail)
    return (value * chance, chance + value * bell * (2.0 * math.pi) ** (-0.5))


def layer_kernel(
    context_ref,
    x_ref,
    pull_ref,
    out_w,
    up_w,
    down_w,
    small_ref,
    bias_up_ref,
    output_ref,
    first_ref,
    active_ref,
    d_down_ref,
    d_up_ref,
    d_att_ref,
    d_context_ref,
    sums_ref,
    up_sums_ref,
    slope_ref,
):
    parameter = lambda row: small_ref[row : row + 1, :]
    gain_one, gain_two, shift_one, shift_two = [parameter(row) for row in range(4)]
    bias_out, bias_down = parameter(6), parameter(7)
    attended = dot_dims(context_ref[...], out_w[...], 1, 1) + bias_out
    first, scaled_one, inv_one = normalize(
        x_ref[...].astype(jnp.float32) + attended, gain_one, shift_one
    )
    first_low = low_of(first)
    first_ref[...] = first_low
    downward = bias_down
    for begin in range(0, FF, PIECE):
        units = slice(begin, begin + PIECE)
        upward = dot_dims(first_low, up_w[units, :], 1, 1) + bias_up_ref[:, units]
        active, slope = gelu_and_slope(upward)
        active = low_of(active)
        active_ref[:, units] = active
        slope_ref[:, units] = slope
        downward = downward + jnp.dot(active, down_w[units, :], preferred_element_type=jnp.float32)
    output, scaled_two, inv_two = normalize(first + downward, gain_two, shift_two)
    output_ref[...] = low_of(output)
    grad_out = pull_ref[...].astype(jnp.float32)
    d_two = norm_back(grad_out, scaled_two, inv_two, gain_two)
    d_down = low_of(d_two)
    d_down_ref[...] = d_down
    d_first = d_two
    up_sums = []
    for begin in range(0, FF, PIECE):
        units = slice(begin, begin + PIECE)
        d_active = dot_dims(d_down, down_w[units, :], 1, 1)
        d_up = low_of(d_active * slope_ref[:, units])
        d_up_ref[:, units] = d_up
        up_sums.append(jnp.sum(d_up.astype(jnp.float32), axis=0, keepdims=True))
        d_first = d_first + jnp.dot(d_up, up_w[units, :], preferred_element_type=jnp.float32)
    d_one = norm_back(d_first, scaled_one, inv_one, gain_one)
    d_att = low_of(d_one)
    d_att_ref[...] = d_att
    d_context_ref[...] = low_of(jnp.dot(d_att, out_w[...], preferred_element_type=jnp.float32))
    total = lambda value: jnp.sum(value, axis=0, keepdims=True)
    nothing = jnp.zeros_like(gain_one)
    sums = jnp.concatenate(
        [
            total(d_first * scaled_one),
            total(grad_out * scaled_two),
            total(d_first),
            total(grad_out),
            nothing,
            nothing,
            total(d_att.astype(jnp.float32)),
            total(d_down.astype(jnp.float32)),
        ],
        axis=0,
    )
    up_sums = jnp.concatenate(up_sums, axis=1)

    @pl.when(pl.program_id(0) == 0)
    def _():
        sums_ref[...] = sums
        up_sums_ref[...] = up_sums

    @pl.when(pl.program_id(0) != 0)
    def _():
        sums_ref[...] += sums
        up_sums_ref[...] += up_sums


def layer(context, x, pull, w_out, w_up, w_down, small):
    tokens = context.shape[0]
    tile = min(TOKENS, tokens)
    narrow = pl.BlockSpec((tile, D), lambda i: (i, 0))
    broad = pl.BlockSpec((tile, FF), lambda i: (i, 0))
    fixed = lambda shape: pl.BlockSpec(shape, lambda i: (0, 0), pipeline_mode=pl.Buffered(1))
    low_narrow = jax.ShapeDtypeStruct((tokens, D), jnp.bfloat16)
    low_broad = jax.ShapeDtypeStruct((tokens, FF), jnp.bfloat16)
    return pl.pallas_call(
        layer_kernel,
        grid=(tokens // tile,),
        out_shape=(
            low_narrow,
            low_narrow,
            low_broad,
            low_narrow,
            low_broad,
            low_narrow,
            low_narrow,
            jax.ShapeDtypeStruct((8, D), jnp.float32),
            jax.ShapeDtypeStruct((1, FF), jnp.float32),
        ),
        in_specs=[
            narrow,
            narrow,
            narrow,
            fixed((D, D)),
            fixed((FF, D)),
            fixed((FF, D)),
            fixed((8, D)),
            fixed((1, FF)),
        ],
        out_specs=(
            narrow,
            narrow,
            broad,
            narrow,
            broad,
            narrow,
            narrow,
            pl.BlockSpec((8, D), lambda i: (0, 0)),
            pl.BlockSpec((1, FF), lambda i: (0, 0)),
        ),
        scratch_shapes=[pltpu.VMEM((tile, FF), jnp.float32)],
        compiler_params=pltpu.CompilerParams(vmem_limit_bytes=VMEM_LIMIT),
        cost_estimate=pl.CostEstimate(
            flops=4 * tokens * D * (D + 2 * FF),
            bytes_accessed=2 * (tokens * (7 * D + 2 * FF) + D * (D + 2 * FF)),
            transcendentals=2 * tokens * FF,
        ),
        name="layer",
    )(context, x, pull, w_out, w_up, w_down, small[: 8 * D].reshape(8, D), small[8 * D :].reshape(1, FF))


MESH = pl.DeviceIdType.MESH
ROWS = 48


def partners(me):
    core, along_x, along_y = me % 2, (me // 2) % 2, me // 4
    side_x = me + 2 - 4 * along_x
    return (me + 1 - 2 * core, side_x, me + 4 - 8 * along_y, side_x + 4 - 8 * along_y)


def send(source, target, send_sem, recv_sem, axis, place):
    return pltpu.make_async_remote_copy(
        src_ref=source,
        dst_ref=target,
        send_sem=send_sem,
        recv_sem=recv_sem,
        device_id={axis: place},
        device_id_type=MESH,
    )


def greet(peers):
    barrier = pltpu.get_barrier_semaphore()
    for axis, place in peers:
        pl.semaphore_signal(barrier, inc=1, device_id={axis: place}, device_id_type=MESH)
    pl.semaphore_wait(barrier, len(peers))


def gather_tasks(widths, starts, places, shard_ref, outs, send_sem, recv_sem, own_sem):
    me = lax.axis_index("dp")
    sib, side_x, side_y, across = partners(me)
    _, sib_x, sib_y, sib_across = partners(sib)
    arrivals = [
        (side_x, None),
        (side_y, None),
        (across, 0),
        (across, 1),
        (sib, None),
        (sib_x, None),
        (sib_y, None),
        (sib_across, 0),
        (sib_across, 1),
    ]
    sent, kept = [], {}

    def rows_at(block, owner, part):
        number, first = places[block]
        width = widths[block]
        begin = first + owner * width
        size = width
        if part is not None:
            size = width // 2
            begin = begin + part * size
        return outs[number].at[pl.ds(pl.multiple_of(begin, 16), size)]

    def put(block, kind, slot, source, owner, part, place):
        copy = send(
            source,
            rows_at(block, owner, part),
            send_sem.at[block, slot],
            recv_sem.at[block, kind],
            "dp",
            place,
        )
        copy.start()
        sent.append(copy)

    def arrived(block, kind):
        owner, part = arrivals[kind]
        region = rows_at(block, owner, part)
        send(region, region, send_sem.at[block, 0], recv_sem.at[block, kind], "dp", sib).wait_recv()

    def forward(block, kind, slot, owner, part, place):
        put(block, kind, slot, rows_at(block, owner, part), owner, part, place)

    def begin(block):
        mine = shard_ref.at[pl.ds(starts[block], widths[block])]
        put(block, 0, 0, mine, me, None, side_x)
        put(block, 1, 1, mine, me, None, side_y)
        put(block, 4, 2, mine, me, None, sib)
        copy = pltpu.make_async_copy(mine, rows_at(block, me, None), own_sem.at[block])
        copy.start()
        kept[block] = copy

    def go_on(block):
        arrived(block, 0)
        forward(block, 2, 3, side_x, 0, side_y)
        forward(block, 5, 4, side_x, None, sib)
        arrived(block, 1)
        forward(block, 3, 5, side_y, 1, side_x)
        forward(block, 6, 6, side_y, None, sib)

    def share(block):
        arrived(block, 2)
        forward(block, 7, 7, across, 0, sib)
        arrived(block, 3)
        forward(block, 8, 8, across, 1, sib)

    def finish(block):
        for kind in range(4, 9):
            arrived(block, kind)
        kept[block].wait()

    return (begin, go_on, share, finish, sent)


def move_task(moves, moved_in, moved_out, z_send, z_recv, z_own, zeros_ref):
    plane = lax.axis_index("seq")
    planes = [(plane + step) % 4 for step in range(1, 4)]

    def each_move(number, act_send, act_own, act_recv):
        source, target = moved_in[number], moved_out[number]
        if moves[number] == "in":
            quarter = source.shape[1]
            part = lambda place: target.at[pl.ds(pl.multiple_of(place * quarter, 16), quarter)]
            for row in range(3):

                @pl.when(plane != row)
                def _(row=row):
                    act_send(
                        send(
                            source.at[row],
                            part(plane),
                            z_send.at[number, row],
                            z_recv.at[number, plane],
                            "seq",
                            row,
                        )
                    )

                @pl.when(plane == row)
                def _(row=row):
                    act_own(pltpu.make_async_copy(source.at[row], part(plane), z_own.at[number, 0]))
                    for place in planes if act_recv else ():
                        act_recv(
                            send(
                                source.at[row],
                                part(place),
                                z_send.at[number, row],
                                z_recv.at[number, place],
                                "seq",
                                place,
                            )
                        )

            @pl.when(plane == 3)
            def _():
                for place in range(4):
                    act_own(pltpu.make_async_copy(zeros_ref, part(place), z_own.at[number, place]))

        else:
            quarter = target.shape[1]
            part = lambda place: source.at[pl.ds(pl.multiple_of(place * quarter, 16), quarter)]

            @pl.when(plane < 3)
            def _():
                for step, place in enumerate(planes):
                    act_send(
                        send(
                            part(place),
                            target.at[plane],
                            z_send.at[number, step],
                            z_recv.at[number, plane],
                            "seq",
                            place,
                        )
                    )
                act_own(pltpu.make_async_copy(part(plane), target.at[plane], z_own.at[number, 0]))

            for row in range(3) if act_recv else ():

                @pl.when(plane != row)
                def _(row=row):
                    act_recv(
                        send(
                            part(plane),
                            target.at[row],
                            z_send.at[number, 0],
                            z_recv.at[number, row],
                            "seq",
                            row,
                        )
                    )

    def start():
        for number in range(len(moves)):
            each_move(number, lambda copy: copy.start(), lambda copy: copy.start(), None)

    def finish():
        for number in range(len(moves)):
            each_move(
                number,
                lambda copy: copy.wait_send(),
                lambda copy: copy.wait(),
                lambda copy: copy.wait_recv(),
            )

    return (start, finish)


def greet_plane(with_planes):
    me, plane = lax.axis_index("dp"), lax.axis_index("seq")
    peers = [("dp", place) for place in partners(me)[:3]]
    if with_planes:
        peers += [("seq", (plane + step) % 4) for step in range(1, 4)]
    greet(peers)


def gather_kernel(widths, starts, places, moves, shard_ref, *refs):
    count = len(widths)
    moved_in = refs[: len(moves)]
    refs = refs[len(moves) :]
    arrays = 1 + max(number for number, _ in places)
    outs = refs[:arrays]
    moved_out = refs[arrays : arrays + len(moves)]
    send_sem, recv_sem, own_sem, z_send, z_recv, z_own, zeros_ref = refs[arrays + len(moves) :]
    zeros_ref[...] = jnp.zeros_like(zeros_ref)
    greet_plane(True)
    start, settle = move_task(moves, moved_in, moved_out, z_send, z_recv, z_own, zeros_ref)
    begin, go_on, share, finish, sent = gather_tasks(
        widths, starts, places, shard_ref, outs, send_sem, recv_sem, own_sem
    )
    start()
    for block in range(count):
        begin(block)
    for step in range(count + 1):
        if step < count:
            go_on(step)
        if step > 0:
            share(step - 1)
    for block in range(count):
        finish(block)
    for copy in sent:
        copy.wait_send()
    settle()


def gather_weights(shard, widths, starts, arrays, length):
    count = len(widths)
    depth = shard.shape[1]
    moves = ("in",) * len(arrays)
    out_shape = [jax.ShapeDtypeStruct((8 * width, depth), shard.dtype) for width in widths]
    out_shape += [jax.ShapeDtypeStruct((length, depth), shard.dtype) for _ in moves]
    dma = pltpu.SemaphoreType.DMA
    return pl.pallas_call(
        functools.partial(
            gather_kernel, widths, starts, [(number, 0) for number in range(count)], moves
        ),
        out_shape=tuple(out_shape),
        in_specs=[pl.BlockSpec(memory_space=pltpu.VMEM)] * (1 + len(moves)),
        out_specs=tuple(pl.BlockSpec(memory_space=pl.ANY) for _ in out_shape),
        scratch_shapes=[
            dma((count, 9)),
            dma((count, 9)),
            dma((count,)),
            dma((len(moves), 3)),
            dma((len(moves), 4)),
            dma((len(moves), 4)),
            pltpu.VMEM((length // 4, depth), shard.dtype),
        ],
        compiler_params=pltpu.CompilerParams(
            collective_id=1, has_side_effects=True, vmem_limit_bytes=16 * 1024 * 1024
        ),
        cost_estimate=pl.CostEstimate(
            flops=0, bytes_accessed=8 * 16 * shard.shape[0] * depth, transcendentals=0
        ),
        name="gather_weights",
    )(shard, *arrays)


def add_rows(target, target_at, terms, count):
    def step(number, carry):
        offset = pl.multiple_of(number * ROWS, 16)
        total = None
        for ref, begin in terms:
            value = ref[pl.ds(begin + offset, ROWS), :].astype(jnp.float32)
            total = value if total is None else total + value
        target[pl.ds(target_at + offset, ROWS), :] = total.astype(target.dtype)
        return carry

    lax.fori_loop(0, count // ROWS, step, 0)


def reduce_kernel(widths, starts, places, across_planes, *refs):
    count = len(widths)
    arrays = 1 + max(place[0] for place in places)
    blocks = refs[:arrays]
    refs = refs[arrays:]
    if across_planes:
        small_ref, out_ref, small_out = refs[:3]
        refs = refs[3:]
    else:
        out_ref = refs[0]
        refs = refs[1:]
    own, given, from_x, from_y, turn_x, turn_y, total = refs[:7]
    load_sem, sib_send, sib_recv, link_send, link_recv, out_sem = refs[7:13]
    refs = refs[13:]
    if across_planes:
        low_first, high_first, low_second, final, z_send, z_recv = refs[:6]
        small_all, small_planes, small_sum, small_send, small_recv, wide_send, wide_recv = refs[6:]
    me = lax.axis_index("dp")
    plane = lax.axis_index("seq")
    sib, side_x, side_y, across = partners(me)
    _, sib_x, sib_y, sib_across = partners(sib)
    owners = (me, side_x, side_y, across)
    sib_owners = (sib, sib_x, sib_y, sib_across)
    if across_planes:
        others = [(me + step) % 8 for step in range(1, 8)]
        planes = [(plane + step) % 4 for step in range(1, 4)]
        greet([("dp", place) for place in others] + [("seq", place) for place in planes])
    else:
        greet([("dp", sib), ("dp", side_x), ("dp", side_y)])
    order = (3, 1, 2, 0)
    loads, sends = {}, []

    def block_rows(block, owner):
        number, first, stride = places[block]
        begin = pl.multiple_of(first + owner * stride, 16)
        return blocks[number].at[pl.ds(begin, widths[block])]

    for block in range(count):
        width = widths[block]
        here = pl.ds(starts[block], width)
        for which in order:
            copy = send(
                block_rows(block, sib_owners[which]),
                given.at[which, here],
                sib_send.at[block, which],
                sib_recv.at[block, which],
                "dp",
                sib,
            )
            copy.start()
            sends.append(copy)
            load = pltpu.make_async_copy(
                block_rows(block, owners[which]),
                own.at[which, here],
                load_sem.at[block, which],
            )
            load.start()
            loads[block, which] = (load, copy)
    if across_planes:
        small_all[me] = small_ref[...]
        for number, place in enumerate(others):
            copy = send(
                small_ref, small_all.at[me], small_send.at[number], small_recv.at[me], "dp", place
            )
            copy.start()
            sends.append(copy)

    def link(block, slot, source, target, place):
        copy = send(source, target, link_send.at[block, slot], link_recv.at[block, slot], "dp", place)
        copy.start()
        sends.append(copy)

    def landed(block, slot, region):
        send(region, region, link_send.at[block, slot], link_recv.at[block, slot], "dp", sib).wait_recv()

    def upper(block):
        return (starts[block], widths[block] // 2)

    def lower(block):
        return (starts[block] + widths[block] // 2, widths[block] // 2)

    def rows_of(part):
        return pl.ds(part[0], part[1])

    def half_of(block):
        return pl.ds(starts[block] // 2, widths[block] // 2)

    def pair_sum(block, which):
        load, copy = loads[block, which]
        load.wait()
        copy.wait_recv()
        add_rows(
            own.at[which],
            starts[block],
            [(own.at[which], starts[block]), (given.at[which], starts[block])],
            widths[block],
        )

    def first_stage(block):
        pair_sum(block, 3)
        link(block, 0, own.at[3, rows_of(upper(block))], turn_x.at[half_of(block)], side_x)
        link(block, 1, own.at[3, rows_of(lower(block))], turn_y.at[half_of(block)], side_y)
        pair_sum(block, 1)
        link(
            block, 2, own.at[1, rows_of(upper(block))], from_x.at[rows_of(upper(block))], side_x
        )
        pair_sum(block, 2)
        link(
            block, 3, own.at[2, rows_of(lower(block))], from_y.at[rows_of(lower(block))], side_y
        )
        pair_sum(block, 0)

    def second_stage(block):
        landed(block, 0, turn_x.at[half_of(block)])
        begin, size = upper(block)
        add_rows(own.at[2], begin, [(own.at[2], begin), (turn_x, starts[block] // 2)], size)
        link(block, 4, own.at[2, rows_of(upper(block))], from_y.at[rows_of(upper(block))], side_y)
        landed(block, 1, turn_y.at[half_of(block)])
        begin, size = lower(block)
        add_rows(own.at[1], begin, [(own.at[1], begin), (turn_y, starts[block] // 2)], size)
        link(block, 5, own.at[1, rows_of(lower(block))], from_x.at[rows_of(lower(block))], side_x)

    def third_stage(block):
        landed(block, 2, from_x.at[rows_of(upper(block))])
        landed(block, 5, from_x.at[rows_of(lower(block))])
        landed(block, 3, from_y.at[rows_of(lower(block))])
        landed(block, 4, from_y.at[rows_of(upper(block))])
        begin = starts[block]
        add_rows(total, begin, [(own.at[0], begin), (from_x, begin), (from_y, begin)], widths[block])

    stages = [first_stage, second_stage, third_stage]
    results = total
    if across_planes:
        results = final

        def z_copy(block, slot, source, target, place):
            return send(source, target, z_send.at[block, slot], z_recv.at[block, slot], "seq", place)

        def z_put(block, slot, source, target, place):
            copy = z_copy(block, slot, source, target, place)
            copy.start()
            return copy

        def z_landed(block, slot, region):
            z_copy(block, slot, region, region, (plane + 1) % 4).wait_recv()

        def fourth_stage(block):
            up, down, half = rows_of(upper(block)), rows_of(lower(block)), half_of(block)

            @pl.when(plane == 0)
            def _():
                z_put(block, 0, total.at[up], low_first.at[half], 1)
                z_put(block, 1, total.at[down], low_second.at[half], 1)

            @pl.when(plane == 2)
            def _():
                z_put(block, 2, total.at[up], high_first.at[half], 1)

        def fifth_stage(block):
            up, down, half = rows_of(upper(block)), rows_of(lower(block)), half_of(block)
            middle = starts[block] // 2

            @pl.when(plane == 1)
            def _():
                z_landed(block, 0, low_first.at[half])
                z_landed(block, 2, high_first.at[half])
                begin, size = upper(block)
                add_rows(
                    final, begin, [(total, begin), (low_first, middle), (high_first, middle)], size
                )
                z_put(block, 3, final.at[up], final.at[up], 0)
                z_put(block, 4, final.at[up], final.at[up], 2)
                z_landed(block, 1, low_second.at[half])
                begin, size = lower(block)
                add_rows(total, begin, [(total, begin), (low_second, middle)], size)
                z_put(block, 5, total.at[down], low_second.at[half], 2)

        def sixth_stage(block):
            up, down, half = rows_of(upper(block)), rows_of(lower(block)), half_of(block)
            middle = starts[block] // 2

            @pl.when(plane == 2)
            def _():
                z_landed(block, 5, low_second.at[half])
                begin, size = lower(block)
                add_rows(final, begin, [(total, begin), (low_second, middle)], size)
                z_put(block, 6, final.at[down], final.at[down], 1)
                z_put(block, 7, final.at[down], final.at[down], 3)
                z_landed(block, 4, final.at[up])
                z_put(block, 8, final.at[up], final.at[up], 3)

        def seventh_stage(block):
            down = rows_of(lower(block))

            @pl.when(plane == 1)
            def _():
                z_landed(block, 6, final.at[down])
                z_put(block, 9, final.at[down], final.at[down], 0)

        def eighth_stage(block):
            up, down, half = rows_of(upper(block)), rows_of(lower(block)), half_of(block)

            @pl.when(plane == 0)
            def _():
                z_landed(block, 3, final.at[up])
                z_landed(block, 9, final.at[down])
                z_copy(block, 0, total.at[up], low_first.at[half], 1).wait_send()
                z_copy(block, 1, total.at[down], low_second.at[half], 1).wait_send()

            @pl.when(plane == 1)
            def _():
                z_copy(block, 3, final.at[up], final.at[up], 0).wait_send()
                z_copy(block, 4, final.at[up], final.at[up], 2).wait_send()
                z_copy(block, 5, total.at[down], low_second.at[half], 2).wait_send()
                z_copy(block, 9, final.at[down], final.at[down], 0).wait_send()

            @pl.when(plane == 2)
            def _():
                z_copy(block, 2, total.at[up], high_first.at[half], 1).wait_send()
                z_copy(block, 6, final.at[down], final.at[down], 1).wait_send()
                z_copy(block, 7, final.at[down], final.at[down], 3).wait_send()
                z_copy(block, 8, final.at[up], final.at[up], 3).wait_send()

            @pl.when(plane == 3)
            def _():
                z_landed(block, 7, final.at[down])
                z_landed(block, 8, final.at[up])

        stages += [fourth_stage, fifth_stage, sixth_stage, seventh_stage, eighth_stage]

    outgoing = []

    def last_stage(block):
        here = pl.ds(starts[block], widths[block])
        copy = pltpu.make_async_copy(results.at[here], out_ref.at[here], out_sem.at[block])
        copy.start()
        outgoing.append(copy)

    stages.append(last_stage)

    def small_first():
        for place in others:
            send(
                small_ref, small_all.at[place], small_send.at[0], small_recv.at[place], "dp", sib
            ).wait_recv()
        total_small = small_all[0]
        for number in range(1, 8):
            total_small = total_small + small_all[number]
        small_sum[...] = total_small
        small_planes[plane] = total_small
        for number, place in enumerate(planes):
            copy = send(
                small_sum, small_planes.at[plane], wide_send.at[number], wide_recv.at[plane], "seq", place
            )
            copy.start()
            sends.append(copy)

    def small_second():
        for place in planes:
            send(
                small_sum, small_planes.at[place], wide_send.at[0], wide_recv.at[place], "seq", place
            ).wait_recv()
        small_out[...] = (small_planes[0] + small_planes[1]) + (small_planes[2] + small_planes[3])

    for tick in range(count + len(stages) - 1):
        for number in range(len(stages) - 1, -1, -1):
            block = tick - number
            if 0 <= block < count:
                stages[number](block)
        if across_planes and tick == 1:
            small_first()
    if across_planes:
        small_second()
    for copy in sends:
        copy.wait_send()
    for copy in outgoing:
        copy.wait()


def pieces_of(widths, starts, joined):
    pieces = []
    for which in (2, 3, 0, 1):
        width, start = widths[which], starts[which]
        number, first = (0, 8 * start) if joined else (which, 0)
        size = next(size for size in (192, 96, width) if width % size == 0)
        pieces += [(size, start + cut, (number, first + cut, width)) for cut in range(0, width, size)]
    return [list(part) for part in zip(*pieces)]


def plane_reduce(terms, widths, starts, small=None):
    share = sum(widths)
    depth = terms[0].shape[1]
    across_planes = small is not None
    widths, starts, places = pieces_of(widths, starts, len(terms) == 1)
    count = len(widths)
    low = terms[0].dtype
    whole = pltpu.VMEM((share, depth), low)
    half = pltpu.VMEM((share // 2, depth), low)
    dma = pltpu.SemaphoreType.DMA
    scratch = [
        pltpu.VMEM((4, share, depth), low),
        pltpu.VMEM((4, share, depth), low),
        whole,
        whole,
        half,
        half,
        whole,
        dma((count, 4)),
        dma((count, 4)),
        dma((count, 4)),
        dma((count, 6)),
        dma((count, 6)),
        dma((count,)),
    ]
    any_spec = pl.BlockSpec(memory_space=pl.ANY)
    vmem_spec = pl.BlockSpec(memory_space=pltpu.VMEM)
    out_shape = [jax.ShapeDtypeStruct((share, depth), low)]
    in_specs = [any_spec] * len(terms)
    out_specs = [any_spec]
    operands = list(terms)
    if across_planes:
        scratch += [
            half,
            half,
            half,
            whole,
            dma((count, 10)),
            dma((count, 10)),
            pltpu.VMEM((8,) + small.shape, small.dtype),
            pltpu.VMEM((4,) + small.shape, small.dtype),
            pltpu.VMEM(small.shape, small.dtype),
            dma((7,)),
            dma((8,)),
            dma((3,)),
            dma((4,)),
        ]
        operands.append(small)
        in_specs.append(vmem_spec)
        out_specs.append(vmem_spec)
        out_shape.append(jax.ShapeDtypeStruct(small.shape, small.dtype))
    return pl.pallas_call(
        functools.partial(reduce_kernel, widths, starts, places, across_planes),
        out_shape=tuple(out_shape),
        in_specs=in_specs,
        out_specs=tuple(out_specs),
        scratch_shapes=scratch,
        compiler_params=pltpu.CompilerParams(
            collective_id=2 if across_planes else 3,
            has_side_effects=True,
            vmem_limit_bytes=48 * 1024 * 1024,
        ),
        cost_estimate=pl.CostEstimate(
            flops=0, bytes_accessed=8 * 20 * share * depth, transcendentals=0
        ),
        name="reduce_all" if across_planes else "plane_reduce",
    )(*operands)


GROUPS = (1, 2, 0)
PART = 384


def group_parts(group, joint):
    if group == 0:
        return [(0, joint, 0), (joint, PART, 1)]
    return [(0, PART, group + 1)]


def group_chunks(group, joint):
    if group == 0:
        return [(0, step * D) for step in range(3)] + [(1, 0)]
    return [(0, step * D) for step in range(4)]


class Stream:
    def __init__(self, copies):
        self.copies, self.next = copies, 0
        for copy in copies[:2]:
            copy.start()

    def take(self):
        self.copies[self.next].wait()
        self.next += 1
        return (self.next - 1) % 2

    def free(self):
        if self.next + 1 < len(self.copies):
            self.copies[self.next + 1].start()


def optimize_kernel(
    block_widths,
    block_starts,
    grad_ref,
    output_ref,
    input_grad_ref,
    right_ref,
    bases_ref,
    first_ref,
    second_ref,
    weights_ref,
    reduced_out,
    first_out,
    second_out,
    new_out,
    low_out,
    every_out,
    output_out,
    input_grad_out,
    term,
    given,
    from_x,
    from_y,
    turn_x,
    turn_y,
    total,
    shard,
    right_buf,
    basis_buf,
    first_buf,
    second_buf,
    wide_buf,
    low_buf,
    every_buf,
    sib_send,
    sib_recv,
    link_send,
    link_recv,
    gather_send,
    gather_recv,
    gather_own,
    z_send,
    z_recv,
    z_own,
    right_sem,
    basis_sem,
    in_sem,
    out_sem,
    every_sem,
):
    joint = block_widths[0]
    me = lax.axis_index("dp")
    sib, side_x, side_y, across = partners(me)
    _, sib_x, sib_y, sib_across = partners(sib)
    owners = (me, side_x, side_y, across)
    sib_owners = (sib, sib_x, sib_y, sib_across)
    widths, starts, places = pieces_of(block_widths, block_starts, True)

    right_loads, basis_loads = [], []
    for group in GROUPS + GROUPS:
        parts = group_parts(group, joint)
        for part, column in group_chunks(group, joint):
            low, high, _ = parts[part]
            slot = len(right_loads) % 2
            right_loads.append(
                pltpu.make_async_copy(
                    right_ref.at[pl.ds(PART * group + low, high - low), pl.ds(column, D)],
                    right_buf.at[slot, pl.ds(0, high - low)],
                    right_sem.at[slot],
                )
            )
        for _, _, basis in parts:
            slot = len(basis_loads) % 2
            basis_loads.append(
                pltpu.make_async_copy(bases_ref.at[basis], basis_buf.at[slot], basis_sem.at[slot])
            )

    def columns(ref, group):
        return ref.at[:, pl.ds(PART * group, PART)]

    def load_moments(turn):
        for number, (ref, buf) in enumerate(((first_ref, first_buf), (second_ref, second_buf))):
            copy = pltpu.make_async_copy(
                columns(ref, GROUPS[turn]), buf.at[turn % 2], in_sem.at[number, turn % 2]
            )
            copy.start()
            moment_loads[number, turn] = copy

    def put_out(number, buf, ref, turn):
        copy = pltpu.make_async_copy(
            buf.at[turn % 2], columns(ref, GROUPS[turn]), out_sem.at[number, turn % 2]
        )
        copy.start()
        outgoing[number, turn] = copy

    moment_loads, outgoing, sends, kept = {}, {}, [], {}
    greet_plane(True)
    move_start, move_finish = move_task(
        ("out", "out"),
        (output_ref, input_grad_ref),
        (output_out, input_grad_out),
        z_send,
        z_recv,
        z_own,
        None,
    )
    rights, bases = Stream(right_loads), Stream(basis_loads)
    move_start()
    for turn in range(2):
        load_moments(turn)


    def turn_group(turn, between):
        group = GROUPS[turn]
        parts = group_parts(group, joint)
        rows = slice(PART * group, PART * (group + 1))
        grad = grad_ref[rows, :]
        if turn >= 2:
            outgoing[0, turn - 2].wait()
        wide_buf[turn % 2] = grad.astype(jnp.float32).T
        put_out(0, wide_buf, reduced_out, turn)
        turned = []
        for low, high, _ in parts:
            slot = bases.take()
            turned.append(
                low_of(
                    jnp.dot(
                        grad[low:high], low_of(basis_buf[slot]), preferred_element_type=jnp.float32
                    )
                )
            )
            bases.free()
        for number, (part, _) in enumerate(group_chunks(group, joint)):
            low, high, _ = parts[part]
            slot = rights.take()
            right = low_of(right_buf[slot, 0 : high - low, :].T)
            begin = FF * group + D * number
            term[begin : begin + D, :] = low_of(
                jnp.dot(right, turned[part], preferred_element_type=jnp.float32)
            )
            rights.free()
            for task in between[number]:
                task()

    def place_of(piece, owner):
        _, first, stride = places[piece]
        return pl.multiple_of(first + owner * stride, 16)

    def begin(piece):
        size = widths[piece]
        for which in (3, 1, 2, 0):
            copy = send(
                term.at[pl.ds(place_of(piece, sib_owners[which]), size)],
                given.at[which, pl.ds(starts[piece], size)],
                sib_send.at[piece, which],
                sib_recv.at[piece, which],
                "dp",
                sib,
            )
            copy.start()
            sends.append(copy)
            kept[piece, which] = copy

    def link(piece, slot, source, target, place):
        copy = send(source, target, link_send.at[piece, slot], link_recv.at[piece, slot], "dp", place)
        copy.start()
        sends.append(copy)

    def landed(piece, slot, region):
        send(region, region, link_send.at[piece, slot], link_recv.at[piece, slot], "dp", sib).wait_recv()

    def own_half(piece, which, part):
        half = widths[piece] // 2
        return pl.multiple_of(place_of(piece, owners[which]) + part * half, 16)

    def own_rows(piece, which, part):
        return term.at[pl.ds(own_half(piece, which, part), widths[piece] // 2)]

    def share_rows(ref, piece, part):
        half = widths[piece] // 2
        return ref.at[pl.ds(starts[piece] + part * half, half)]

    def turn_rows(ref, piece):
        return ref.at[pl.ds(starts[piece] // 2, widths[piece] // 2)]

    def pair_sum(piece, which):
        kept[piece, which].wait_recv()
        here = place_of(piece, owners[which])
        add_rows(term, here, [(term, here), (given.at[which], starts[piece])], widths[piece])

    def first_stage(piece):
        pair_sum(piece, 3)
        link(piece, 0, own_rows(piece, 3, 0), turn_rows(turn_x, piece), side_x)
        link(piece, 1, own_rows(piece, 3, 1), turn_rows(turn_y, piece), side_y)
        pair_sum(piece, 1)
        link(piece, 2, own_rows(piece, 1, 0), share_rows(from_x, piece, 0), side_x)
        pair_sum(piece, 2)
        link(piece, 3, own_rows(piece, 2, 1), share_rows(from_y, piece, 1), side_y)
        pair_sum(piece, 0)

    def second_stage(piece):
        half = widths[piece] // 2
        landed(piece, 0, turn_rows(turn_x, piece))
        here = own_half(piece, 2, 0)
        add_rows(term, here, [(term, here), (turn_x, starts[piece] // 2)], half)
        link(piece, 4, own_rows(piece, 2, 0), share_rows(from_y, piece, 0), side_y)
        landed(piece, 1, turn_rows(turn_y, piece))
        here = own_half(piece, 1, 1)
        add_rows(term, here, [(term, here), (turn_y, starts[piece] // 2)], half)
        link(piece, 5, own_rows(piece, 1, 1), share_rows(from_x, piece, 1), side_x)

    def third_stage(piece):
        landed(piece, 2, share_rows(from_x, piece, 0))
        landed(piece, 5, share_rows(from_x, piece, 1))
        landed(piece, 3, share_rows(from_y, piece, 1))
        landed(piece, 4, share_rows(from_y, piece, 0))
        here = starts[piece]
        add_rows(
            total,
            here,
            [(term, place_of(piece, me)), (from_x, here), (from_y, here)],
            widths[piece],
        )


    def adam_group(turn):
        group = GROUPS[turn]
        slot = turn % 2
        for number in range(2):
            moment_loads[number, turn].wait()
        rows = slice(PART * group, PART * (group + 1))
        rotated = total[rows, :].astype(jnp.float32).T
        first, second, heading = moments(rotated, first_buf[slot], second_buf[slot])
        first_buf[slot] = first
        second_buf[slot] = second
        put_out(1, first_buf, first_out, turn)
        put_out(2, second_buf, second_out, turn)
        heading = low_of(heading.T)
        for low, high, _ in group_parts(group, joint):
            basis = bases.take()
            shard[PART * group + low : PART * group + high, :] = low_of(
                dot_dims(heading[low:high], low_of(basis_buf[basis]), 1, 1)
            )
            bases.free()
        if turn == 1:
            for number in (1, 2):
                outgoing[number, 0].wait()
            load_moments(2)

    every_places = [(0, 8 * start) for start in block_starts]
    g_begin, g_go_on, g_share, g_finish, g_sent = gather_tasks(
        block_widths, block_starts, every_places, shard, [every_out], gather_send, gather_recv, gather_own
    )


    def load_weights(turn):
        copy = pltpu.make_async_copy(
            columns(weights_ref, GROUPS[turn]), wide_buf.at[turn % 2], in_sem.at[2, turn % 2]
        )
        copy.start()
        moment_loads[2, turn] = copy

    def update_group(turn):
        group = GROUPS[turn]
        slot = turn % 2
        parts = group_parts(group, joint)
        chunks = group_chunks(group, joint)
        loads = Stream(
            [
                pltpu.make_async_copy(
                    every_out.at[pl.ds(FF * group + D * number, D)],
                    every_buf.at[number % 2],
                    every_sem.at[number % 2],
                )
                for number in range(4)
            ]
        )
        sums = [None] * len(parts)
        for number, (part, _) in enumerate(chunks):
            low, high, _ = parts[part]
            right = rights.take()
            here = loads.take()
            piece = jnp.dot(
                low_of(right_buf[right, 0 : high - low, :]),
                every_buf[here],
                preferred_element_type=jnp.float32,
            )
            sums[part] = piece if sums[part] is None else sums[part] + piece
            rights.free()
            loads.free()
        update = sums[0] if len(sums) == 1 else jnp.concatenate(sums, axis=0)
        moment_loads[2, turn].wait()
        new = wide_buf[slot] - learn_rate * update.T
        if turn >= 2:
            outgoing[4, turn - 2].wait()
        wide_buf[slot] = new
        low_buf[slot] = low_of(new)
        put_out(3, wide_buf, new_out, turn)
        put_out(4, low_buf, low_out, turn)

    turn_group(0, [[], [], [], []])
    for piece in (0, 1):
        begin(piece)
    do = lambda act, piece: lambda: act(piece)
    turn_group(
        1, [[do(first_stage, 0)], [do(first_stage, 1)], [do(second_stage, 0)], [do(second_stage, 1)]]
    )
    for piece in (2, 3):
        begin(piece)
    turn_group(
        2,
        [[do(first_stage, 2)], [do(first_stage, 3)], [do(third_stage, 0)], [do(second_stage, 2)]],
    )
    for piece in (4, 5, 6, 7):
        begin(piece)
    third_stage(1)
    first_stage(4)
    first_stage(5)
    adam_group(0)
    g_begin(2)
    second_stage(3)
    first_stage(6)
    first_stage(7)
    third_stage(2)
    third_stage(3)
    second_stage(4)
    second_stage(5)
    adam_group(1)
    g_begin(3)
    second_stage(6)
    second_stage(7)
    outgoing[0, 1].wait()
    outgoing[0, 2].wait()
    load_weights(0)
    load_weights(1)
    for piece in (4, 5, 6, 7):
        third_stage(piece)
    adam_group(2)
    g_begin(0)
    g_begin(1)
    g_go_on(2)
    g_go_on(3)
    g_share(2)
    g_finish(2)
    update_group(0)
    g_go_on(0)
    g_go_on(1)
    g_share(3)
    g_finish(3)
    update_group(1)
    g_share(0)
    g_share(1)
    outgoing[3, 0].wait()
    load_weights(2)
    g_finish(0)
    g_finish(1)
    update_group(2)
    for copy in sends + g_sent:
        copy.wait_send()
    for number, turn in ((1, 1), (1, 2), (2, 1), (2, 2), (3, 1), (3, 2), (4, 1), (4, 2)):
        outgoing[number, turn].wait()
    move_finish()


def optimize(
    grad, output, input_grad, right_bases, bases, first_moment, second_moment, weights, widths, starts
):
    share = grad.shape[0]
    length = output.shape[0]
    low = grad.dtype
    pieces = len(pieces_of(widths, starts, True)[0])
    any_spec = pl.BlockSpec(memory_space=pl.ANY)
    vmem_spec = pl.BlockSpec(memory_space=pltpu.VMEM)
    wide = jax.ShapeDtypeStruct((D, share), jnp.float32)
    moved = jax.ShapeDtypeStruct((3, length // 4, D), low)
    dma = pltpu.SemaphoreType.DMA
    whole = pltpu.VMEM((share, D), low)
    half = pltpu.VMEM((share // 2, D), low)
    return pl.pallas_call(
        functools.partial(optimize_kernel, widths, starts),
        out_shape=(
            wide,
            wide,
            wide,
            wide,
            jax.ShapeDtypeStruct((D, share), low),
            jax.ShapeDtypeStruct((8 * share, D), low),
            moved,
            moved,
        ),
        in_specs=[vmem_spec] * 3 + [any_spec] * 5,
        out_specs=(any_spec,) * 8,
        scratch_shapes=[
            pltpu.VMEM((8 * share, D), low),
            pltpu.VMEM((4, share, D), low),
            whole,
            whole,
            half,
            half,
            whole,
            whole,
            pltpu.VMEM((2, PART, D), jnp.float32),
            pltpu.VMEM((2, D, D), jnp.float32),
            pltpu.VMEM((2, D, PART), jnp.float32),
            pltpu.VMEM((2, D, PART), jnp.float32),
            pltpu.VMEM((2, D, PART), jnp.float32),
            pltpu.VMEM((2, D, PART), low),
            pltpu.VMEM((2, D, D), low),
            dma((pieces, 4)),
            dma((pieces, 4)),
            dma((pieces, 6)),
            dma((pieces, 6)),
            dma((4, 9)),
            dma((4, 9)),
            dma((4,)),
            dma((2, 3)),
            dma((2, 4)),
            dma((2, 4)),
            dma((2,)),
            dma((2,)),
            dma((3, 2)),
            dma((5, 2)),
            dma((2,)),
        ],
        compiler_params=pltpu.CompilerParams(
            collective_id=4, has_side_effects=True, vmem_limit_bytes=67043328
        ),
        cost_estimate=pl.CostEstimate(
            flops=4 * share * D * (D + FF), bytes_accessed=8 * 40 * share * D, transcendentals=0
        ),
        name="optimize",
    )(grad, output, input_grad, right_bases, bases, first_moment, second_moment, weights)


def on_device(
    inputs,
    segments,
    cotangent,
    weights,
    first_moment,
    second_moment,
    bases,
    right_bases,
    small,
    small_first,
    small_second,
):
    number, quarter, width = inputs.shape
    length = segments.shape[1]
    groups = lax.axis_size("seq")
    owners = lax.axis_size("dp")
    place = lax.axis_index("seq")
    rows = -(-number // groups)
    padded = rows * groups
    tokens = rows * length
    block_widths = [3 * D // owners, D // owners, FF // owners, FF // owners]
    block_starts = [sum(block_widths[:which]) for which in range(4)]

    def blocks_of(matrix):
        return [
            matrix[block_starts[which] : block_starts[which] + block_widths[which]]
            for which in range(4)
        ]

    def to_rows(array):
        array = jnp.pad(array, ((0, padded - number), (0, 0), (0, 0)))
        moved = lax.all_to_all(array, "seq", split_axis=0, concat_axis=1, tiled=True)
        return moved.reshape(tokens, width)

    def to_quarters(array):
        array = array.reshape(rows, length, width)
        moved = lax.all_to_all(array, "seq", split_axis=1, concat_axis=0, tiled=True)
        return moved[:number]

    on_plane = owners == 8 and groups == 4 and number == 3
    shard = weights.astype(jnp.bfloat16).T
    if on_plane:
        w_qkv, w_out, w_up, w_down, x, pull = gather_weights(
            shard, block_widths, block_starts, (inputs, cotangent), length
        )
    else:
        x = to_rows(inputs)
        pull = to_rows(cotangent)
        w_qkv, w_out, w_up, w_down = [
            lax.all_gather(block, "dp", axis=0, tiled=True) for block in blocks_of(shard)
        ]
    bias_query, bias_value = small[4 * D : 5 * D], small[5 * D : 6 * D]
    filler = jnp.broadcast_to(
        (jnp.arange(length, dtype=jnp.int32) // TILE)[None], (padded - number, length)
    )
    marks = lax.dynamic_slice_in_dim(
        jnp.concatenate([segments, filler], axis=0), place * rows, rows, axis=0
    )
    table = key_windows(marks)
    marks_col = jnp.broadcast_to(marks.reshape(tokens, 1), (tokens, LANES))
    marks_row = marks.reshape(rows, 1, length)

    bias_qkv = jnp.concatenate([bias_query, jnp.zeros_like(bias_query), bias_value])
    project = (dot_dims(x, w_qkv, 1, 1) + bias_qkv).astype(jnp.bfloat16)
    context, log_sum = attend(table, project, marks_col, marks_row, rows, length)
    output, first_low, active, d_down, d_up, d_att, d_context, sums, up_sums = layer(
        context, x, pull, w_out, w_up, w_down, small
    )
    grad_down = low_of(dot_dims(active, d_down, 0, 0))
    grad_up = low_of(dot_dims(d_up, first_low, 0, 0))
    grad_outw = low_of(dot_dims(d_att, context, 0, 0))
    d_qkv = attend_back(table, project, d_context, marks_col, marks_row, log_sum, rows, length)
    grad_bias_query = jnp.sum(d_qkv[0].astype(jnp.float32), axis=0)
    grad_bias_value = jnp.sum(d_qkv[2].astype(jnp.float32), axis=0)
    grad_qkv = jnp.concatenate([dot_dims(d_qkv[part], x, 0, 0) for part in range(3)], axis=0).astype(
        jnp.bfloat16
    )
    input_grad = d_att.astype(jnp.float32)
    for part in range(3):
        input_grad = input_grad + dot_dims(d_qkv[part], w_qkv[part * D : (part + 1) * D], 1, 0)
    input_grad = input_grad.astype(jnp.bfloat16)

    small_local = jnp.concatenate(
        [
            sums[:4].reshape(-1),
            grad_bias_query,
            grad_bias_value,
            sums[6:].reshape(-1),
            up_sums.reshape(-1),
        ]
    )
    grads = [grad_qkv, grad_outw, grad_up, grad_down]
    if on_plane:
        mine, small_grad = plane_reduce(
            grads, block_widths, block_starts, small_local.reshape(-1, LANES)
        )
        small_grad = small_grad.reshape(-1)
        reduced, first_new, second_new, weights_new, weights_low, _, output, input_grad = optimize(
            mine,
            output,
            input_grad,
            right_bases,
            bases,
            first_moment,
            second_moment,
            weights,
            block_widths,
            block_starts,
        )
    else:
        output = to_quarters(output)
        input_grad = to_quarters(input_grad)
        scatter = lambda array: lax.psum_scatter(array, "dp", scatter_dimension=0, tiled=True)
        mine = lax.psum(jnp.concatenate([scatter(grad) for grad in grads], axis=0), "seq")
        small_grad = lax.psum(small_local, ("dp", "seq"))
        reduced = mine.T.astype(jnp.float32)
        bases_low = bases.astype(jnp.bfloat16)
        rights = [
            right_bases[
                block_starts[which] : block_starts[which] + block_widths[which],
                : owners * block_widths[which],
            ].astype(jnp.bfloat16)
            for which in range(4)
        ]
        rotated = []
        for which, block in enumerate(blocks_of(mine)):
            turned = low_of(dot_dims(block, bases_low[which], 1, 0))
            rotated.append(scatter(low_of(dot_dims(rights[which], turned, 0, 0))))
        rotated = jnp.concatenate(rotated, axis=0).T.astype(jnp.float32)
        first_new, second_new, heading = moments(rotated, first_moment, second_moment)
        heading = low_of(heading)
        update = []
        for which in range(4):
            block = heading[:, block_starts[which] : block_starts[which] + block_widths[which]]
            step = low_of(dot_dims(block, bases_low[which], 0, 1))
            every = lax.all_gather(step, "dp", axis=0, tiled=True)
            update.append(dot_dims(every, rights[which], 0, 1))
        weights_new = weights - learn_rate * jnp.concatenate(update, axis=1)
        weights_low = low_of(weights_new)
    small_first_new, small_second_new, small_heading = moments(
        small_grad, small_first, small_second
    )
    small_new = small - small_rate * small_heading
    return (
        output,
        input_grad,
        reduced,
        first_new,
        second_new,
        weights_new,
        weights_low,
        small_grad,
        small_first_new,
        small_second_new,
        small_new,
    )


def solution(mesh):
    return jax.shard_map(
        on_device,
        mesh=mesh,
        in_specs=(
            P("dp", "seq", None),
            P("dp", None),
            P("dp", "seq", None),
            P(None, "dp"),
            P(None, "dp"),
            P(None, "dp"),
            P(),
            P("dp", None),
            P(),
            P(),
            P(),
        ),
        out_specs=(
            P("dp", "seq", None),
            P("dp", "seq", None),
            P(None, "dp"),
            P(None, "dp"),
            P(None, "dp"),
            P(None, "dp"),
            P(None, "dp"),
            P(),
            P(),
            P(),
            P(),
        ),
        check_vma=False,
    )
```

```python
import functools
import math

import jax
import jax.numpy as jnp
from jax import lax
from jax.experimental import pallas as pl
from jax.experimental.pallas import tpu as pltpu
from jax.sharding import PartitionSpec as P

D = 768
HEADS = 12
HD = 64
FF = 3072
STEP = 10


norm_eps = 1e-12
beta_first = 0.9
beta_second = 0.999
adam_eps = 1e-08
learn_rate = 0.03
small_rate = 0.3

TILE = 256
LANES = 128
SIDE = 4
WINDOWS = (256, 512, 640, 768, 1024)
NEG = -1e30
VMEM_LIMIT = 60 * 1024 * 1024


def dot_dims(left, right, left_dim, right_dim):
    return lax.dot_general(
        left, right, (((left_dim,), (right_dim,)), ((), ())), preferred_element_type=jnp.float32
    )


def low_of(value):
    return value.astype(jnp.bfloat16)


def normalize(resid, gain, shift):
    centre = resid - jnp.mean(resid, axis=-1, keepdims=True)
    spread = jnp.mean(centre * centre, axis=-1, keepdims=True)
    inv_std = lax.rsqrt(spread + norm_eps)
    scaled = centre * inv_std
    return (scaled * gain + shift, scaled, inv_std)


def norm_back(grad, scaled, inv_std, gain):
    lifted = grad * gain
    return inv_std * (
        lifted
        - jnp.mean(lifted, axis=-1, keepdims=True)
        - scaled * jnp.mean(lifted * scaled, axis=-1, keepdims=True)
    )


def moments(grad, first, second):
    first_out = beta_first * first + (1.0 - beta_first) * grad
    second_out = beta_second * second + (1.0 - beta_second) * grad * grad
    heading = (
        first_out
        / (1.0 - beta_first**STEP)
        / (jnp.sqrt(second_out / (1.0 - beta_second**STEP)) + adam_eps)
    )
    return (first_out, second_out, heading)


def windows_of(length):
    return tuple(size for size in WINDOWS if size < length) + (length,)


def key_windows(marks):
    rows, length = marks.shape
    tile = min(TILE, length)
    sizes = windows_of(length)
    heads = marks[:, ::tile]
    tails = marks[:, tile - 1 :: tile]
    low = jnp.sum((marks[:, None, :] < heads[:, :, None]).astype(jnp.int32), axis=-1)
    high = jnp.sum((marks[:, None, :] <= tails[:, :, None]).astype(jnp.int32), axis=-1)
    begin = low // LANES * LANES
    need = high - begin
    which = jnp.zeros_like(need)
    for size in sizes[:-1]:
        which = which + (need > size).astype(jnp.int32)
    width = jnp.asarray(sizes, jnp.int32)[which]
    begin = jnp.minimum(begin, length - width)
    return jnp.stack([begin, which], axis=-1).reshape(rows, -1)


def head_lanes(half, shape):
    lane = lax.broadcasted_iota(jnp.int32, shape, 1)
    return (lane >= half * HD) & (lane < (half + 1) * HD)


def attend_tile(here, keys, values_of, same):
    done, logs = [], []
    for half in range(SIDE):
        mine = jnp.where(head_lanes(half, here.shape), here * HD ** (-0.5), 0.0).astype(jnp.bfloat16)
        raw = jnp.where(same, dot_dims(keys, mine, 1, 1), NEG)
        peak = jnp.max(raw, axis=0, keepdims=True)
        expo = jnp.exp(raw - peak)
        sums = jnp.sum(expo, axis=0, keepdims=True)
        mixed = jnp.dot(values_of(half), expo.astype(jnp.bfloat16), preferred_element_type=jnp.float32)
        done.append(mixed * (1.0 / sums))
        logs.append(peak + jnp.log(sums))
    return (low_of(jnp.concatenate(done, axis=0).T), jnp.concatenate(logs, axis=0))


def attend_kernel(sizes, tile, table, q_ref, k_ref, v_ref, col_ref, row_ref, ctx_ref, log_ref, vt_ref):
    length = k_ref.shape[0]
    row = pl.program_id(0)
    vt_ref[...] = v_ref[...].astype(jnp.float32).T.astype(jnp.bfloat16)

    @pl.loop(0, length // tile)
    def _(step):
        begin = pl.multiple_of(table[row, 2 * step], LANES)
        which = table[row, 2 * step + 1]
        rows = pl.ds(pl.multiple_of(step * tile, tile), tile)
        for number, size in enumerate(sizes):

            @pl.when(which == number)
            def _(size=size):
                keys = k_ref[pl.ds(begin, size), :]
                marks = col_ref[pl.ds(begin, size), :]
                same = jnp.concatenate([marks] * (tile // LANES), axis=1) == row_ref[0, :, rows]
                ctx_ref[rows, :], log_ref[0, :, rows] = attend_tile(
                    q_ref[rows, :],
                    keys,
                    lambda half: vt_ref[half * HD : (half + 1) * HD, pl.ds(begin, size)],
                    same,
                )


def attend(table, project, marks_col, marks_row, rows, length):
    pairs = HEADS // SIDE
    tile = min(TILE, length)
    sizes = windows_of(length)
    columns = lambda part: pl.BlockSpec((length, SIDE * HD), lambda i, j, t: (i, part * pairs + j))
    flops = 4 * rows * HEADS * length * length * HD
    return pl.pallas_call(
        functools.partial(attend_kernel, sizes, tile),
        out_shape=(
            jax.ShapeDtypeStruct((rows * length, D), jnp.bfloat16),
            jax.ShapeDtypeStruct((rows * pairs, SIDE, length), jnp.float32),
        ),
        grid_spec=pltpu.PrefetchScalarGridSpec(
            num_scalar_prefetch=1,
            grid=(rows, pairs),
            in_specs=[
                columns(0),
                columns(1),
                columns(2),
                pl.BlockSpec((length, LANES), lambda i, j, t: (i, 0)),
                pl.BlockSpec((1, 1, length), lambda i, j, t: (i, 0, 0)),
            ],
            out_specs=[
                pl.BlockSpec((length, SIDE * HD), lambda i, j, t: (i, j)),
                pl.BlockSpec((1, SIDE, length), lambda i, j, t: (i * pairs + j, 0, 0)),
            ],
            scratch_shapes=[pltpu.VMEM((SIDE * HD, length), jnp.bfloat16)],
        ),
        compiler_params=pltpu.CompilerParams(vmem_limit_bytes=VMEM_LIMIT),
        cost_estimate=pl.CostEstimate(
            flops=flops, bytes_accessed=8 * rows * length * D, transcendentals=rows * HEADS * length * length
        ),
        name="attend",
    )(table, project, project, project, marks_col, marks_row)


def attend_back_kernel(
    sizes, tile, table, q_ref, k_ref, v_ref, g_ref, col_ref, row_ref, log_ref, out_ref, kt_ref, dk_ref, dv_ref
):
    length = k_ref.shape[0]
    row = pl.program_id(0)
    kt_ref[...] = k_ref[...].astype(jnp.float32).T.astype(jnp.bfloat16)
    dk_ref[...] = jnp.zeros_like(dk_ref)
    dv_ref[...] = jnp.zeros_like(dv_ref)
    scale = HD ** (-0.5)

    @pl.loop(0, length // tile)
    def _(step):
        begin = pl.multiple_of(table[row, 2 * step], LANES)
        which = table[row, 2 * step + 1]
        rows = pl.ds(pl.multiple_of(step * tile, tile), tile)
        for number, size in enumerate(sizes):

            @pl.when(which == number)
            def _(size=size):
                window = pl.ds(begin, size)
                keys = k_ref[window, :]
                vals = v_ref[window, :]
                marks = col_ref[window, :]
                same = jnp.concatenate([marks] * (tile // LANES), axis=1) == row_ref[0, :, rows]
                here = q_ref[rows, :]
                grad = g_ref[rows, :]
                done = []
                for half in range(SIDE):
                    lanes = head_lanes(half, here.shape)
                    mine = jnp.where(lanes, here * scale, 0.0).astype(jnp.bfloat16)
                    own = jnp.where(lanes, grad, 0.0).astype(jnp.bfloat16)
                    raw = jnp.where(same, dot_dims(keys, mine, 1, 1), NEG)
                    probs = jnp.exp(raw - log_ref[0, half : half + 1, rows])
                    d_probs = dot_dims(vals, own, 1, 1)
                    dv_ref[window, :] += jnp.dot(
                        probs.astype(jnp.bfloat16), own, preferred_element_type=jnp.float32
                    )
                    product = probs * d_probs
                    inner = jnp.sum(product, axis=0, keepdims=True)
                    d_scores = (product - probs * inner).astype(jnp.bfloat16)
                    dk_ref[window, :] += jnp.dot(d_scores, mine, preferred_element_type=jnp.float32)
                    done.append(
                        jnp.dot(
                            kt_ref[half * HD : (half + 1) * HD, window],
                            d_scores,
                            preferred_element_type=jnp.float32,
                        )
                    )
                out_ref[0, rows, :] = (jnp.concatenate(done, axis=0) * scale).T.astype(jnp.bfloat16)

    out_ref[1, :, :] = dk_ref[...].astype(jnp.bfloat16)
    out_ref[2, :, :] = dv_ref[...].astype(jnp.bfloat16)


def attend_back(table, project, grad, marks_col, marks_row, log_sum, rows, length):
    pairs = HEADS // SIDE
    tile = min(TILE, length)
    sizes = windows_of(length)
    columns = lambda part: pl.BlockSpec((length, SIDE * HD), lambda i, j, t: (i, part * pairs + j))
    flops = 10 * rows * HEADS * length * length * HD
    return pl.pallas_call(
        functools.partial(attend_back_kernel, sizes, tile),
        out_shape=jax.ShapeDtypeStruct((3, rows * length, D), jnp.bfloat16),
        grid_spec=pltpu.PrefetchScalarGridSpec(
            num_scalar_prefetch=1,
            grid=(rows, pairs),
            in_specs=[
                columns(0),
                columns(1),
                columns(2),
                columns(0),
                pl.BlockSpec((length, LANES), lambda i, j, t: (i, 0)),
                pl.BlockSpec((1, 1, length), lambda i, j, t: (i, 0, 0)),
                pl.BlockSpec((1, SIDE, length), lambda i, j, t: (i * pairs + j, 0, 0)),
            ],
            out_specs=pl.BlockSpec((3, length, SIDE * HD), lambda i, j, t: (0, i, j)),
            scratch_shapes=[
                pltpu.VMEM((SIDE * HD, length), jnp.bfloat16),
                pltpu.VMEM((length, SIDE * HD), jnp.float32),
                pltpu.VMEM((length, SIDE * HD), jnp.float32),
            ],
        ),
        compiler_params=pltpu.CompilerParams(vmem_limit_bytes=VMEM_LIMIT),
        cost_estimate=pl.CostEstimate(
            flops=flops, bytes_accessed=14 * rows * length * D, transcendentals=rows * HEADS * length * length
        ),
        name="attend_back",
    )(table, project, project, project, grad, marks_col, marks_row, log_sum)


TOKENS = 256
PIECE = 768


def gelu_and_slope(value):
    size = jnp.abs(value)
    turn_at = 1.0 / (1.0 + size * (0.3275911 * 0.5**0.5))
    bell = jnp.exp(value * value * -0.5)
    tail = turn_at * (
        0.5 * 0.254829592
        + turn_at
        * (
            0.5 * -0.284496736
            + turn_at
            * (0.5 * 1.421413741 + turn_at * (0.5 * -1.453152027 + turn_at * (0.5 * 1.061405429)))
        )
    )
    tail = tail * bell
    chance = jnp.where(value >= 0.0, 1.0 - tail, tail)
    return (value * chance, chance + value * bell * (2.0 * math.pi) ** (-0.5))


def layer_kernel(
    context_ref,
    x_ref,
    pull_ref,
    out_w,
    up_w,
    down_w,
    small_ref,
    bias_up_ref,
    output_ref,
    first_ref,
    active_ref,
    d_down_ref,
    d_up_ref,
    d_att_ref,
    d_context_ref,
    sums_ref,
    up_sums_ref,
    slope_ref,
):
    parameter = lambda row: small_ref[row : row + 1, :]
    gain_one, gain_two, shift_one, shift_two = [parameter(row) for row in range(4)]
    bias_out, bias_down = parameter(6), parameter(7)
    attended = dot_dims(context_ref[...], out_w[...], 1, 1) + bias_out
    first, scaled_one, inv_one = normalize(
        x_ref[...].astype(jnp.float32) + attended, gain_one, shift_one
    )
    first_low = low_of(first)
    first_ref[...] = first_low
    downward = bias_down
    for begin in range(0, FF, PIECE):
        units = slice(begin, begin + PIECE)
        upward = dot_dims(first_low, up_w[units, :], 1, 1) + bias_up_ref[:, units]
        active, slope = gelu_and_slope(upward)
        active = low_of(active)
        active_ref[:, units] = active
        slope_ref[:, units] = slope
        downward = downward + jnp.dot(active, down_w[units, :], preferred_element_type=jnp.float32)
    output, scaled_two, inv_two = normalize(first + downward, gain_two, shift_two)
    output_ref[...] = low_of(output)
    grad_out = pull_ref[...].astype(jnp.float32)
    d_two = norm_back(grad_out, scaled_two, inv_two, gain_two)
    d_down = low_of(d_two)
    d_down_ref[...] = d_down
    d_first = d_two
    up_sums = []
    for begin in range(0, FF, PIECE):
        units = slice(begin, begin + PIECE)
        d_active = dot_dims(d_down, down_w[units, :], 1, 1)
        d_up = low_of(d_active * slope_ref[:, units])
        d_up_ref[:, units] = d_up
        up_sums.append(jnp.sum(d_up.astype(jnp.float32), axis=0, keepdims=True))
        d_first = d_first + jnp.dot(d_up, up_w[units, :], preferred_element_type=jnp.float32)
    d_one = norm_back(d_first, scaled_one, inv_one, gain_one)
    d_att = low_of(d_one)
    d_att_ref[...] = d_att
    d_context_ref[...] = low_of(jnp.dot(d_att, out_w[...], preferred_element_type=jnp.float32))
    total = lambda value: jnp.sum(value, axis=0, keepdims=True)
    nothing = jnp.zeros_like(gain_one)
    sums = jnp.concatenate(
        [
            total(d_first * scaled_one),
            total(grad_out * scaled_two),
            total(d_first),
            total(grad_out),
            nothing,
            nothing,
            total(d_att.astype(jnp.float32)),
            total(d_down.astype(jnp.float32)),
        ],
        axis=0,
    )
    up_sums = jnp.concatenate(up_sums, axis=1)

    @pl.when(pl.program_id(0) == 0)
    def _():
        sums_ref[...] = sums
        up_sums_ref[...] = up_sums

    @pl.when(pl.program_id(0) != 0)
    def _():
        sums_ref[...] += sums
        up_sums_ref[...] += up_sums


def layer(context, x, pull, w_out, w_up, w_down, small):
    tokens = context.shape[0]
    tile = min(TOKENS, tokens)
    narrow = pl.BlockSpec((tile, D), lambda i: (i, 0))
    broad = pl.BlockSpec((tile, FF), lambda i: (i, 0))
    fixed = lambda shape: pl.BlockSpec(shape, lambda i: (0, 0), pipeline_mode=pl.Buffered(1))
    low_narrow = jax.ShapeDtypeStruct((tokens, D), jnp.bfloat16)
    low_broad = jax.ShapeDtypeStruct((tokens, FF), jnp.bfloat16)
    return pl.pallas_call(
        layer_kernel,
        grid=(tokens // tile,),
        out_shape=(
            low_narrow,
            low_narrow,
            low_broad,
            low_narrow,
            low_broad,
            low_narrow,
            low_narrow,
            jax.ShapeDtypeStruct((8, D), jnp.float32),
            jax.ShapeDtypeStruct((1, FF), jnp.float32),
        ),
        in_specs=[
            narrow,
            narrow,
            narrow,
            fixed((D, D)),
            fixed((FF, D)),
            fixed((FF, D)),
            fixed((8, D)),
            fixed((1, FF)),
        ],
        out_specs=(
            narrow,
            narrow,
            broad,
            narrow,
            broad,
            narrow,
            narrow,
            pl.BlockSpec((8, D), lambda i: (0, 0)),
            pl.BlockSpec((1, FF), lambda i: (0, 0)),
        ),
        scratch_shapes=[pltpu.VMEM((tile, FF), jnp.float32)],
        compiler_params=pltpu.CompilerParams(vmem_limit_bytes=VMEM_LIMIT),
        cost_estimate=pl.CostEstimate(
            flops=4 * tokens * D * (D + 2 * FF),
            bytes_accessed=2 * (tokens * (7 * D + 2 * FF) + D * (D + 2 * FF)),
            transcendentals=2 * tokens * FF,
        ),
        name="layer",
    )(context, x, pull, w_out, w_up, w_down, small[: 8 * D].reshape(8, D), small[8 * D :].reshape(1, FF))


MESH = pl.DeviceIdType.MESH
ROWS = 48


def partners(me):
    core, along_x, along_y = me % 2, (me // 2) % 2, me // 4
    side_x = me + 2 - 4 * along_x
    return (me + 1 - 2 * core, side_x, me + 4 - 8 * along_y, side_x + 4 - 8 * along_y)


def send(source, target, send_sem, recv_sem, axis, place):
    return pltpu.make_async_remote_copy(
        src_ref=source,
        dst_ref=target,
        send_sem=send_sem,
        recv_sem=recv_sem,
        device_id={axis: place},
        device_id_type=MESH,
    )


def greet(peers):
    barrier = pltpu.get_barrier_semaphore()
    for axis, place in peers:
        pl.semaphore_signal(barrier, inc=1, device_id={axis: place}, device_id_type=MESH)
    pl.semaphore_wait(barrier, len(peers))


def gather_tasks(widths, starts, places, shard_ref, outs, send_sem, recv_sem, own_sem):
    me = lax.axis_index("dp")
    sib, side_x, side_y, across = partners(me)
    _, sib_x, sib_y, sib_across = partners(sib)
    arrivals = [
        (side_x, None),
        (side_y, None),
        (across, 0),
        (across, 1),
        (sib, None),
        (sib_x, None),
        (sib_y, None),
        (sib_across, 0),
        (sib_across, 1),
    ]
    sent, kept = [], {}

    def rows_at(block, owner, part):
        number, first = places[block]
        width = widths[block]
        begin = first + owner * width
        size = width
        if part is not None:
            size = width // 2
            begin = begin + part * size
        return outs[number].at[pl.ds(pl.multiple_of(begin, 16), size)]

    def put(block, kind, slot, source, owner, part, place):
        copy = send(
            source,
            rows_at(block, owner, part),
            send_sem.at[block, slot],
            recv_sem.at[block, kind],
            "dp",
            place,
        )
        copy.start()
        sent.append(copy)

    def arrived(block, kind):
        owner, part = arrivals[kind]
        region = rows_at(block, owner, part)
        send(region, region, send_sem.at[block, 0], recv_sem.at[block, kind], "dp", sib).wait_recv()

    def forward(block, kind, slot, owner, part, place):
        put(block, kind, slot, rows_at(block, owner, part), owner, part, place)

    def begin(block):
        mine = shard_ref.at[pl.ds(starts[block], widths[block])]
        put(block, 0, 0, mine, me, None, side_x)
        put(block, 1, 1, mine, me, None, side_y)
        put(block, 4, 2, mine, me, None, sib)
        copy = pltpu.make_async_copy(mine, rows_at(block, me, None), own_sem.at[block])
        copy.start()
        kept[block] = copy

    def go_on(block):
        arrived(block, 0)
        forward(block, 2, 3, side_x, 0, side_y)
        forward(block, 5, 4, side_x, None, sib)
        arrived(block, 1)
        forward(block, 3, 5, side_y, 1, side_x)
        forward(block, 6, 6, side_y, None, sib)

    def share(block):
        arrived(block, 2)
        forward(block, 7, 7, across, 0, sib)
        arrived(block, 3)
        forward(block, 8, 8, across, 1, sib)

    def finish(block):
        for kind in range(4, 9):
            arrived(block, kind)
        kept[block].wait()

    return (begin, go_on, share, finish, sent)


def move_task(moves, moved_in, moved_out, z_send, z_recv, z_own, zeros_ref):
    plane = lax.axis_index("seq")
    planes = [(plane + step) % 4 for step in range(1, 4)]

    def each_move(number, act_send, act_own, act_recv):
        source, target = moved_in[number], moved_out[number]
        if moves[number] == "in":
            quarter = source.shape[1]
            part = lambda place: target.at[pl.ds(pl.multiple_of(place * quarter, 16), quarter)]
            for row in range(3):

                @pl.when(plane != row)
                def _(row=row):
                    act_send(
                        send(
                            source.at[row],
                            part(plane),
                            z_send.at[number, row],
                            z_recv.at[number, plane],
                            "seq",
                            row,
                        )
                    )

                @pl.when(plane == row)
                def _(row=row):
                    act_own(pltpu.make_async_copy(source.at[row], part(plane), z_own.at[number, 0]))
                    for place in planes if act_recv else ():
                        act_recv(
                            send(
                                source.at[row],
                                part(place),
                                z_send.at[number, row],
                                z_recv.at[number, place],
                                "seq",
                                place,
                            )
                        )

            @pl.when(plane == 3)
            def _():
                for place in range(4):
                    act_own(pltpu.make_async_copy(zeros_ref, part(place), z_own.at[number, place]))

        else:
            quarter = target.shape[1]
            part = lambda place: source.at[pl.ds(pl.multiple_of(place * quarter, 16), quarter)]

            @pl.when(plane < 3)
            def _():
                for step, place in enumerate(planes):
                    act_send(
                        send(
                            part(place),
                            target.at[plane],
                            z_send.at[number, step],
                            z_recv.at[number, plane],
                            "seq",
                            place,
                        )
                    )
                act_own(pltpu.make_async_copy(part(plane), target.at[plane], z_own.at[number, 0]))

            for row in range(3) if act_recv else ():

                @pl.when(plane != row)
                def _(row=row):
                    act_recv(
                        send(
                            part(plane),
                            target.at[row],
                            z_send.at[number, 0],
                            z_recv.at[number, row],
                            "seq",
                            row,
                        )
                    )

    def start(number):
        each_move(number, lambda copy: copy.start(), lambda copy: copy.start(), None)

    def finish(number):
        each_move(
            number,
            lambda copy: copy.wait_send(),
            lambda copy: copy.wait(),
            lambda copy: copy.wait_recv(),
        )

    return (start, finish)


def greet_plane(with_planes):
    me, plane = lax.axis_index("dp"), lax.axis_index("seq")
    peers = [("dp", place) for place in partners(me)[:3]]
    if with_planes:
        peers += [("seq", (plane + step) % 4) for step in range(1, 4)]
    greet(peers)


SPAN = 512


def front_kernel(
    widths,
    starts,
    shard_ref,
    inputs_ref,
    cotangent_ref,
    bias_ref,
    col_ref,
    row_ref,
    w_qkv,
    w_out,
    w_up,
    w_down,
    x_out,
    pull_out,
    project_ref,
    context_ref,
    log_ref,
    x_buf,
    w_buf,
    vt_ref,
    zeros_ref,
    send_sem,
    recv_sem,
    own_sem,
    z_send,
    z_recv,
    z_own,
    load_sem,
):
    count = len(widths)
    length = x_buf.shape[0]
    wide = SIDE * HD
    zeros_ref[...] = jnp.zeros_like(zeros_ref)
    greet_plane(True)
    move, settle = move_task(
        ("in", "in"),
        (inputs_ref, cotangent_ref),
        (x_out, pull_out),
        z_send,
        z_recv,
        z_own,
        zeros_ref,
    )
    begin, go_on, share, finish, sent = gather_tasks(
        widths,
        starts,
        [(number, 0) for number in range(count)],
        shard_ref,
        [w_qkv, w_out, w_up, w_down],
        send_sem,
        recv_sem,
        own_sem,
    )
    move(0)
    for block in range(count):
        begin(block)
    go_on(0)
    go_on(1)
    share(0)
    finish(0)
    load_w = pltpu.make_async_copy(w_qkv, w_buf, load_sem.at[0])
    load_w.start()
    settle(0)
    move(1)
    load_x = pltpu.make_async_copy(x_out, x_buf, load_sem.at[1])
    load_x.start()
    share(1)
    load_w.wait()
    load_x.wait()
    tasks = {
        (0, 0): [lambda: go_on(2)],
        (1, 0): [lambda: share(2)],
        (1, 2): [lambda: go_on(3)],
        (2, 1): [lambda: share(3)],
    }
    for group in range(D // wide):
        for part in range(3):
            columns = slice(part * D + group * wide, part * D + (group + 1) * wide)
            project_ref[:, columns] = low_of(
                dot_dims(x_buf[...], w_buf[columns, :], 1, 1) + bias_ref[:, columns]
            )
        lanes = slice(group * wide, (group + 1) * wide)
        values = project_ref[:, 2 * D + group * wide : 2 * D + (group + 1) * wide]
        vt_ref[...] = low_of(values.astype(jnp.float32).T)
        for step in range(length // TILE):
            rows = slice(step * TILE, (step + 1) * TILE)
            low = max(0, step * TILE - SPAN + 1) // LANES * LANES
            high = min(length, -(-((step + 1) * TILE + SPAN - 1) // LANES) * LANES)
            marks = col_ref[low:high, :]
            same = jnp.concatenate([marks] * (TILE // LANES), axis=1) == row_ref[0, :, rows]
            context_ref[rows, lanes], log_ref[group, :, rows] = attend_tile(
                project_ref[rows, lanes],
                project_ref[low:high, D + group * wide : D + (group + 1) * wide],
                lambda half: vt_ref[half * HD : (half + 1) * HD, low:high],
                same,
            )
            for task in tasks.get((group, step), []):
                task()
    for block in range(1, count):
        finish(block)
    for copy in sent:
        copy.wait_send()
    settle(1)


def front(shard, inputs, cotangent, bias_qkv, marks_col, marks_row, widths, starts):
    count = len(widths)
    length = marks_col.shape[0]
    low = shard.dtype
    any_spec = pl.BlockSpec(memory_space=pl.ANY)
    vmem_spec = pl.BlockSpec(memory_space=pltpu.VMEM)
    dma = pltpu.SemaphoreType.DMA
    rows = jax.ShapeDtypeStruct((length, D), low)
    wide = SIDE * HD
    return pl.pallas_call(
        functools.partial(front_kernel, widths, starts),
        out_shape=tuple(jax.ShapeDtypeStruct((8 * width, D), low) for width in widths)
        + (
            rows,
            rows,
            jax.ShapeDtypeStruct((length, 3 * D), low),
            rows,
            jax.ShapeDtypeStruct((D // wide, SIDE, length), jnp.float32),
        ),
        in_specs=[vmem_spec] * 6,
        out_specs=(any_spec,) * 6 + (vmem_spec,) * 3,
        scratch_shapes=[
            pltpu.VMEM((length, D), low),
            pltpu.VMEM((3 * D, D), low),
            pltpu.VMEM((wide, length), low),
            pltpu.VMEM((length // 4, D), low),
            dma((count, 9)),
            dma((count, 9)),
            dma((count,)),
            dma((2, 3)),
            dma((2, 4)),
            dma((2, 4)),
            dma((2,)),
        ],
        compiler_params=pltpu.CompilerParams(
            collective_id=1, has_side_effects=True, vmem_limit_bytes=56 * 1024 * 1024
        ),
        cost_estimate=pl.CostEstimate(
            flops=6 * length * D * D + 4 * length * length * D,
            bytes_accessed=8 * 16 * shard.shape[0] * D,
            transcendentals=HEADS * length * length,
        ),
        name="front",
    )(shard, inputs, cotangent, bias_qkv.reshape(1, 3 * D), marks_col, marks_row)


def add_rows(target, target_at, terms, count):
    def step(number, carry):
        offset = pl.multiple_of(number * ROWS, 16)
        total = None
        for ref, begin in terms:
            value = ref[pl.ds(begin + offset, ROWS), :].astype(jnp.float32)
            total = value if total is None else total + value
        target[pl.ds(target_at + offset, ROWS), :] = total.astype(target.dtype)
        return carry

    lax.fori_loop(0, count // ROWS, step, 0)


GROUPS = (1, 2, 0)
PART = 384


def group_parts(group, joint):
    if group == 0:
        return [(0, joint, 0), (joint, PART, 1)]
    return [(0, PART, group + 1)]


def group_chunks(group, joint):
    if group == 0:
        return [(0, step * D) for step in range(3)] + [(1, 0)]
    return [(0, step * D) for step in range(4)]


class Stream:
    def __init__(self, copies):
        self.copies, self.next = copies, 0
        for copy in copies[:2]:
            copy.start()

    def take(self):
        self.copies[self.next].wait()
        self.next += 1
        return (self.next - 1) % 2

    def free(self):
        if self.next + 1 < len(self.copies):
            self.copies[self.next + 1].start()


def pieces_of(widths, starts):
    pieces = []
    for which in (2, 3, 0, 1):
        width, start = widths[which], starts[which]
        size = next(size for size in (192, 96, width) if width % size == 0)
        pieces += [(size, start + cut, (8 * start + cut, width)) for cut in range(0, width, size)]
    return [list(part) for part in zip(*pieces)]


def reduce_tasks(widths, starts, places, term, buffers, semaphores):
    given, from_x, from_y, turn_x, turn_y, total = buffers
    sib_send, sib_recv, link_send, link_recv = semaphores
    me = lax.axis_index("dp")
    sib, side_x, side_y, across = partners(me)
    _, sib_x, sib_y, sib_across = partners(sib)
    owners = (me, side_x, side_y, across)
    sib_owners = (sib, sib_x, sib_y, sib_across)
    sends, kept = [], {}

    def place_of(piece, owner):
        first, stride = places[piece]
        return pl.multiple_of(first + owner * stride, 16)

    def begin(piece):
        size = widths[piece]
        for which in (3, 1, 2, 0):
            copy = send(
                term.at[pl.ds(place_of(piece, sib_owners[which]), size)],
                given.at[which, pl.ds(starts[piece], size)],
                sib_send.at[piece, which],
                sib_recv.at[piece, which],
                "dp",
                sib,
            )
            copy.start()
            sends.append(copy)
            kept[piece, which] = copy

    def link(piece, slot, source, target, place):
        copy = send(source, target, link_send.at[piece, slot], link_recv.at[piece, slot], "dp", place)
        copy.start()
        sends.append(copy)

    def landed(piece, slot, region):
        send(region, region, link_send.at[piece, slot], link_recv.at[piece, slot], "dp", sib).wait_recv()

    def own_half(piece, which, part):
        half = widths[piece] // 2
        return pl.multiple_of(place_of(piece, owners[which]) + part * half, 16)

    def own_rows(piece, which, part):
        return term.at[pl.ds(own_half(piece, which, part), widths[piece] // 2)]

    def share_rows(ref, piece, part):
        half = widths[piece] // 2
        return ref.at[pl.ds(starts[piece] + part * half, half)]

    def turn_rows(ref, piece):
        return ref.at[pl.ds(starts[piece] // 2, widths[piece] // 2)]

    def pair_sum(piece, which):
        kept[piece, which].wait_recv()
        here = place_of(piece, owners[which])
        add_rows(term, here, [(term, here), (given.at[which], starts[piece])], widths[piece])

    def first_stage(piece):
        pair_sum(piece, 3)
        link(piece, 0, own_rows(piece, 3, 0), turn_rows(turn_x, piece), side_x)
        link(piece, 1, own_rows(piece, 3, 1), turn_rows(turn_y, piece), side_y)
        pair_sum(piece, 1)
        link(piece, 2, own_rows(piece, 1, 0), share_rows(from_x, piece, 0), side_x)
        pair_sum(piece, 2)
        link(piece, 3, own_rows(piece, 2, 1), share_rows(from_y, piece, 1), side_y)
        pair_sum(piece, 0)

    def second_stage(piece):
        half = widths[piece] // 2
        landed(piece, 0, turn_rows(turn_x, piece))
        here = own_half(piece, 2, 0)
        add_rows(term, here, [(term, here), (turn_x, starts[piece] // 2)], half)
        link(piece, 4, own_rows(piece, 2, 0), share_rows(from_y, piece, 0), side_y)
        landed(piece, 1, turn_rows(turn_y, piece))
        here = own_half(piece, 1, 1)
        add_rows(term, here, [(term, here), (turn_y, starts[piece] // 2)], half)
        link(piece, 5, own_rows(piece, 1, 1), share_rows(from_x, piece, 1), side_x)

    def third_stage(piece):
        landed(piece, 2, share_rows(from_x, piece, 0))
        landed(piece, 5, share_rows(from_x, piece, 1))
        landed(piece, 3, share_rows(from_y, piece, 1))
        landed(piece, 4, share_rows(from_y, piece, 0))
        here = starts[piece]
        add_rows(
            total,
            here,
            [(term, place_of(piece, me)), (from_x, here), (from_y, here)],
            widths[piece],
        )

    return (begin, first_stage, second_stage, third_stage, sends)


def reduce_kernel(
    widths,
    starts,
    places,
    d_up_ref,
    active_ref,
    d_qkv_ref,
    d_att_ref,
    first_low_ref,
    d_down_ref,
    x_ref,
    context_ref,
    small_ref,
    out_ref,
    small_out,
    term,
    given,
    from_x,
    from_y,
    turn_x,
    turn_y,
    total,
    left_buf,
    sib_send,
    sib_recv,
    link_send,
    link_recv,
    left_sem,
    out_sem,
    low_first,
    high_first,
    low_second,
    final,
    z_send,
    z_recv,
    small_all,
    small_planes,
    small_sum,
    small_send,
    small_recv,
    wide_send,
    wide_recv,
):
    count = len(widths)
    me = lax.axis_index("dp")
    sib = partners(me)[0]
    plane = lax.axis_index("seq")
    left_loads, right_refs = [], []
    for group in GROUPS:
        for number in range(4):
            columns = pl.ds(D * number, D)
            if group == 1:
                left, right = d_up_ref.at[:, columns], first_low_ref
            elif group == 2:
                left, right = active_ref.at[:, columns], d_down_ref
            elif number < 3:
                left, right = d_qkv_ref.at[number], x_ref
            else:
                left, right = d_att_ref, context_ref
            slot = len(left_loads) % 2
            left_loads.append(pltpu.make_async_copy(left, left_buf.at[slot], left_sem.at[slot]))
            right_refs.append(right)
    lefts = Stream(left_loads)
    others = [(me + step) % 8 for step in range(1, 8)]
    planes = [(plane + step) % 4 for step in range(1, 4)]
    greet([("dp", place) for place in others] + [("seq", place) for place in planes])
    begin, first_stage, second_stage, third_stage, sends = reduce_tasks(
        widths,
        starts,
        places,
        term,
        (given, from_x, from_y, turn_x, turn_y, total),
        (sib_send, sib_recv, link_send, link_recv),
    )
    small_all[me] = small_ref[...]
    for number, place in enumerate(others):
        copy = send(
            small_ref, small_all.at[me], small_send.at[number], small_recv.at[me], "dp", place
        )
        copy.start()
        sends.append(copy)

    def upper(block):
        return (starts[block], widths[block] // 2)

    def lower(block):
        return (starts[block] + widths[block] // 2, widths[block] // 2)

    def rows_of(part):
        return pl.ds(part[0], part[1])

    def half_of(block):
        return pl.ds(starts[block] // 2, widths[block] // 2)

    stages = [first_stage, second_stage, third_stage]
    def z_copy(block, slot, source, target, place):
        return send(source, target, z_send.at[block, slot], z_recv.at[block, slot], "seq", place)

    def z_put(block, slot, source, target, place):
        copy = z_copy(block, slot, source, target, place)
        copy.start()
        return copy

    def z_landed(block, slot, region):
        z_copy(block, slot, region, region, (plane + 1) % 4).wait_recv()

    def fourth_stage(block):
        up, down, half = rows_of(upper(block)), rows_of(lower(block)), half_of(block)

        @pl.when(plane == 0)
        def _():
            z_put(block, 0, total.at[up], low_first.at[half], 1)
            z_put(block, 1, total.at[down], low_second.at[half], 1)

        @pl.when(plane == 2)
        def _():
            z_put(block, 2, total.at[up], high_first.at[half], 1)

    def fifth_stage(block):
        up, down, half = rows_of(upper(block)), rows_of(lower(block)), half_of(block)
        middle = starts[block] // 2

        @pl.when(plane == 1)
        def _():
            z_landed(block, 0, low_first.at[half])
            z_landed(block, 2, high_first.at[half])
            begin, size = upper(block)
            add_rows(
                final, begin, [(total, begin), (low_first, middle), (high_first, middle)], size
            )
            z_put(block, 3, final.at[up], final.at[up], 0)
            z_put(block, 4, final.at[up], final.at[up], 2)
            z_landed(block, 1, low_second.at[half])
            begin, size = lower(block)
            add_rows(total, begin, [(total, begin), (low_second, middle)], size)
            z_put(block, 5, total.at[down], low_second.at[half], 2)

    def sixth_stage(block):
        up, down, half = rows_of(upper(block)), rows_of(lower(block)), half_of(block)
        middle = starts[block] // 2

        @pl.when(plane == 2)
        def _():
            z_landed(block, 5, low_second.at[half])
            begin, size = lower(block)
            add_rows(final, begin, [(total, begin), (low_second, middle)], size)
            z_put(block, 6, final.at[down], final.at[down], 1)
            z_put(block, 7, final.at[down], final.at[down], 3)
            z_landed(block, 4, final.at[up])
            z_put(block, 8, final.at[up], final.at[up], 3)

    def seventh_stage(block):
        down = rows_of(lower(block))

        @pl.when(plane == 1)
        def _():
            z_landed(block, 6, final.at[down])
            z_put(block, 9, final.at[down], final.at[down], 0)

    def eighth_stage(block):
        up, down, half = rows_of(upper(block)), rows_of(lower(block)), half_of(block)

        @pl.when(plane == 0)
        def _():
            z_landed(block, 3, final.at[up])
            z_landed(block, 9, final.at[down])
            z_copy(block, 0, total.at[up], low_first.at[half], 1).wait_send()
            z_copy(block, 1, total.at[down], low_second.at[half], 1).wait_send()

        @pl.when(plane == 1)
        def _():
            z_copy(block, 3, final.at[up], final.at[up], 0).wait_send()
            z_copy(block, 4, final.at[up], final.at[up], 2).wait_send()
            z_copy(block, 5, total.at[down], low_second.at[half], 2).wait_send()
            z_copy(block, 9, final.at[down], final.at[down], 0).wait_send()

        @pl.when(plane == 2)
        def _():
            z_copy(block, 2, total.at[up], high_first.at[half], 1).wait_send()
            z_copy(block, 6, final.at[down], final.at[down], 1).wait_send()
            z_copy(block, 7, final.at[down], final.at[down], 3).wait_send()
            z_copy(block, 8, final.at[up], final.at[up], 3).wait_send()

        @pl.when(plane == 3)
        def _():
            z_landed(block, 7, final.at[down])
            z_landed(block, 8, final.at[up])

    stages += [fourth_stage, fifth_stage, sixth_stage, seventh_stage, eighth_stage]

    outgoing = []

    def last_stage(block):
        here = pl.ds(starts[block], widths[block])
        copy = pltpu.make_async_copy(final.at[here], out_ref.at[here], out_sem.at[block])
        copy.start()
        outgoing.append(copy)

    stages.append(last_stage)

    def small_first():
        for place in others:
            send(
                small_ref, small_all.at[place], small_send.at[0], small_recv.at[place], "dp", sib
            ).wait_recv()
        total_small = small_all[0]
        for number in range(1, 8):
            total_small = total_small + small_all[number]
        small_sum[...] = total_small
        small_planes[plane] = total_small
        for number, place in enumerate(planes):
            copy = send(
                small_sum, small_planes.at[plane], wide_send.at[number], wide_recv.at[plane], "seq", place
            )
            copy.start()
            sends.append(copy)

    def small_second():
        for place in planes:
            send(
                small_sum, small_planes.at[place], wide_send.at[0], wide_recv.at[place], "seq", place
            ).wait_recv()
        small_out[...] = (small_planes[0] + small_planes[1]) + (small_planes[2] + small_planes[3])

    done = [0] * count

    def advance(piece, upto):
        while done[piece] < upto:
            stages[done[piece]](piece)
            done[piece] += 1

    between = {
        (1, 0): [(0, 1)],
        (1, 1): [(1, 1)],
        (1, 2): [(0, 2)],
        (1, 3): [(1, 2)],
        (2, 0): [(2, 1), (0, 4)],
        (2, 1): [(3, 1), (1, 4)],
        (2, 2): [(2, 2), (0, 5)],
        (2, 3): [(3, 2), (1, 5)],
    }
    ready = ((0, 1), (2, 3), (4, 5, 6, 7))
    for turn, group in enumerate(GROUPS):
        for number in range(4):
            right = right_refs[4 * turn + number]
            slot = lefts.take()
            begin_row = FF * group + D * number
            term[begin_row : begin_row + D, :] = low_of(dot_dims(left_buf[slot], right[...], 0, 0))
            lefts.free()
            for piece, upto in between.get((turn, number), []):
                advance(piece, upto)
        for piece in ready[turn]:
            begin(piece)
    small_first()
    for tick in range(count + len(stages) - 1):
        for number in range(len(stages) - 1, -1, -1):
            piece = tick - number
            if 0 <= piece < count and done[piece] <= number:
                advance(piece, number + 1)
    small_second()
    for copy in sends:
        copy.wait_send()
    for copy in outgoing:
        copy.wait()


def reduce_all(lefts, rights, small, widths, starts):
    widths, starts, places = pieces_of(widths, starts)
    count = len(widths)
    share = sum(widths)
    tokens, depth = rights[0].shape
    low = rights[0].dtype
    whole = pltpu.VMEM((share, depth), low)
    half = pltpu.VMEM((share // 2, depth), low)
    dma = pltpu.SemaphoreType.DMA
    any_spec = pl.BlockSpec(memory_space=pl.ANY)
    vmem_spec = pl.BlockSpec(memory_space=pltpu.VMEM)
    return pl.pallas_call(
        functools.partial(reduce_kernel, widths, starts, places),
        out_shape=(
            jax.ShapeDtypeStruct((share, depth), low),
            jax.ShapeDtypeStruct(small.shape, small.dtype),
        ),
        in_specs=[any_spec] * 4 + [vmem_spec] * 5,
        out_specs=(any_spec, vmem_spec),
        scratch_shapes=[
            pltpu.VMEM((8 * share, depth), low),
            pltpu.VMEM((4, share, depth), low),
            whole,
            whole,
            half,
            half,
            whole,
            pltpu.VMEM((2, tokens, depth), low),
            dma((count, 4)),
            dma((count, 4)),
            dma((count, 6)),
            dma((count, 6)),
            dma((2,)),
            dma((count,)),
            half,
            half,
            half,
            whole,
            dma((count, 10)),
            dma((count, 10)),
            pltpu.VMEM((8,) + small.shape, small.dtype),
            pltpu.VMEM((4,) + small.shape, small.dtype),
            pltpu.VMEM(small.shape, small.dtype),
            dma((7,)),
            dma((8,)),
            dma((3,)),
            dma((4,)),
        ],
        compiler_params=pltpu.CompilerParams(
            collective_id=2, has_side_effects=True, vmem_limit_bytes=60 * 1024 * 1024
        ),
        cost_estimate=pl.CostEstimate(
            flops=2 * tokens * 8 * share * depth, bytes_accessed=8 * 20 * share * depth, transcendentals=0
        ),
        name="reduce_all",
    )(*lefts, *rights, small)


def optimize_kernel(
    block_widths,
    block_starts,
    grad_ref,
    output_ref,
    input_grad_ref,
    right_ref,
    bases_ref,
    first_ref,
    second_ref,
    weights_ref,
    reduced_out,
    first_out,
    second_out,
    new_out,
    low_out,
    every_out,
    output_out,
    input_grad_out,
    term,
    given,
    from_x,
    from_y,
    turn_x,
    turn_y,
    total,
    shard,
    right_buf,
    basis_buf,
    first_buf,
    second_buf,
    wide_buf,
    low_buf,
    every_buf,
    sib_send,
    sib_recv,
    link_send,
    link_recv,
    gather_send,
    gather_recv,
    gather_own,
    z_send,
    z_recv,
    z_own,
    right_sem,
    basis_sem,
    in_sem,
    out_sem,
    every_sem,
):
    joint = block_widths[0]
    widths, starts, places = pieces_of(block_widths, block_starts)

    right_loads, basis_loads = [], []
    for group in GROUPS + GROUPS:
        parts = group_parts(group, joint)
        for part, column in group_chunks(group, joint):
            low, high, _ = parts[part]
            slot = len(right_loads) % 2
            right_loads.append(
                pltpu.make_async_copy(
                    right_ref.at[pl.ds(PART * group + low, high - low), pl.ds(column, D)],
                    right_buf.at[slot, pl.ds(0, high - low)],
                    right_sem.at[slot],
                )
            )
        for _, _, basis in parts:
            slot = len(basis_loads) % 2
            basis_loads.append(
                pltpu.make_async_copy(bases_ref.at[basis], basis_buf.at[slot], basis_sem.at[slot])
            )

    def columns(ref, group):
        return ref.at[:, pl.ds(PART * group, PART)]

    def load_moments(turn):
        for number, (ref, buf) in enumerate(((first_ref, first_buf), (second_ref, second_buf))):
            copy = pltpu.make_async_copy(
                columns(ref, GROUPS[turn]), buf.at[turn % 2], in_sem.at[number, turn % 2]
            )
            copy.start()
            moment_loads[number, turn] = copy

    def put_out(number, buf, ref, turn):
        copy = pltpu.make_async_copy(
            buf.at[turn % 2], columns(ref, GROUPS[turn]), out_sem.at[number, turn % 2]
        )
        copy.start()
        outgoing[number, turn] = copy

    moment_loads, outgoing = {}, {}
    greet_plane(True)
    move_start, move_finish = move_task(
        ("out", "out"),
        (output_ref, input_grad_ref),
        (output_out, input_grad_out),
        z_send,
        z_recv,
        z_own,
        None,
    )
    rights, bases = Stream(right_loads), Stream(basis_loads)
    for number in range(2):
        move_start(number)
    for turn in range(2):
        load_moments(turn)


    def turn_group(turn, between):
        group = GROUPS[turn]
        parts = group_parts(group, joint)
        rows = slice(PART * group, PART * (group + 1))
        grad = grad_ref[rows, :]
        if turn >= 2:
            outgoing[0, turn - 2].wait()
        wide_buf[turn % 2] = grad.astype(jnp.float32).T
        put_out(0, wide_buf, reduced_out, turn)
        turned = []
        for low, high, _ in parts:
            slot = bases.take()
            turned.append(
                low_of(
                    jnp.dot(
                        grad[low:high], low_of(basis_buf[slot]), preferred_element_type=jnp.float32
                    )
                )
            )
            bases.free()
        for number, (part, _) in enumerate(group_chunks(group, joint)):
            low, high, _ = parts[part]
            slot = rights.take()
            right = low_of(right_buf[slot, 0 : high - low, :].T)
            begin = FF * group + D * number
            term[begin : begin + D, :] = low_of(
                jnp.dot(right, turned[part], preferred_element_type=jnp.float32)
            )
            rights.free()
            for task in between[number]:
                task()

    begin, first_stage, second_stage, third_stage, sends = reduce_tasks(
        widths,
        starts,
        places,
        term,
        (given, from_x, from_y, turn_x, turn_y, total),
        (sib_send, sib_recv, link_send, link_recv),
    )


    def adam_group(turn):
        group = GROUPS[turn]
        slot = turn % 2
        for number in range(2):
            moment_loads[number, turn].wait()
        rows = slice(PART * group, PART * (group + 1))
        rotated = total[rows, :].astype(jnp.float32).T
        first, second, heading = moments(rotated, first_buf[slot], second_buf[slot])
        first_buf[slot] = first
        second_buf[slot] = second
        put_out(1, first_buf, first_out, turn)
        put_out(2, second_buf, second_out, turn)
        heading = low_of(heading.T)
        for low, high, _ in group_parts(group, joint):
            basis = bases.take()
            shard[PART * group + low : PART * group + high, :] = low_of(
                dot_dims(heading[low:high], low_of(basis_buf[basis]), 1, 1)
            )
            bases.free()
        if turn == 1:
            for number in (1, 2):
                outgoing[number, 0].wait()
            load_moments(2)

    every_places = [(0, 8 * start) for start in block_starts]
    g_begin, g_go_on, g_share, g_finish, g_sent = gather_tasks(
        block_widths, block_starts, every_places, shard, [every_out], gather_send, gather_recv, gather_own
    )


    def load_weights(turn):
        copy = pltpu.make_async_copy(
            columns(weights_ref, GROUPS[turn]), wide_buf.at[turn % 2], in_sem.at[2, turn % 2]
        )
        copy.start()
        moment_loads[2, turn] = copy

    def update_group(turn):
        group = GROUPS[turn]
        slot = turn % 2
        parts = group_parts(group, joint)
        chunks = group_chunks(group, joint)
        loads = Stream(
            [
                pltpu.make_async_copy(
                    every_out.at[pl.ds(FF * group + D * number, D)],
                    every_buf.at[number % 2],
                    every_sem.at[number % 2],
                )
                for number in range(4)
            ]
        )
        sums = [None] * len(parts)
        for number, (part, _) in enumerate(chunks):
            low, high, _ = parts[part]
            right = rights.take()
            here = loads.take()
            piece = jnp.dot(
                low_of(right_buf[right, 0 : high - low, :]),
                every_buf[here],
                preferred_element_type=jnp.float32,
            )
            sums[part] = piece if sums[part] is None else sums[part] + piece
            rights.free()
            loads.free()
        update = sums[0] if len(sums) == 1 else jnp.concatenate(sums, axis=0)
        moment_loads[2, turn].wait()
        new = wide_buf[slot] - learn_rate * update.T
        if turn >= 2:
            outgoing[4, turn - 2].wait()
        wide_buf[slot] = new
        low_buf[slot] = low_of(new)
        put_out(3, wide_buf, new_out, turn)
        put_out(4, low_buf, low_out, turn)

    turn_group(0, [[], [], [], []])
    for piece in (0, 1):
        begin(piece)
    do = lambda act, piece: lambda: act(piece)
    turn_group(
        1, [[do(first_stage, 0)], [do(first_stage, 1)], [do(second_stage, 0)], [do(second_stage, 1)]]
    )
    for piece in (2, 3):
        begin(piece)
    turn_group(
        2,
        [[do(first_stage, 2)], [do(first_stage, 3)], [do(third_stage, 0)], [do(second_stage, 2)]],
    )
    for piece in (4, 5, 6, 7):
        begin(piece)
    third_stage(1)
    first_stage(4)
    first_stage(5)
    adam_group(0)
    g_begin(2)
    second_stage(3)
    first_stage(6)
    first_stage(7)
    third_stage(2)
    third_stage(3)
    second_stage(4)
    second_stage(5)
    adam_group(1)
    g_begin(3)
    second_stage(6)
    second_stage(7)
    outgoing[0, 1].wait()
    outgoing[0, 2].wait()
    load_weights(0)
    load_weights(1)
    for piece in (4, 5, 6, 7):
        third_stage(piece)
    adam_group(2)
    g_begin(0)
    g_begin(1)
    g_go_on(2)
    g_go_on(3)
    g_share(2)
    g_finish(2)
    update_group(0)
    g_go_on(0)
    g_go_on(1)
    g_share(3)
    g_finish(3)
    update_group(1)
    g_share(0)
    g_share(1)
    outgoing[3, 0].wait()
    load_weights(2)
    g_finish(0)
    g_finish(1)
    update_group(2)
    for copy in sends + g_sent:
        copy.wait_send()
    for number, turn in ((1, 1), (1, 2), (2, 1), (2, 2), (3, 1), (3, 2), (4, 1), (4, 2)):
        outgoing[number, turn].wait()
    for number in range(2):
        move_finish(number)


def optimize(
    grad, output, input_grad, right_bases, bases, first_moment, second_moment, weights, widths, starts
):
    share = grad.shape[0]
    length = output.shape[0]
    low = grad.dtype
    pieces = len(pieces_of(widths, starts)[0])
    any_spec = pl.BlockSpec(memory_space=pl.ANY)
    vmem_spec = pl.BlockSpec(memory_space=pltpu.VMEM)
    wide = jax.ShapeDtypeStruct((D, share), jnp.float32)
    moved = jax.ShapeDtypeStruct((3, length // 4, D), low)
    dma = pltpu.SemaphoreType.DMA
    whole = pltpu.VMEM((share, D), low)
    half = pltpu.VMEM((share // 2, D), low)
    return pl.pallas_call(
        functools.partial(optimize_kernel, widths, starts),
        out_shape=(
            wide,
            wide,
            wide,
            wide,
            jax.ShapeDtypeStruct((D, share), low),
            jax.ShapeDtypeStruct((8 * share, D), low),
            moved,
            moved,
        ),
        in_specs=[vmem_spec] * 3 + [any_spec] * 5,
        out_specs=(any_spec,) * 8,
        scratch_shapes=[
            pltpu.VMEM((8 * share, D), low),
            pltpu.VMEM((4, share, D), low),
            whole,
            whole,
            half,
            half,
            whole,
            whole,
            pltpu.VMEM((2, PART, D), jnp.float32),
            pltpu.VMEM((2, D, D), jnp.float32),
            pltpu.VMEM((2, D, PART), jnp.float32),
            pltpu.VMEM((2, D, PART), jnp.float32),
            pltpu.VMEM((2, D, PART), jnp.float32),
            pltpu.VMEM((2, D, PART), low),
            pltpu.VMEM((2, D, D), low),
            dma((pieces, 4)),
            dma((pieces, 4)),
            dma((pieces, 6)),
            dma((pieces, 6)),
            dma((4, 9)),
            dma((4, 9)),
            dma((4,)),
            dma((2, 3)),
            dma((2, 4)),
            dma((2, 4)),
            dma((2,)),
            dma((2,)),
            dma((3, 2)),
            dma((5, 2)),
            dma((2,)),
        ],
        compiler_params=pltpu.CompilerParams(
            collective_id=4, has_side_effects=True, vmem_limit_bytes=67043328
        ),
        cost_estimate=pl.CostEstimate(
            flops=4 * share * D * (D + FF), bytes_accessed=8 * 40 * share * D, transcendentals=0
        ),
        name="optimize",
    )(grad, output, input_grad, right_bases, bases, first_moment, second_moment, weights)


def on_device(
    inputs,
    segments,
    cotangent,
    weights,
    first_moment,
    second_moment,
    bases,
    right_bases,
    small,
    small_first,
    small_second,
):
    number, quarter, width = inputs.shape
    length = segments.shape[1]
    groups = lax.axis_size("seq")
    owners = lax.axis_size("dp")
    place = lax.axis_index("seq")
    rows = -(-number // groups)
    padded = rows * groups
    tokens = rows * length
    block_widths = [3 * D // owners, D // owners, FF // owners, FF // owners]
    block_starts = [sum(block_widths[:which]) for which in range(4)]

    def blocks_of(matrix):
        return [
            matrix[block_starts[which] : block_starts[which] + block_widths[which]]
            for which in range(4)
        ]

    def to_rows(array):
        array = jnp.pad(array, ((0, padded - number), (0, 0), (0, 0)))
        moved = lax.all_to_all(array, "seq", split_axis=0, concat_axis=1, tiled=True)
        return moved.reshape(tokens, width)

    def to_quarters(array):
        array = array.reshape(rows, length, width)
        moved = lax.all_to_all(array, "seq", split_axis=1, concat_axis=0, tiled=True)
        return moved[:number]

    on_plane = owners == 8 and groups == 4 and number == 3
    shard = weights.astype(jnp.bfloat16).T
    bias_query, bias_value = small[4 * D : 5 * D], small[5 * D : 6 * D]
    filler = jnp.broadcast_to(
        (jnp.arange(length, dtype=jnp.int32) // TILE)[None], (padded - number, length)
    )
    marks = lax.dynamic_slice_in_dim(
        jnp.concatenate([segments, filler], axis=0), place * rows, rows, axis=0
    )
    table = key_windows(marks)
    marks_col = jnp.broadcast_to(marks.reshape(tokens, 1), (tokens, LANES))
    marks_row = marks.reshape(rows, 1, length)

    bias_qkv = jnp.concatenate([bias_query, jnp.zeros_like(bias_query), bias_value])
    if on_plane:
        w_qkv, w_out, w_up, w_down, x, pull, project, context, log_sum = front(
            shard, inputs, cotangent, bias_qkv, marks_col, marks_row, block_widths, block_starts
        )
    else:
        x = to_rows(inputs)
        pull = to_rows(cotangent)
        w_qkv, w_out, w_up, w_down = [
            lax.all_gather(block, "dp", axis=0, tiled=True) for block in blocks_of(shard)
        ]
        project = low_of(dot_dims(x, w_qkv, 1, 1) + bias_qkv)
        context, log_sum = attend(table, project, marks_col, marks_row, rows, length)
    output, first_low, active, d_down, d_up, d_att, d_context, sums, up_sums = layer(
        context, x, pull, w_out, w_up, w_down, small
    )
    d_qkv = attend_back(table, project, d_context, marks_col, marks_row, log_sum, rows, length)
    grad_bias_query = jnp.sum(d_qkv[0].astype(jnp.float32), axis=0)
    grad_bias_value = jnp.sum(d_qkv[2].astype(jnp.float32), axis=0)
    input_grad = d_att.astype(jnp.float32)
    for part in range(3):
        input_grad = input_grad + dot_dims(d_qkv[part], w_qkv[part * D : (part + 1) * D], 1, 0)
    input_grad = input_grad.astype(jnp.bfloat16)

    small_local = jnp.concatenate(
        [
            sums[:4].reshape(-1),
            grad_bias_query,
            grad_bias_value,
            sums[6:].reshape(-1),
            up_sums.reshape(-1),
        ]
    )
    if on_plane:
        mine, small_grad = reduce_all(
            (d_up, active, d_qkv, d_att),
            (first_low, d_down, x, context),
            small_local.reshape(-1, LANES),
            block_widths,
            block_starts,
        )
        small_grad = small_grad.reshape(-1)
        reduced, first_new, second_new, weights_new, weights_low, _, output, input_grad = optimize(
            mine,
            output,
            input_grad,
            right_bases,
            bases,
            first_moment,
            second_moment,
            weights,
            block_widths,
            block_starts,
        )
    else:
        grads = [dot_dims(d_qkv[part], x, 0, 0) for part in range(3)]
        grads = [
            low_of(grad)
            for grad in (
                jnp.concatenate(grads, axis=0),
                dot_dims(d_att, context, 0, 0),
                dot_dims(d_up, first_low, 0, 0),
                dot_dims(active, d_down, 0, 0),
            )
        ]
        output = to_quarters(output)
        input_grad = to_quarters(input_grad)
        scatter = lambda array: lax.psum_scatter(array, "dp", scatter_dimension=0, tiled=True)
        mine = lax.psum(jnp.concatenate([scatter(grad) for grad in grads], axis=0), "seq")
        small_grad = lax.psum(small_local, ("dp", "seq"))
        reduced = mine.T.astype(jnp.float32)
        bases_low = bases.astype(jnp.bfloat16)
        rights = [
            right_bases[
                block_starts[which] : block_starts[which] + block_widths[which],
                : owners * block_widths[which],
            ].astype(jnp.bfloat16)
            for which in range(4)
        ]
        rotated = []
        for which, block in enumerate(blocks_of(mine)):
            turned = low_of(dot_dims(block, bases_low[which], 1, 0))
            rotated.append(scatter(low_of(dot_dims(rights[which], turned, 0, 0))))
        rotated = jnp.concatenate(rotated, axis=0).T.astype(jnp.float32)
        first_new, second_new, heading = moments(rotated, first_moment, second_moment)
        heading = low_of(heading)
        update = []
        for which in range(4):
            block = heading[:, block_starts[which] : block_starts[which] + block_widths[which]]
            step = low_of(dot_dims(block, bases_low[which], 0, 1))
            every = lax.all_gather(step, "dp", axis=0, tiled=True)
            update.append(dot_dims(every, rights[which], 0, 1))
        weights_new = weights - learn_rate * jnp.concatenate(update, axis=1)
        weights_low = low_of(weights_new)
    small_first_new, small_second_new, small_heading = moments(
        small_grad, small_first, small_second
    )
    small_new = small - small_rate * small_heading
    return (
        output,
        input_grad,
        reduced,
        first_new,
        second_new,
        weights_new,
        weights_low,
        small_grad,
        small_first_new,
        small_second_new,
        small_new,
    )


def solution(mesh):
    return jax.shard_map(
        on_device,
        mesh=mesh,
        in_specs=(
            P("dp", "seq", None),
            P("dp", None),
            P("dp", "seq", None),
            P(None, "dp"),
            P(None, "dp"),
            P(None, "dp"),
            P(),
            P("dp", None),
            P(),
            P(),
            P(),
        ),
        out_specs=(
            P("dp", "seq", None),
            P("dp", "seq", None),
            P(None, "dp"),
            P(None, "dp"),
            P(None, "dp"),
            P(None, "dp"),
            P(None, "dp"),
            P(),
            P(),
            P(),
            P(),
        ),
        check_vma=False,
    )
```
